32 devices in a mesh: region: 8 (over z, core), feat: 4 (over y, x).
Axes of the slice: x: 2, y: 2, z: 4, core: 2. Of those that a mesh axis runs over, the one named last changes fastest.
Arguments:
- node_lat: bfloat16 [3072, 512], P(('region', 'feat')), may hold values from -6 to 6
- edge_lat: bfloat16 [24576, 512], P(('region', 'feat')), may hold values from -6 to 6
- receiver_row: int32 [24576], P('region'), may hold values from 0 to 383
- sender_slot: int32 [24576], P('region'), may hold values from 0 to 511, as said below
- send_rows: int32 [8, 8, 16], P('region'), may hold values from 0 to 383
- w_edge_in: bfloat16 [3, 512, 512], P(None, 'feat'), may hold values from -0.15625 to 0.15625
- w_edge_out: bfloat16 [512, 512], P('feat'), may hold values from -0.25 to 0.25
- w_node_in: bfloat16 [2, 512, 512], P(None, 'feat'), may hold values from -0.1875 to 0.1875
- w_node_out: bfloat16 [512, 512], P('feat'), may hold values from -0.25 to 0.25
- edge_gain: float32 [512], P('feat'), may hold values from 0.1 to 1.9
- node_gain: float32 [512], P('feat'), may hold values from 0.1 to 1.9
- node_cot: bfloat16 [3072, 512], P(('region', 'feat')), may hold values from -6 to 6
- edge_cot: bfloat16 [24576, 512], P(('region', 'feat')), may hold values from -6 to 6
Outputs:
- node_new: bfloat16 [3072, 512], P(('region', 'feat'))
- edge_new: bfloat16 [24576, 512], P(('region', 'feat'))
- node_grad: float32 [3072, 512], P(('region', 'feat'))
- edge_grad: float32 [24576, 512], P(('region', 'feat'))
- grad_edge_in: float32 [3, 512, 512], P(None, 'feat')
- grad_edge_out: float32 [512, 512], P('feat')
- grad_node_in: float32 [2, 512, 512], P(None, 'feat')
- grad_node_out: float32 [512, 512], P('feat')
The draws below stay inside these ranges and needn't reach their ends.
Inputs may be any that keep to these rules, and one draw needn't show every extreme that they name: `receiver_row`: edge e lies in region e // 3072; its receiver is that row of the region's 384 nodes. `sender_slot`: A value below 384 is a row of the edge's own region; a value 384 + p * 16 + s names the node that region p lists in slot s for the edge's region, and p is never the edge's own region. send_rows[p, r, s] is a row of region p's 384 nodes.
All inputs are finite; a program needn't handle non-finite values.
Results may differ from the reference program's by a relative error of at most 0.02.
Values may be sent and summed in bfloat16 or wider, within the bound.
No kernel may reach another device: no remote copies, remote signals or barrier semaphores. Data moves between devices by JAX's collectives and lax.ppermute only.
A program may use at most 64 MiB of HBM per device.

```python
import jax
import jax.numpy as jnp
from jax import lax

D = 512
NODE_DEV = 384
DEGREE = 8
SLOTS = 16
REGIONS = 8
EDGE_DEV = 3072
NODES = 3072
EDGES = 24576


def draw_sender_slot(key, part):
    edge_total = NODE_DEV * DEGREE * REGIONS
    subkeys = jax.random.split(jax.random.fold_in(key, 17), 6)
    region = jnp.arange(edge_total, dtype=jnp.int32) // (NODE_DEV * DEGREE)
    kind_draw = jax.random.randint(subkeys[0], (edge_total,), 0, 10)
    local_rows = jax.random.randint(subkeys[1], (edge_total,), 0, NODE_DEV)
    near_steps = jax.random.randint(subkeys[2], (edge_total,), 1, 4) * (2 * jax.random.randint(subkeys[3], (edge_total,), 0, 2) - 1)
    far_steps = jax.random.randint(subkeys[4], (edge_total,), 1, REGIONS)
    step_draw = jnp.where(kind_draw < 7, near_steps, far_steps)
    peer_ids = (region + step_draw) % REGIONS
    slot_draw = jax.random.randint(subkeys[5], (edge_total,), 0, SLOTS)
    return jnp.where(kind_draw < 4, local_rows, NODE_DEV + peer_ids * SLOTS + slot_draw).astype(jnp.int32)


def set_ends(array, own_key, smallest, top_value):
    place = [jax.random.randint(jax.random.fold_in(own_key, axis), (), 0, length) for axis, length in enumerate(array.shape)]
    widest = array.shape.index(max(array.shape))
    neighbour = place[:widest] + [(place[widest] + 1) % array.shape[widest]] + place[widest + 1:]
    return array.at[tuple(place)].set(smallest).at[tuple(neighbour)].set(top_value)


def shard_levels(stream_key, extent, shards, low, high):
    level = 1.0
    for axis_at, parts in shards:
        heights = jax.random.uniform(jax.random.fold_in(jax.random.fold_in(stream_key, 6), axis_at), (parts,), jnp.float32, low / len(shards), high / len(shards))
        level = level * jnp.repeat(jnp.exp(heights), extent[axis_at] // parts).reshape((-1,) + (1,) * (len(extent) - 1 - axis_at))
    return level


def noise(own_key, extent, width, bound, shards=(), held_as=jnp.bfloat16):
    entries = width * jax.random.normal(own_key, extent, jnp.float32)
    if shards:
        entries = entries * shard_levels(own_key, extent, shards, -0.22, 0.18)
    return jnp.clip(entries, -bound, bound).astype(held_as)


def setup_inputs(seed: int = 0) -> dict:
    arg_keys = jax.random.split(jax.random.key(seed), 14)
    return {
        "node_lat": noise(arg_keys[0], (NODES, D), 1.0, 6.0, ((0, 32),)),
        "edge_lat": noise(arg_keys[1], (EDGES, D), 1.0, 6.0, ((0, 32),)),
        "receiver_row": set_ends(jax.random.randint(arg_keys[2], (EDGES,), 0, NODE_DEV), jax.random.fold_in(arg_keys[2], 1), 0, NODE_DEV - 1).astype(jnp.int32),
        "sender_slot": draw_sender_slot(jax.random.fold_in(arg_keys[13], 71), 0),
        "send_rows": set_ends(jax.random.randint(arg_keys[4], (REGIONS, REGIONS, SLOTS), 0, NODE_DEV), jax.random.fold_in(arg_keys[4], 1), 0, NODE_DEV - 1).astype(jnp.int32),
        "w_edge_in": noise(arg_keys[5], (3, D, D), (3 * D) ** -0.5, 0.15625, ((1, 4),)),
        "w_edge_out": noise(arg_keys[6], (D, D), D ** -0.5, 0.25, ((0, 4),)),
        "w_node_in": noise(arg_keys[7], (2, D, D), (2 * D) ** -0.5, 0.1875, ((1, 4),)),
        "w_node_out": noise(arg_keys[8], (D, D), D ** -0.5, 0.25, ((0, 4),)),
        "edge_gain": jnp.clip(1.0 + 0.18 * jax.random.normal(arg_keys[9], (D,), jnp.float32), 0.1, 1.9),
        "node_gain": jnp.clip(1.0 + 0.18 * jax.random.normal(arg_keys[10], (D,), jnp.float32), 0.1, 1.9),
        "node_cot": noise(arg_keys[11], (NODES, D), 1.0, 6.0, ((0, 32),)),
        "edge_cot": noise(arg_keys[12], (EDGES, D), 1.0, 6.0, ((0, 32),)),
    }


EPSILON = 1e-05

def apply_swish(values):
    return values * jax.nn.sigmoid(values)

def swish_slope(values):
    sigmoid_value = jax.nn.sigmoid(values)
    return sigmoid_value * (1.0 + values * (1.0 - sigmoid_value))

def layer_norm(values, gain_values):
    average = lax.optimization_barrier(jnp.mean(values, axis=1, keepdims=True))
    variance = lax.optimization_barrier(jnp.mean(values * values, axis=1, keepdims=True)) - average * average
    inverse = lax.rsqrt(variance + EPSILON)
    normed = (values - average) * inverse
    return (normed, inverse, normed * gain_values)

def layer_norm_back(cotangent, normed, inverse, gain_values):
    scaled = cotangent * gain_values
    first_mean = lax.optimization_barrier(jnp.mean(scaled, axis=1, keepdims=True))
    second_mean = lax.optimization_barrier(jnp.mean(scaled * normed, axis=1, keepdims=True))
    return (inverse * (scaled - first_mean - normed * second_mean)).astype(jnp.bfloat16)

def matmul(first_operand, second_operand):
    return jnp.dot(first_operand, second_operand, preferred_element_type=jnp.float32)

def matmul_back(first_operand, second_operand):
    return jnp.dot(first_operand, second_operand.T, preferred_element_type=jnp.float32)

def transposed(first_operand, second_operand):
    return jnp.dot(first_operand.T, second_operand, preferred_element_type=jnp.float32)

def reference(node_lat, edge_lat, receiver_row, sender_slot, send_rows, w_edge_in, w_edge_out, w_node_in, w_node_out, edge_gain, node_gain, node_cot, edge_cot):
    edge_region = (jnp.arange(EDGES, dtype=jnp.int32) // EDGE_DEV).astype(jnp.int32)
    receiver_index = (edge_region * NODE_DEV + receiver_row).astype(jnp.int32)
    remote = jnp.maximum(sender_slot - NODE_DEV, 0).astype(jnp.int32)
    peer_region = (remote // SLOTS).astype(jnp.int32)
    slot_index = (remote % SLOTS).astype(jnp.int32)
    remote_row = send_rows[peer_region, edge_region, slot_index]
    sender_index = jnp.where(sender_slot < NODE_DEV, edge_region * NODE_DEV + sender_slot, peer_region * NODE_DEV + remote_row).astype(jnp.int32)
    senders = node_lat[sender_index]
    receivers = node_lat[receiver_index]
    pre_hidden = matmul(edge_lat, w_edge_in[0]) + matmul(senders, w_edge_in[1]) + matmul(receivers, w_edge_in[2])
    hidden = apply_swish(pre_hidden).astype(jnp.bfloat16)
    edge_mix = matmul(hidden, w_edge_out)
    edge_normed, edge_inverse, edge_update = layer_norm(edge_mix, edge_gain)
    edge_new = (edge_lat.astype(jnp.float32) + edge_update).astype(jnp.bfloat16)
    pooled = jax.ops.segment_sum(edge_new.astype(jnp.float32), receiver_index, num_segments=NODES).astype(jnp.bfloat16)
    node_pre = matmul(node_lat, w_node_in[0]) + matmul(pooled, w_node_in[1])
    node_hidden = apply_swish(node_pre).astype(jnp.bfloat16)
    node_mix = matmul(node_hidden, w_node_out)
    node_normed, node_inverse, node_update = layer_norm(node_mix, node_gain)
    node_new = (node_lat.astype(jnp.float32) + node_update).astype(jnp.bfloat16)
    node_mix_grad = layer_norm_back(node_cot.astype(jnp.float32), node_normed, node_inverse, node_gain)
    node_pre_grad = (matmul_back(node_mix_grad, w_node_out) * swish_slope(node_pre)).astype(jnp.bfloat16)
    node_direct = matmul_back(node_pre_grad, w_node_in[0])
    pooled_grad = matmul_back(node_pre_grad, w_node_in[1])
    edge_total = edge_cot.astype(jnp.float32) + pooled_grad[receiver_index]
    edge_mix_grad = layer_norm_back(edge_total, edge_normed, edge_inverse, edge_gain)
    pre_grad = (matmul_back(edge_mix_grad, w_edge_out) * swish_slope(pre_hidden)).astype(jnp.bfloat16)
    edge_grad = edge_total + matmul_back(pre_grad, w_edge_in[0])
    sender_grad = matmul_back(pre_grad, w_edge_in[1])
    receiver_grad = matmul_back(pre_grad, w_edge_in[2])
    node_grad = node_cot.astype(jnp.float32) + node_direct + jax.ops.segment_sum(receiver_grad, receiver_index, num_segments=NODES) + jax.ops.segment_sum(sender_grad, sender_index, num_segments=NODES)
    edge_norm = 1.0 / jnp.sqrt(jnp.float32(EDGES))
    node_norm = 1.0 / jnp.sqrt(jnp.float32(NODES))
    grad_edge_in = jnp.stack([transposed(edge_lat, pre_grad), transposed(senders, pre_grad), transposed(receivers, pre_grad)], axis=0) * edge_norm
    grad_edge_out = transposed(hidden, edge_mix_grad) * edge_norm
    grad_node_in = jnp.stack([transposed(node_lat, node_pre_grad), transposed(pooled, node_pre_grad)], axis=0) * node_norm
    grad_node_out = transposed(node_hidden, node_mix_grad) * node_norm
    return (node_new, edge_new, node_grad, edge_grad, grad_edge_in, grad_edge_out, grad_node_in, grad_node_out)
```

```python
import jax
import jax.numpy as jnp
from jax import lax
from jax.sharding import PartitionSpec as P

EPSILON = 1e-05
F32 = jnp.float32
BF16 = jnp.bfloat16


def dot(a, b):
    return jnp.dot(a, b, preferred_element_type=F32)


def dot_t(a, b):
    return lax.dot_general(a, b, (((1,), (1,)), ((), ())), preferred_element_type=F32)


def t_dot(a, b):
    return lax.dot_general(a, b, (((0,), (0,)), ((), ())), preferred_element_type=F32)


def swap(x, axis, bits):
    n = lax.axis_size(axis)
    return lax.ppermute(x, axis, [(i, i ^ bits) for i in range(n)])


def add_all(parts):
    total = parts[0].astype(F32)
    for part in parts[1:]:
        total = total + part.astype(F32)
    return total


def layer_norm(values):
    breadth = values.shape[1]
    average = jnp.sum(values, axis=1, keepdims=True) / breadth
    variance = jnp.sum(values * values, axis=1, keepdims=True) / breadth - average * average
    inverse = lax.rsqrt(variance + EPSILON)
    return (values - average) * inverse, inverse


def layer_norm_back(scaled, normed, inverse):
    breadth = scaled.shape[1]
    first = jnp.sum(scaled, axis=1, keepdims=True) / breadth
    second = jnp.sum(scaled * normed, axis=1, keepdims=True) / breadth
    return (inverse * (scaled - first - normed * second)).astype(BF16)


def swish_and_slope(values):
    s = jax.nn.sigmoid(values)
    return (values * s).astype(BF16), s * (1.0 + values * (1.0 - s))


def gather_weights(stacked, parity):
    n = lax.axis_size("feat")
    here = lax.axis_index("feat")
    m, portion, d = stacked.shape
    half = portion // 2
    mine = lax.dynamic_slice(stacked, (0, parity * half, 0), (m, half, d))
    full = jnp.zeros((m, n * portion, d), stacked.dtype)
    full = lax.dynamic_update_slice(full, stacked, (0, here * portion, 0))
    for b in range(1, n):
        got = swap(mine, "feat", b)
        other = swap(got, "region", 1)
        start = (here ^ b) * portion
        full = lax.dynamic_update_slice(full, got, (0, start + parity * half, 0))
        full = lax.dynamic_update_slice(full, other, (0, start + (1 - parity) * half, 0))
    return full


def region_exchange(rows):
    regions, slots, d = rows.shape
    pairs = rows.reshape(regions // 2, 2, slots, d)
    keep = pairs[:, 0]
    other = swap(pairs[:, 1], "region", 1)
    both = jnp.concatenate([keep, other], axis=1)
    blocks = [both[0]] + [swap(both[b], "region", 2 * b) for b in range(1, regions // 2)]
    return jnp.concatenate(blocks, axis=0)


def reduce_grads(partial, parity, here):
    n = lax.axis_size("feat")
    regions = lax.axis_size("region")
    nz = regions // 2
    z = lax.axis_index("region") // 2
    m, rows, d = partial.shape
    portion = rows // n
    half = m * portion // 2
    blocks = partial.astype(BF16).reshape(m, n, portion, d).transpose(1, 0, 2, 3).reshape(n, 2, half, d)
    keep = lax.dynamic_index_in_dim(blocks, parity, 1, keepdims=False)
    send = lax.dynamic_index_in_dim(blocks, 1 - parity, 1, keepdims=False)
    chip = (keep.astype(F32) + swap(send, "region", 1).astype(F32)).astype(BF16)
    parts = [
        lax.dynamic_index_in_dim(chip, here ^ b, 0, keepdims=False) for b in range(n)
    ]
    parts = [parts[0]] + [swap(parts[b], "feat", b) for b in range(1, n)]
    mine = add_all(parts).astype(BF16).reshape(nz, half // nz, d)
    parts = [lax.dynamic_index_in_dim(mine, z ^ b, 0, keepdims=False) for b in range(nz)]
    parts = [parts[0]] + [swap(parts[b], "region", 2 * b) for b in range(1, nz)]
    chunk = add_all(parts).astype(BF16)
    whole = jnp.zeros((nz, half // nz, d), BF16)
    for b in range(nz):
        got = chunk if b == 0 else swap(chunk, "region", 2 * b)
        whole = lax.dynamic_update_slice(whole, got[None], (z ^ b, 0, 0))
    whole = whole.reshape(half, d)
    other = swap(whole, "region", 1)
    out = jnp.where(
        parity == 0,
        jnp.concatenate([whole, other], axis=0),
        jnp.concatenate([other, whole], axis=0),
    )
    return out.astype(F32).reshape(m, portion, d)


def shards(
    node_lat,
    edge_lat,
    receiver_row,
    sender_slot,
    send_rows,
    w_edge_in,
    w_edge_out,
    w_node_in,
    w_node_out,
    edge_gain,
    node_gain,
    node_cot,
    edge_cot,
):
    n = lax.axis_size("feat")
    regions = lax.axis_size("region")
    here = lax.axis_index("feat")
    region = lax.axis_index("region")
    parity = region % 2
    own, d = node_lat.shape
    nodes = own * n
    share = edge_lat.shape[0]
    slots = send_rows.shape[2]

    def relative(row):
        return ((row // own) ^ here) * own + row % own

    local_receivers = lax.dynamic_slice_in_dim(receiver_row, here * share, share)
    local_senders = lax.dynamic_slice_in_dim(sender_slot, here * share, share)
    remote = jnp.maximum(local_senders - nodes, 0)
    sender_at = jnp.where(
        local_senders < nodes,
        relative(local_senders),
        nodes + ((remote // slots) ^ region) * slots + remote % slots,
    )
    receiver_at = relative(local_receivers)
    send_at = relative(send_rows[0])[jnp.arange(regions) ^ region].reshape(-1)
    table_size = nodes + regions * slots

    gains = jnp.stack([edge_gain, node_gain], axis=0)
    gain_full = jnp.zeros((2, n * gains.shape[1]), F32)
    for b in range(n):
        got = gains if b == 0 else swap(gains, "feat", b)
        gain_full = lax.dynamic_update_slice(gain_full, got, (0, (here ^ b) * gains.shape[1]))

    near = jnp.concatenate([node_lat] + [swap(node_lat, "feat", b) for b in range(1, n)], axis=0)
    w_edge = gather_weights(jnp.concatenate([w_edge_in, w_edge_out[None]], axis=0), parity)
    w_node = gather_weights(jnp.concatenate([w_node_in, w_node_out[None]], axis=0), parity)

    send_hot = (send_at[:, None] == jnp.arange(nodes)[None, :]).astype(BF16)
    outgoing = dot(send_hot, near).astype(BF16).reshape(regions, slots, d)
    table = jnp.concatenate([near, region_exchange(outgoing)], axis=0)

    sender_hot = (sender_at[:, None] == jnp.arange(table_size)[None, :]).astype(BF16)
    receiver_hot = (receiver_at[:, None] == jnp.arange(nodes)[None, :]).astype(BF16)
    senders = dot(sender_hot, table).astype(BF16)
    receivers = dot(receiver_hot, near).astype(BF16)
    pre_hidden = dot(edge_lat, w_edge[0]) + dot(senders, w_edge[1]) + dot(receivers, w_edge[2])
    hidden, slope = swish_and_slope(pre_hidden)
    normed, inverse = layer_norm(dot(hidden, w_edge[3]))
    edge_new = (edge_lat.astype(F32) + normed * gain_full[0]).astype(BF16)
    pooled_part = t_dot(receiver_hot, edge_new).astype(BF16).reshape(n, own, d)
    pooled = add_all(
        [pooled_part[0]] + [swap(pooled_part[b], "feat", b) for b in range(1, n)]
    ).astype(BF16)

    node_pre = dot(node_lat, w_node[0]) + dot(pooled, w_node[1])
    node_hidden, node_slope = swish_and_slope(node_pre)
    node_normed, node_inverse = layer_norm(dot(node_hidden, w_node[2]))
    node_new = (node_lat.astype(F32) + node_normed * gain_full[1]).astype(BF16)
    cot = node_cot.astype(F32)
    node_mix_grad = layer_norm_back(cot * gain_full[1], node_normed, node_inverse)
    node_pre_grad = (dot_t(node_mix_grad, w_node[2]) * node_slope).astype(BF16)
    pooled_grad = dot_t(node_pre_grad, w_node[1]).astype(BF16)
    grad_near = jnp.concatenate(
        [pooled_grad] + [swap(pooled_grad, "feat", b) for b in range(1, n)], axis=0
    )
    node_base = cot + dot_t(node_pre_grad, w_node[0])
    node_partial = jnp.stack(
        [t_dot(node_lat, node_pre_grad), t_dot(pooled, node_pre_grad), t_dot(node_hidden, node_mix_grad)]
    )
    node_grads = reduce_grads(node_partial, parity, here)

    edge_total = edge_cot.astype(F32) + dot(receiver_hot, grad_near)
    edge_mix_grad = layer_norm_back(edge_total * gain_full[0], normed, inverse)
    pre_grad = (dot_t(edge_mix_grad, w_edge[3]) * slope).astype(BF16)
    edge_partial = jnp.stack(
        [
            t_dot(edge_lat, pre_grad),
            t_dot(senders, pre_grad),
            t_dot(receivers, pre_grad),
            t_dot(hidden, edge_mix_grad),
        ]
    )
    edge_grads = reduce_grads(edge_partial, parity, here)
    edge_grad = edge_total + dot_t(pre_grad, w_edge[0])

    sent = t_dot(sender_hot, pre_grad).astype(BF16)
    received = t_dot(receiver_hot, pre_grad).astype(BF16)
    table_grad = dot_t(sent, w_edge[1])
    remote_grad = table_grad[nodes:].astype(BF16).reshape(regions, slots, d)
    returned = region_exchange(remote_grad)
    near_grad = table_grad[:nodes] + dot_t(received, w_edge[2])
    near_grad = (near_grad + t_dot(send_hot, returned)).astype(BF16).reshape(n, own, d)
    node_grad = node_base + add_all(
        [near_grad[0]] + [swap(near_grad[b], "feat", b) for b in range(1, n)]
    )

    edge_norm = 1.0 / jnp.sqrt(F32(share * n * regions))
    node_norm = 1.0 / jnp.sqrt(F32(nodes * regions))
    return (
        node_new,
        edge_new,
        node_grad,
        edge_grad,
        edge_grads[:3] * edge_norm,
        edge_grads[3] * edge_norm,
        node_grads[:2] * node_norm,
        node_grads[2] * node_norm,
    )


def solution(mesh):
    rows = P(("region", "feat"), None)
    in_specs = (
        rows,
        rows,
        P("region"),
        P("region"),
        P("region", None, None),
        P(None, "feat", None),
        P("feat", None),
        P(None, "feat", None),
        P("feat", None),
        P("feat"),
        P("feat"),
        rows,
        rows,
    )
    out_specs = (
        rows,
        rows,
        rows,
        rows,
        P(None, "feat", None),
        P("feat", None),
        P(None, "feat", None),
        P("feat", None),
    )
    return jax.shard_map(shards, mesh=mesh, in_specs=in_specs, out_specs=out_specs, check_vma=False)
```

```python
import functools

import jax
import jax.numpy as jnp
from jax import lax
from jax.experimental import pallas as pl
from jax.experimental.pallas import tpu as pltpu
from jax.sharding import PartitionSpec as P

EPSILON = 1e-05
F32 = jnp.float32
BF16 = jnp.bfloat16
VMEM_LIMIT = 36 * 1024 * 1024


def dot(a, b):
    return jnp.dot(a, b, preferred_element_type=F32)


def dot_t(a, b):
    return lax.dot_general(a, b, (((1,), (1,)), ((), ())), preferred_element_type=F32)


def t_dot(a, b):
    return lax.dot_general(a, b, (((0,), (0,)), ((), ())), preferred_element_type=F32)


def swap(x, axis, bits):
    n = lax.axis_size(axis)
    return lax.ppermute(x, axis, [(i, i ^ bits) for i in range(n)])


def add_all(parts):
    total = parts[0].astype(F32)
    for part in parts[1:]:
        total = total + part.astype(F32)
    return total


def layer_norm(values):
    breadth = values.shape[1]
    average = jnp.sum(values, axis=1, keepdims=True) / breadth
    variance = jnp.sum(values * values, axis=1, keepdims=True) / breadth - average * average
    inverse = lax.rsqrt(variance + EPSILON)
    return (values - average) * inverse, inverse


def layer_norm_back(scaled, normed, inverse):
    breadth = scaled.shape[1]
    first = jnp.sum(scaled, axis=1, keepdims=True) / breadth
    second = jnp.sum(scaled * normed, axis=1, keepdims=True) / breadth
    return (inverse * (scaled - first - normed * second)).astype(BF16)


def swish_and_slope(values):
    s = 1.0 / (1.0 + jnp.exp(-values))
    return (values * s).astype(BF16), s * (1.0 + values * (1.0 - s))


def hot(column, width):
    at = lax.broadcasted_iota(jnp.int32, (column.shape[0], width), 1)
    return jnp.where(column == at, 1.0, 0.0).astype(BF16)


def hot_t(row, height):
    at = lax.broadcasted_iota(jnp.int32, (height, row.shape[1]), 0)
    return jnp.where(row == at, 1.0, 0.0).astype(BF16)


def tile_of(rows):
    for size in (256, 192, 128, 96, 64, 48, 32, 16):
        if rows % size == 0:
            return size
    return rows


def shape(dims, dtype=BF16):
    return jax.ShapeDtypeStruct(tuple(dims), dtype)


def whole_block(dims):
    return pl.BlockSpec(tuple(dims), lambda *_: (0,) * len(dims))


def call(kernel, ins, outs, scratch=(), name=None, flops=0):
    return pl.pallas_call(
        kernel,
        out_shape=tuple(outs),
        grid=(1,),
        in_specs=[whole_block(x.shape) for x in ins],
        out_specs=tuple(whole_block(x.shape) for x in outs),
        scratch_shapes=list(scratch),
        compiler_params=pltpu.CompilerParams(vmem_limit_bytes=VMEM_LIMIT),
        cost_estimate=pl.CostEstimate(
            flops=flops,
            bytes_accessed=sum(x.size * x.dtype.itemsize for x in (*ins, *outs)),
            transcendentals=0,
        ),
        name=name,
    )(*ins)


def fill_weights(w_ref, own_in, own_out, pieces, parity, here):
    m = w_ref.shape[0]
    portion = own_out.shape[0]
    half = portion // 2
    at = pl.multiple_of(here * portion, half)
    for k in range(m):
        w_ref[k, pl.ds(at, portion), :] = own_in[k] if k < m - 1 else own_out[...]
    for b, (got, other) in enumerate(pieces, start=1):
        start = (here ^ b) * portion
        first = pl.multiple_of(start + parity * half, half)
        second = pl.multiple_of(start + (1 - parity) * half, half)
        for k in range(m):
            w_ref[k, pl.ds(first, half), :] = got[k]
            w_ref[k, pl.ds(second, half), :] = other[k]


def split_grads(read, m, n, portion, keep, send, parity, here):
    half = portion // 2
    for side in range(2):

        @pl.when(parity == side)
        def _():
            for f in range(n):
                for u in range(2 * m):
                    out = keep if u // m == side else send
                    rows = read(u // 2, f * portion + (u % 2) * half, half)
                    out[f ^ here, pl.ds((u % m) * half, half), :] = rows.astype(BF16)


def outgoing_kernel(n, at_ref, *refs):
    near, (keep, send) = refs[:n], refs[n : n + 2]
    own = near[0].shape[0]
    rows = jnp.zeros((at_ref.shape[0], near[0].shape[1]), F32)
    for b in range(n):
        rows = rows + dot(hot(at_ref[...] - b * own, own), near[b][...])
    rows = rows.astype(BF16)
    pairs, slots, _ = keep.shape
    for b in range(pairs):
        keep[b] = rows[(2 * b) * slots : (2 * b + 1) * slots]
        send[b] = rows[(2 * b + 1) * slots : (2 * b + 2) * slots]


def edge_forward_kernel(n, pairs, *refs):
    edge, s_at, r_at, r_row, gain, own_in, own_out = refs[:7]
    refs = refs[7:]
    tables, refs = refs[: n + pairs], refs[n + pairs :]
    pieces = [(refs[2 * b], refs[2 * b + 1]) for b in range(n - 1)]
    refs = refs[2 * (n - 1) :]
    new, hidden_ref, slope_ref, normed_ref, inverse_ref, table, w = refs[:7]
    pooled, total = refs[7 : 7 + n], refs[7 + n]
    here = lax.axis_index("feat")
    parity = lax.axis_index("region") % 2
    own = tables[0].shape[0]
    nodes = own * n

    @pl.when(pl.program_id(0) == 0)
    def _():
        at = 0
        for piece in tables:
            table[at : at + piece.shape[0], :] = piece[...]
            at += piece.shape[0]
        fill_weights(w, own_in, own_out, pieces, parity, here)
        total[...] = jnp.zeros_like(total)

    lat = edge[...]
    senders = dot(hot(s_at[...], table.shape[0]), table[...]).astype(BF16)
    receivers = dot(hot(r_at[...], nodes), table[:nodes, :]).astype(BF16)
    pre = dot(lat, w[0]) + dot(senders, w[1]) + dot(receivers, w[2])
    hidden, slope = swish_and_slope(pre)
    hidden_ref[...] = hidden
    slope_ref[...] = slope.astype(BF16)
    normed, inverse = layer_norm(dot(hidden, w[3]))
    normed_ref[...] = normed.astype(BF16)
    inverse_ref[...] = jnp.broadcast_to(inverse, inverse_ref.shape)
    updated = (lat.astype(F32) + normed * gain[...]).astype(BF16)
    new[...] = updated
    total[...] += dot(hot_t(r_row[...], nodes), updated)

    @pl.when(pl.program_id(0) == pl.num_programs(0) - 1)
    def _():
        for b in range(n):
            pooled[b][...] = total[b * own : (b + 1) * own, :].astype(BF16)


def node_kernel(n, lat_ref, cot_ref, gain, own_in, own_out, *refs):
    parts, refs = refs[:n], refs[n:]
    pieces = [(refs[2 * b], refs[2 * b + 1]) for b in range(n - 1)]
    refs = refs[2 * (n - 1) :]
    new, pooled_grad, base, pooled_ref, hidden_ref, mix_grad_ref, pre_grad_ref, w = refs
    here = lax.axis_index("feat")
    parity = lax.axis_index("region") % 2
    fill_weights(w, own_in, own_out, pieces, parity, here)
    pooled = add_all([part[...] for part in parts]).astype(BF16)
    pooled_ref[...] = pooled
    lat = lat_ref[...]
    pre = dot(lat, w[0]) + dot(pooled, w[1])
    hidden, slope = swish_and_slope(pre)
    hidden_ref[...] = hidden
    normed, inverse = layer_norm(dot(hidden, w[2]))
    new[...] = (lat.astype(F32) + normed * gain[...]).astype(BF16)
    cot = cot_ref[...].astype(F32)
    mix_grad = layer_norm_back(cot * gain[...], normed, inverse)
    mix_grad_ref[...] = mix_grad
    pre_grad = (dot_t(mix_grad, w[2]) * slope).astype(BF16)
    pre_grad_ref[...] = pre_grad
    pooled_grad[...] = dot_t(pre_grad, w[1]).astype(BF16)
    base[...] = cot + dot_t(pre_grad, w[0])


def node_weight_kernel(n, lat, pooled, hidden, pre_grad, mix_grad, keep, send, grads):
    here = lax.axis_index("feat")
    parity = lax.axis_index("region") % 2
    grads[0] = t_dot(lat[...], pre_grad[...])
    grads[1] = t_dot(pooled[...], pre_grad[...])
    grads[2] = t_dot(hidden[...], mix_grad[...])
    portion = grads.shape[1] // n
    split_grads(lambda k, at, size: grads[k, at : at + size, :], 3, n, portion, keep, send, parity, here)


def edge_backward_kernel(n, *refs):
    edge, cot, hidden, slope, normed, inverse, r_at, s_row, r_row, gain, table, w = refs[:12]
    near, refs = refs[12 : 12 + n], refs[12 + n :]
    edge_grad, keep, send, near_grad, back_keep, back_send = refs[:6]
    near_all, grads, sent, received = refs[6:]
    here = lax.axis_index("feat")
    parity = lax.axis_index("region") % 2
    own = near[0].shape[0]
    nodes = own * n

    @pl.when(pl.program_id(0) == 0)
    def _():
        for b in range(n):
            near_all[b * own : (b + 1) * own, :] = near[b][...]
        grads[...] = jnp.zeros_like(grads)
        sent[...] = jnp.zeros_like(sent)
        received[...] = jnp.zeros_like(received)

    total = cot[...].astype(F32) + dot(hot(r_at[...], nodes), near_all[...])
    mix_grad = layer_norm_back(total * gain[...], normed[...].astype(F32), inverse[:, :1])
    pre_grad = (dot_t(mix_grad, w[3]) * slope[...].astype(F32)).astype(BF16)
    edge_grad[...] = total + dot_t(pre_grad, w[0])
    grads[0] += t_dot(edge[...], pre_grad)
    grads[3] += t_dot(hidden[...], mix_grad)
    sent[...] += dot(hot_t(s_row[...], table.shape[0]), pre_grad)
    received[...] += dot(hot_t(r_row[...], nodes), pre_grad)

    @pl.when(pl.program_id(0) == pl.num_programs(0) - 1)
    def _():
        from_senders = sent[...].astype(BF16)
        from_receivers = received[...].astype(BF16)
        grads[1] = t_dot(table[...], from_senders)
        grads[2] = t_dot(table[:nodes, :], from_receivers)
        portion = grads.shape[1] // n
        split_grads(lambda k, at, size: grads[k, at : at + size, :], 4, n, portion, keep, send, parity, here)
        to_table = dot_t(from_senders, w[1])
        near_grad[...] = to_table[:nodes] + dot_t(from_receivers, w[2])
        back = to_table[nodes:].astype(BF16)
        pairs, slots, _ = back_keep.shape
        for b in range(pairs):
            back_keep[b] = back[(2 * b) * slots : (2 * b + 1) * slots]
            back_send[b] = back[(2 * b + 1) * slots : (2 * b + 2) * slots]


def return_kernel(n, pairs, near_grad, at_row, *refs):
    blocks, outs = refs[:pairs], refs[pairs:]
    nodes, d = near_grad.shape
    own = nodes // n
    rows = blocks[0].shape[0]
    total = near_grad[...]
    for b in range(pairs):
        total = total + dot(hot_t(at_row[:, b * rows : (b + 1) * rows], nodes), blocks[b][...])
    for b in range(n):
        outs[b][...] = total[b * own : (b + 1) * own, :].astype(BF16)


def pair_sum_kernel(n, keep, got, *outs):
    for b in range(n):
        outs[b][...] = (keep[b].astype(F32) + got[b].astype(F32)).astype(BF16)


def scatter_sum_kernel(n, pairs, *refs):
    parts, outs, total = refs[:n], refs[n : n + pairs], refs[n + pairs]
    z = lax.axis_index("region") // 2
    total[...] = add_all([part[...] for part in parts])
    rows = outs[0].shape[0]
    for b in range(pairs):
        outs[b][...] = total[pl.ds(pl.multiple_of((z ^ b) * rows, rows), rows), :].astype(BF16)


def sum_kernel(*refs):
    refs[-1][...] = add_all([part[...] for part in refs[:-1]]).astype(BF16)


def finish_kernel(pairs, norm, *refs):
    mine, theirs = refs[:pairs], refs[pairs : 2 * pairs]
    first, last, total = refs[2 * pairs :]
    region = lax.axis_index("region")
    parity, z = region % 2, region // 2
    rows = mine[0].shape[0]
    for b in range(pairs):
        at = (z ^ b) * rows
        for side, ref in ((parity, mine[b]), (1 - parity, theirs[b])):
            start = pl.multiple_of(side * pairs * rows + at, rows)
            total[pl.ds(start, rows), :] = ref[...].astype(F32) * norm
    cut = first.shape[0]
    first[...] = total[:cut, :]
    last[...] = total[cut:, :]


def gather_weights(inner, outer, parity):
    n = lax.axis_size("feat")
    half = outer.shape[0] // 2
    stacked = jnp.concatenate([inner, outer[None]], axis=0)
    mine = lax.dynamic_slice_in_dim(stacked, parity * half, half, 1)
    pieces = []
    for b in range(1, n):
        got = swap(mine, "feat", b)
        pieces += [got, swap(got, "region", 1)]
    return pieces


def region_exchange(keep, send):
    other = swap(send, "region", 1)
    blocks = [jnp.concatenate([keep[b], other[b]], axis=0) for b in range(keep.shape[0])]
    return [blocks[0]] + [swap(blocks[b], "region", 2 * b) for b in range(1, len(blocks))]


def reduce_grads(keep, send, m, norm, name):
    n, half, d = keep.shape
    pairs = lax.axis_size("region") // 2
    portion = 2 * half // m
    z = lax.axis_index("region") // 2
    parity = lax.axis_index("region") % 2
    got = swap(send, "region", 1)
    parts = call(
        functools.partial(pair_sum_kernel, n), [keep, got], [shape((half, d))] * n, name=name + "_pair"
    )
    parts = [parts[0]] + [swap(parts[b], "feat", b) for b in range(1, n)]
    rows = half // pairs
    if rows % 16 == 0:
        parts = call(
            functools.partial(scatter_sum_kernel, n, pairs),
            parts,
            [shape((rows, d))] * pairs,
            [pltpu.VMEM((half, d), F32)],
            name=name + "_feat",
        )
    else:
        mine = add_all(parts).astype(BF16).reshape(pairs, rows, d)
        parts = [lax.dynamic_index_in_dim(mine, z ^ b, 0, keepdims=False) for b in range(pairs)]
    parts = [parts[0]] + [swap(parts[b], "region", 2 * b) for b in range(1, pairs)]
    if rows % 16 == 0:
        (chunk,) = call(sum_kernel, parts, [shape((rows, d))], name=name + "_z")
    else:
        chunk = add_all(parts).astype(BF16)
    mine = [chunk] + [swap(chunk, "region", 2 * b) for b in range(1, pairs)]
    theirs = [swap(piece, "region", 1) for piece in mine]
    if rows % 16 == 0:
        return call(
            functools.partial(finish_kernel, pairs, norm),
            mine + theirs,
            [shape(((m - 1) * portion, d), F32), shape((portion, d), F32)],
            [pltpu.VMEM((m * portion, d), F32)],
            name=name + "_end",
        )
    order = jnp.arange(pairs) ^ z
    sides = [jnp.stack(side)[order].reshape(half, d) for side in (mine, theirs)]
    total = jnp.where(parity == 0, jnp.concatenate(sides), jnp.concatenate(sides[::-1])).astype(F32) * norm
    return total[: (m - 1) * portion], total[(m - 1) * portion :]


def shards(
    node_lat,
    edge_lat,
    receiver_row,
    sender_slot,
    send_rows,
    w_edge_in,
    w_edge_out,
    w_node_in,
    w_node_out,
    edge_gain,
    node_gain,
    node_cot,
    edge_cot,
):
    n = lax.axis_size("feat")
    regions = lax.axis_size("region")
    pairs = regions // 2
    here = lax.axis_index("feat")
    region = lax.axis_index("region")
    parity = region % 2
    own, d = node_lat.shape
    nodes = own * n
    share = edge_lat.shape[0]
    slots = send_rows.shape[2]
    table_size = nodes + regions * slots

    def relative(row):
        return ((row // own) ^ here) * own + row % own

    local_receivers = lax.dynamic_slice_in_dim(receiver_row, here * share, share)
    local_senders = lax.dynamic_slice_in_dim(sender_slot, here * share, share)
    remote = jnp.maximum(local_senders - nodes, 0)
    sender_at = jnp.where(
        local_senders < nodes,
        relative(local_senders),
        nodes + ((remote // slots) ^ region) * slots + remote % slots,
    )
    receiver_at = relative(local_receivers)
    send_at = relative(send_rows[0])[jnp.arange(regions) ^ region].reshape(-1)

    gains = jnp.stack([edge_gain, node_gain], axis=0)
    near = [node_lat] + [swap(node_lat, "feat", b) for b in range(1, n)]
    w_edge = gather_weights(w_edge_in, w_edge_out, parity)
    gain_full = jnp.zeros((2, n * gains.shape[1]), F32)
    for b in range(n):
        got = gains if b == 0 else swap(gains, "feat", b)
        gain_full = lax.dynamic_update_slice(gain_full, got, (0, (here ^ b) * gains.shape[1]))
    w_node = gather_weights(w_node_in, w_node_out, parity)

    square = 2 * d * d
    keep, send = call(
        functools.partial(outgoing_kernel, n),
        [send_at[:, None], *near],
        [shape((pairs, slots, d))] * 2,
        name="outgoing",
        flops=2 * regions * slots * nodes * d,
    )
    remote_rows = region_exchange(keep, send)

    tile = tile_of(share)
    steps = share // tile
    by_rows = lambda width: pl.BlockSpec((tile, width), lambda i: (i, 0))
    by_columns = pl.BlockSpec((1, tile), lambda i: (0, i))
    edge_params = pltpu.CompilerParams(
        dimension_semantics=("arbitrary",), vmem_limit_bytes=VMEM_LIMIT
    )
    ins = [edge_lat, sender_at[:, None], receiver_at[:, None], receiver_at[None], gain_full[:1]]
    rest = [w_edge_in, w_edge_out, *near, *remote_rows, *w_edge]
    outs = [shape((share, d))] * 4 + [shape((share, 128), F32)]
    kept = [shape((table_size, d)), shape((4, d, d))] + [shape((own, d))] * n
    edge_new, hidden, slope, normed, inverse, table, w_full, *pooled_parts = pl.pallas_call(
        functools.partial(edge_forward_kernel, n, pairs),
        out_shape=tuple(outs + kept),
        grid=(steps,),
        in_specs=[by_rows(d), by_rows(1), by_rows(1), by_columns, whole_block((1, d))]
        + [whole_block(x.shape) for x in rest],
        out_specs=tuple([by_rows(d)] * 4 + [by_rows(128)] + [whole_block(x.shape) for x in kept]),
        scratch_shapes=[pltpu.VMEM((nodes, d), F32)],
        compiler_params=edge_params,
        cost_estimate=pl.CostEstimate(
            flops=7 * share * square, bytes_accessed=8 * share * d, transcendentals=share * d
        ),
        name="edge_forward",
    )(*ins, *rest)

    parts = [pooled_parts[0]] + [swap(pooled_parts[b], "feat", b) for b in range(1, n)]
    node_new, pooled_grad, node_base, pooled, node_hidden, mix_grad, pre_grad = call(
        functools.partial(node_kernel, n),
        [node_lat, node_cot, gain_full[1:], w_node_in, w_node_out, *parts, *w_node],
        [shape((own, d)), shape((own, d)), shape((own, d), F32)] + [shape((own, d))] * 4,
        [pltpu.VMEM((3, d, d), BF16)],
        name="node",
        flops=6 * own * square,
    )
    grad_near = [pooled_grad] + [swap(pooled_grad, "feat", b) for b in range(1, n)]
    portion = d // n
    node_keep, node_send = call(
        functools.partial(node_weight_kernel, n),
        [node_lat, pooled, node_hidden, pre_grad, mix_grad],
        [shape((n, 3 * portion // 2, d))] * 2,
        [pltpu.VMEM((3, d, d), F32)],
        name="node_weights",
        flops=3 * own * square,
    )
    node_norm = float((nodes * regions) ** -0.5)
    grad_node_in, grad_node_out = reduce_grads(node_keep, node_send, 3, node_norm, "node")

    ins = [edge_lat, edge_cot, hidden, slope, normed, inverse, receiver_at[:, None], sender_at[None], receiver_at[None]]
    rest = [gain_full[:1], table, w_full, *grad_near]
    kept = [shape((n, 2 * portion, d))] * 2 + [shape((nodes, d), F32)] + [shape((pairs, slots, d))] * 2
    edge_grad, keep, send, near_grad, back_keep, back_send = pl.pallas_call(
        functools.partial(edge_backward_kernel, n),
        out_shape=tuple([shape((share, d), F32)] + kept),
        grid=(steps,),
        in_specs=[by_rows(d)] * 5 + [by_rows(128), by_rows(1), by_columns, by_columns]
        + [whole_block(x.shape) for x in rest],
        out_specs=tuple([by_rows(d)] + [whole_block(x.shape) for x in kept]),
        scratch_shapes=[
            pltpu.VMEM((nodes, d), BF16),
            pltpu.VMEM((4, d, d), F32),
            pltpu.VMEM((table_size, d), F32),
            pltpu.VMEM((nodes, d), F32),
        ],
        compiler_params=edge_params,
        cost_estimate=pl.CostEstimate(
            flops=10 * share * square, bytes_accessed=16 * share * d, transcendentals=0
        ),
        name="edge_backward",
    )(*ins, *rest)
    edge_norm = float((share * n * regions) ** -0.5)
    grad_edge_in, grad_edge_out = reduce_grads(keep, send, 4, edge_norm, "edge")

    returned = region_exchange(back_keep, back_send)
    parts = call(
        functools.partial(return_kernel, n, pairs),
        [near_grad, send_at[None], *returned],
        [shape((own, d))] * n,
        name="give_back",
        flops=2 * regions * slots * nodes * d,
    )
    node_grad = node_base + add_all([parts[0]] + [swap(parts[b], "feat", b) for b in range(1, n)])

    return (
        node_new,
        edge_new,
        node_grad,
        edge_grad,
        grad_edge_in.reshape(w_edge_in.shape),
        grad_edge_out,
        grad_node_in.reshape(w_node_in.shape),
        grad_node_out,
    )


def solution(mesh):
    rows = P(("region", "feat"), None)
    in_specs = (
        rows,
        rows,
        P("region"),
        P("region"),
        P("region", None, None),
        P(None, "feat", None),
        P("feat", None),
        P(None, "feat", None),
        P("feat", None),
        P("feat"),
        P("feat"),
        rows,
        rows,
    )
    out_specs = (
        rows,
        rows,
        rows,
        rows,
        P(None, "feat", None),
        P("feat", None),
        P(None, "feat", None),
        P("feat", None),
    )
    return jax.shard_map(shards, mesh=mesh, in_specs=in_specs, out_specs=out_specs, check_vma=False)
```

```python
import functools

import jax
import jax.numpy as jnp
from jax import lax
from jax.experimental import pallas as pl
from jax.experimental.pallas import tpu as pltpu
from jax.sharding import PartitionSpec as P

EPSILON = 1e-05
F32 = jnp.float32
BF16 = jnp.bfloat16
VMEM_LIMIT = 36 * 1024 * 1024


def dot(a, b):
    return jnp.dot(a, b, preferred_element_type=F32)


def dot_t(a, b):
    return lax.dot_general(a, b, (((1,), (1,)), ((), ())), preferred_element_type=F32)


def t_dot(a, b):
    return lax.dot_general(a, b, (((0,), (0,)), ((), ())), preferred_element_type=F32)


def swap(x, axis, bits):
    n = lax.axis_size(axis)
    return lax.ppermute(x, axis, [(i, i ^ bits) for i in range(n)])


def add_all(parts):
    total = parts[0].astype(F32)
    for part in parts[1:]:
        total = total + part.astype(F32)
    return total


def layer_norm(values):
    breadth = values.shape[1]
    average = jnp.sum(values, axis=1, keepdims=True) / breadth
    variance = jnp.sum(values * values, axis=1, keepdims=True) / breadth - average * average
    inverse = lax.rsqrt(variance + EPSILON)
    return (values - average) * inverse, inverse


def layer_norm_back(scaled, normed, inverse):
    breadth = scaled.shape[1]
    first = jnp.sum(scaled, axis=1, keepdims=True) / breadth
    second = jnp.sum(scaled * normed, axis=1, keepdims=True) / breadth
    return (inverse * (scaled - first - normed * second)).astype(BF16)


def swish_and_slope(values):
    s = 1.0 / (1.0 + jnp.exp(-values))
    return (values * s).astype(BF16), s * (1.0 + values * (1.0 - s))


def hot(column, width):
    at = lax.broadcasted_iota(jnp.int32, (column.shape[0], width), 1)
    return jnp.where(column == at, 1.0, 0.0).astype(BF16)


def hot_t(row, height):
    at = lax.broadcasted_iota(jnp.int32, (height, row.shape[1]), 0)
    return jnp.where(row == at, 1.0, 0.0).astype(BF16)


def tile_of(rows):
    for size in (256, 192, 128, 96, 64, 48, 32, 16):
        if rows % size == 0:
            return size
    return rows


def shape(dims, dtype=BF16):
    return jax.ShapeDtypeStruct(tuple(dims), dtype)


def whole_block(dims):
    return pl.BlockSpec(tuple(dims), lambda *_: (0,) * len(dims))


def call(kernel, ins, outs, scratch=(), name=None, flops=0):
    return pl.pallas_call(
        kernel,
        out_shape=tuple(outs),
        grid=(1,),
        in_specs=[whole_block(x.shape) for x in ins],
        out_specs=tuple(whole_block(x.shape) for x in outs),
        scratch_shapes=list(scratch),
        compiler_params=pltpu.CompilerParams(vmem_limit_bytes=VMEM_LIMIT),
        cost_estimate=pl.CostEstimate(
            flops=flops,
            bytes_accessed=sum(x.size * x.dtype.itemsize for x in (*ins, *outs)),
            transcendentals=0,
        ),
        name=name,
    )(*ins)


def fill_weights(w_ref, own_in, own_out, pieces, parity, here):
    m = w_ref.shape[0]
    portion = own_out.shape[0]
    half = portion // 2
    at = pl.multiple_of(here * portion, half)
    for k in range(m):
        w_ref[k, pl.ds(at, portion), :] = own_in[k] if k < m - 1 else own_out[...]
    for b, (got, other) in enumerate(pieces, start=1):
        start = (here ^ b) * portion
        first = pl.multiple_of(start + parity * half, half)
        second = pl.multiple_of(start + (1 - parity) * half, half)
        for k in range(m):
            w_ref[k, pl.ds(first, half), :] = got[k * half : (k + 1) * half, :]
            w_ref[k, pl.ds(second, half), :] = other[k * half : (k + 1) * half, :]


def split_grads(grads, n, keep, send, parity, here):
    m = grads.shape[0]
    portion = grads.shape[1] // n
    half = portion // 2
    block = m * half
    for side in range(2):

        @pl.when(parity == side)
        def _():
            for f in range(n):
                for u in range(2 * m):
                    out = keep if u // m == side else send
                    at = f * portion + (u % 2) * half
                    start = pl.multiple_of((f ^ here) * block + (u % m) * half, half)
                    out[pl.ds(start, half), :] = grads[u // 2, at : at + half, :].astype(BF16)


def pack_kernel(edge_in, edge_out, node_in, node_out, edge_gain, node_gain, edge_pack, node_pack):
    half = edge_out.shape[0] // 2
    at = pl.multiple_of(lax.axis_index("region") % 2 * half, half)
    for inner, outer, pack in ((edge_in, edge_out, edge_pack), (node_in, node_out, node_pack)):
        m = inner.shape[0]
        for k in range(m):
            pack[k * half : (k + 1) * half, :] = inner[k, pl.ds(at, half), :]
        pack[m * half : (m + 1) * half, :] = outer[pl.ds(at, half), :]
    parts = []
    for gain in (edge_gain, node_gain):
        left = gain[...]
        for _ in range(3):
            part = left.astype(BF16)
            left = left - part.astype(F32)
            parts.append(part.astype(F32))
    parts.append(jnp.zeros((16 - len(parts), left.shape[1]), F32))
    below = edge_pack.shape[0] - 16
    edge_pack[below:, :] = jnp.zeros((16, edge_pack.shape[1]), BF16)
    edge_pack[below:, : left.shape[1]] = jnp.concatenate(parts, axis=0).astype(BF16)


def fill_gains(gain_ref, blocks, own, pieces, here):
    portion = blocks.shape[2]
    blocks[here, 0:1, :] = own[0][...]
    blocks[here, 1:2, :] = own[1][...]
    for b, (got, _) in enumerate(pieces, start=1):
        parts = got[got.shape[0] - 16 :, :portion].astype(F32)
        blocks[here ^ b, 0:1, :] = parts[0:1] + parts[1:2] + parts[2:3]
        blocks[here ^ b, 1:2, :] = parts[3:4] + parts[4:5] + parts[5:6]
    for f in range(blocks.shape[0]):
        gain_ref[0:2, f * portion : (f + 1) * portion] = blocks[f, 0:2, :]


def outgoing_kernel(n, at_ref, *refs):
    near, (keep, send) = refs[:n], refs[n : n + 2]
    own = near[0].shape[0]
    rows = jnp.zeros((at_ref.shape[0], near[0].shape[1]), F32)
    for b in range(n):
        rows = rows + dot(hot(at_ref[...] - b * own, own), near[b][...])
    rows = rows.astype(BF16)
    pairs, slots, _ = keep.shape
    for b in range(pairs):
        keep[b] = rows[(2 * b) * slots : (2 * b + 1) * slots]
        send[b] = rows[(2 * b + 1) * slots : (2 * b + 2) * slots]


def edge_forward_kernel(n, pairs, *refs):
    edge, s_at, r_at, r_row, edge_gain, node_gain, own_in, own_out = refs[:8]
    refs = refs[8:]
    tables, refs = refs[: n + pairs], refs[n + pairs :]
    pieces = [(refs[2 * b], refs[2 * b + 1]) for b in range(n - 1)]
    refs = refs[2 * (n - 1) :]
    new, hidden_ref, slope_ref, normed_ref, inverse_ref, table, w, gains = refs[:8]
    pooled, total, blocks = refs[8 : 8 + n], refs[8 + n], refs[9 + n]
    here = lax.axis_index("feat")
    parity = lax.axis_index("region") % 2
    own = tables[0].shape[0]
    nodes = own * n

    @pl.when(pl.program_id(0) == 0)
    def _():
        at = 0
        for piece in tables:
            table[at : at + piece.shape[0], :] = piece[...]
            at += piece.shape[0]
        fill_weights(w, own_in, own_out, pieces, parity, here)
        fill_gains(gains, blocks, (edge_gain, node_gain), pieces, here)
        total[...] = jnp.zeros_like(total)

    lat = edge[...]
    senders = dot(hot(s_at[...], table.shape[0]), table[...]).astype(BF16)
    receivers = dot(hot(r_at[...], nodes), table[:nodes, :]).astype(BF16)
    pre = dot(lat, w[0]) + dot(senders, w[1]) + dot(receivers, w[2])
    hidden, slope = swish_and_slope(pre)
    hidden_ref[...] = hidden
    slope_ref[...] = slope.astype(BF16)
    normed, inverse = layer_norm(dot(hidden, w[3]))
    normed_ref[...] = normed.astype(BF16)
    inverse_ref[...] = jnp.broadcast_to(inverse, inverse_ref.shape)
    updated = (lat.astype(F32) + normed * gains[0:1, :]).astype(BF16)
    new[...] = updated
    total[...] += dot(hot_t(r_row[...], nodes), updated)

    @pl.when(pl.program_id(0) == pl.num_programs(0) - 1)
    def _():
        for b in range(n):
            pooled[b][...] = total[b * own : (b + 1) * own, :].astype(BF16)


def node_kernel(n, lat_ref, cot_ref, gains, own_in, own_out, *refs):
    parts, refs = refs[:n], refs[n:]
    pieces = [(refs[2 * b], refs[2 * b + 1]) for b in range(n - 1)]
    refs = refs[2 * (n - 1) :]
    new, pooled_grad, base = refs[:3]
    messages, w = refs[3 : 3 + n], refs[3 + n]
    here = lax.axis_index("feat")
    parity = lax.axis_index("region") % 2
    gain = gains[1:2, :]
    fill_weights(w, own_in, own_out, pieces, parity, here)
    pooled = add_all([part[...] for part in parts]).astype(BF16)
    lat = lat_ref[...]
    pre = dot(lat, w[0]) + dot(pooled, w[1])
    hidden, slope = swish_and_slope(pre)
    normed, inverse = layer_norm(dot(hidden, w[2]))
    new[...] = (lat.astype(F32) + normed * gain).astype(BF16)
    cot = cot_ref[...].astype(F32)
    mix_grad = layer_norm_back(cot * gain, normed, inverse)
    pre_grad = (dot_t(mix_grad, w[2]) * slope).astype(BF16)
    pooled_grad[...] = dot_t(pre_grad, w[1]).astype(BF16)
    base[...] = cot + dot_t(pre_grad, w[0])
    d = lat.shape[1]
    portion = d // n
    for b in range(n):
        messages[b][:, :d] = pre_grad
        messages[b][:, d : 2 * d] = mix_grad
    for f in range(n):

        @pl.when(here == f)
        def _():
            for b in range(n):
                block = slice((f ^ b) * portion, ((f ^ b) + 1) * portion)
                messages[b][:, 2 * d : 2 * d + portion] = pooled[:, block]
                messages[b][:, 2 * d + portion :] = hidden[:, block]


def node_weight_kernel(n, *refs):
    near, messages, (keep, send, lat, grads) = refs[:n], refs[n : 2 * n], refs[2 * n :]
    here = lax.axis_index("feat")
    parity = lax.axis_index("region") % 2
    own, d = near[0].shape
    portion = d // n
    for f in range(n):

        @pl.when(here == f)
        def _():
            for b in range(n):
                lat[b] = near[b][:, f * portion : (f + 1) * portion]

    totals = [jnp.zeros((portion, d), F32)] * 3
    for b in range(n):
        pre_grad = messages[b][:, :d]
        mix_grad = messages[b][:, d : 2 * d]
        totals[0] = totals[0] + t_dot(lat[b], pre_grad)
        totals[1] = totals[1] + t_dot(messages[b][:, 2 * d : 2 * d + portion], pre_grad)
        totals[2] = totals[2] + t_dot(messages[b][:, 2 * d + portion :], mix_grad)
    for k in range(3):
        grads[k * portion : (k + 1) * portion, :] = totals[k]
    half = keep.shape[0]
    keep[...] = grads[pl.ds(pl.multiple_of(parity * half, 16), half), :].astype(BF16)
    send[...] = grads[pl.ds(pl.multiple_of((1 - parity) * half, 16), half), :].astype(BF16)


def edge_backward_kernel(n, slots, *refs):
    edge, cot, hidden, slope, normed, inverse, r_at, s_row, r_row, gains, table, w = refs[:12]
    near, refs = refs[12 : 12 + n], refs[12 + n :]
    edge_grad, keep, send, near_grad = refs[:4]
    near_all, grads, sent, received = refs[4:]
    here = lax.axis_index("feat")
    parity = lax.axis_index("region") % 2
    own = near[0].shape[0]
    nodes = own * n

    @pl.when(pl.program_id(0) == 0)
    def _():
        for b in range(n):
            near_all[b * own : (b + 1) * own, :] = near[b][...]
        grads[...] = jnp.zeros_like(grads)
        sent[...] = jnp.zeros_like(sent)
        received[...] = jnp.zeros_like(received)

    total = cot[...].astype(F32) + dot(hot(r_at[...], nodes), near_all[...])
    mix_grad = layer_norm_back(total * gains[0:1, :], normed[...].astype(F32), inverse[:, :1])
    pre_grad = (dot_t(mix_grad, w[3]) * slope[...].astype(F32)).astype(BF16)
    edge_grad[...] = total + dot_t(pre_grad, w[0])
    grads[0] += t_dot(edge[...], pre_grad)
    grads[3] += t_dot(hidden[...], mix_grad)
    sent[...] += dot(hot_t(s_row[...], table.shape[0]), pre_grad)
    received[...] += dot(hot_t(r_row[...], nodes), pre_grad)

    @pl.when(pl.program_id(0) == pl.num_programs(0) - 1)
    def _():
        from_senders = sent[...].astype(BF16)
        from_receivers = received[...].astype(BF16)
        grads[1] = t_dot(table[...], from_senders)
        grads[2] = t_dot(table[:nodes, :], from_receivers)
        split_grads(grads, n, keep, send, parity, here)
        to_table = dot_t(from_senders, w[1])
        near_grad[...] = to_table[:nodes] + dot_t(from_receivers, w[2])
        back = to_table[nodes:].astype(BF16)
        at = n * grads.shape[0] * (grads.shape[1] // n // 2)
        count = (keep.shape[0] - at) // slots
        for b in range(count):
            rows = slice(at + b * slots, at + (b + 1) * slots)
            keep[rows, :] = back[(2 * b) * slots : (2 * b + 1) * slots]
            send[rows, :] = back[(2 * b + 1) * slots : (2 * b + 2) * slots]


def return_kernel(n, pairs, near_grad, at_row, *refs):
    blocks, outs = refs[:pairs], refs[pairs:]
    nodes, d = near_grad.shape
    own = nodes // n
    rows = blocks[0].shape[0]
    total = near_grad[...]
    for b in range(pairs):
        total = total + dot(hot_t(at_row[:, b * rows : (b + 1) * rows], nodes), blocks[b][...])
    for b in range(n):
        outs[b][...] = total[b * own : (b + 1) * own, :].astype(BF16)


def pair_sum_kernel(n, slots, keep, got, *outs):
    block = outs[0].shape[0]
    for b in range(n):
        rows = slice(b * block, (b + 1) * block)
        outs[b][...] = (keep[rows, :].astype(F32) + got[rows, :].astype(F32)).astype(BF16)
    for b, out in enumerate(outs[n:]):
        rows = slice(n * block + b * slots, n * block + (b + 1) * slots)
        out[:slots, :] = keep[rows, :]
        out[slots:, :] = got[rows, :]


def scatter_sum_kernel(n, pairs, *refs):
    parts, node_parts = refs[:n], refs[n : n + 2]
    outs, total = refs[n + 2 : n + 2 + pairs], refs[n + 2 + pairs]
    z = lax.axis_index("region") // 2
    cut = parts[0].shape[0]
    total[:cut, :] = add_all([part[...] for part in parts])
    total[cut:, :] = add_all([part[...] for part in node_parts])
    rows = outs[0].shape[0]
    for b in range(pairs):
        outs[b][...] = total[pl.ds(pl.multiple_of((z ^ b) * rows, rows), rows), :].astype(BF16)


def sum_kernel(*refs):
    refs[-1][...] = add_all([part[...] for part in refs[:-1]]).astype(BF16)


def finish_kernel(pairs, edge_norm, node_norm, *refs):
    mine, theirs = refs[:pairs], refs[pairs : 2 * pairs]
    outs, total = refs[2 * pairs : -1], refs[-1]
    region = lax.axis_index("region")
    parity, z = region % 2, region // 2
    rows = mine[0].shape[0]
    for b in range(pairs):
        at = (z ^ b) * rows
        for side, ref in ((parity, mine[b]), (1 - parity, theirs[b])):
            start = pl.multiple_of(side * pairs * rows + at, rows)
            total[pl.ds(start, rows), :] = ref[...].astype(F32)
    spread(total, outs, edge_norm, node_norm)


def spread(total, outs, edge_norm, node_norm):
    portion = outs[1].shape[0]
    size = total.shape[0] // 2
    for norm, m, at, pair in ((edge_norm, 4, 0, outs[:2]), (node_norm, 3, 2 * portion, outs[2:])):
        half = m * portion // 2
        for u in range(2 * m):
            row = u * (portion // 2)
            source = (row // half) * size + at + row % half
            out, start = (pair[0], row) if u < 2 * m - 2 else (pair[1], row - (m - 1) * portion)
            out[start : start + portion // 2, :] = total[source : source + portion // 2, :] * norm


def gather_halves(mine):
    pieces = []
    for b in range(1, lax.axis_size("feat")):
        got = swap(mine, "feat", b)
        pieces += [got, swap(got, "region", 1)]
    return pieces


def chip_exchange(blocks):
    return [blocks[0]] + [swap(blocks[b], "region", 2 * b) for b in range(1, len(blocks))]


def reduce_grads(parts, node_parts, portion, edge_norm, node_norm):
    n = len(parts)
    half, d = parts[0].shape
    pairs = lax.axis_size("region") // 2
    z = lax.axis_index("region") // 2
    parity = lax.axis_index("region") % 2
    size = half + node_parts[0].shape[0]
    rows = size // pairs
    outs = [shape((k * portion, d), F32) for k in (3, 1, 2, 1)]
    if rows % 16 == 0:
        parts = call(
            functools.partial(scatter_sum_kernel, n, pairs),
            [*parts, *node_parts],
            [shape((rows, d))] * pairs,
            [pltpu.VMEM((size, d), F32)],
            name="feat_sum",
        )
    else:
        mine = jnp.concatenate([add_all(parts), add_all(node_parts)]).astype(BF16).reshape(pairs, rows, d)
        parts = [lax.dynamic_index_in_dim(mine, z ^ b, 0, keepdims=False) for b in range(pairs)]
    parts = chip_exchange(parts)
    if rows % 16 == 0:
        (chunk,) = call(sum_kernel, parts, [shape((rows, d))], name="z_sum")
    else:
        chunk = add_all(parts).astype(BF16)
    mine = chip_exchange([chunk] * pairs)
    theirs = [swap(piece, "region", 1) for piece in mine]
    if rows % 16 == 0:
        return call(
            functools.partial(finish_kernel, pairs, edge_norm, node_norm),
            mine + theirs,
            outs,
            [pltpu.VMEM((2 * size, d), F32)],
            name="finish",
        )
    order = jnp.arange(pairs) ^ z
    sides = [jnp.stack(side)[order].reshape(size, d) for side in (mine, theirs)]
    total = jnp.where(parity == 0, jnp.concatenate(sides), jnp.concatenate(sides[::-1])).astype(F32)

    def from_total(*refs):
        spread(refs[0], refs[1:], edge_norm, node_norm)

    return call(from_total, [total], outs, name="finish")


def shards(
    node_lat,
    edge_lat,
    receiver_row,
    sender_slot,
    send_rows,
    w_edge_in,
    w_edge_out,
    w_node_in,
    w_node_out,
    edge_gain,
    node_gain,
    node_cot,
    edge_cot,
):
    n = lax.axis_size("feat")
    regions = lax.axis_size("region")
    pairs = regions // 2
    here = lax.axis_index("feat")
    region = lax.axis_index("region")
    parity = region % 2
    own, d = node_lat.shape
    nodes = own * n
    share = edge_lat.shape[0]
    slots = send_rows.shape[2]
    table_size = nodes + regions * slots

    def relative(row):
        return ((row // own) ^ here) * own + row % own

    local_receivers = lax.dynamic_slice_in_dim(receiver_row, here * share, share)
    local_senders = lax.dynamic_slice_in_dim(sender_slot, here * share, share)
    remote = jnp.maximum(local_senders - nodes, 0)
    sender_at = jnp.where(
        local_senders < nodes,
        relative(local_senders),
        nodes + ((remote // slots) ^ region) * slots + remote % slots,
    )
    receiver_at = relative(local_receivers)
    send_at = relative(send_rows[0])[jnp.arange(regions) ^ region].reshape(-1)

    portion = d // n
    half = portion // 2
    gain_rows = [edge_gain[None], node_gain[None]]
    near = [node_lat] + [swap(node_lat, "feat", b) for b in range(1, n)]
    edge_pack, node_pack = call(
        pack_kernel,
        [w_edge_in, w_edge_out, w_node_in, w_node_out, *gain_rows],
        [shape((4 * half + 16, d)), shape((3 * half, d))],
        name="pack",
    )
    w_edge = gather_halves(edge_pack)

    square = 2 * d * d
    keep, send = call(
        functools.partial(outgoing_kernel, n),
        [send_at[:, None], *near],
        [shape((pairs, slots, d))] * 2,
        name="outgoing",
        flops=2 * regions * slots * nodes * d,
    )
    other = swap(send, "region", 1)
    remote_rows = chip_exchange([jnp.concatenate([keep[b], other[b]], axis=0) for b in range(pairs)])
    node_pack, _ = lax.optimization_barrier((node_pack, other))
    w_node = gather_halves(node_pack)

    tile = tile_of(share)
    steps = share // tile
    by_rows = lambda width: pl.BlockSpec((tile, width), lambda i: (i, 0))
    by_columns = pl.BlockSpec((1, tile), lambda i: (0, i))
    edge_params = pltpu.CompilerParams(
        dimension_semantics=("arbitrary",), vmem_limit_bytes=VMEM_LIMIT
    )
    ins = [edge_lat, sender_at[:, None], receiver_at[:, None], receiver_at[None]]
    rest = [*gain_rows, w_edge_in, w_edge_out, *near, *remote_rows, *w_edge]
    outs = [shape((share, d))] * 4 + [shape((share, 128), F32)]
    kept = [shape((table_size, d)), shape((4, d, d)), shape((8, d), F32)] + [shape((own, d))] * n
    edge_new, hidden, slope, normed, inverse, table, w_full, gains, *pooled_parts = pl.pallas_call(
        functools.partial(edge_forward_kernel, n, pairs),
        out_shape=tuple(outs + kept),
        grid=(steps,),
        in_specs=[by_rows(d), by_rows(1), by_rows(1), by_columns]
        + [whole_block(x.shape) for x in rest],
        out_specs=tuple([by_rows(d)] * 4 + [by_rows(128)] + [whole_block(x.shape) for x in kept]),
        scratch_shapes=[pltpu.VMEM((nodes, d), F32), pltpu.VMEM((n, 8, portion), F32)],
        compiler_params=edge_params,
        cost_estimate=pl.CostEstimate(
            flops=7 * share * square, bytes_accessed=8 * share * d, transcendentals=share * d
        ),
        name="edge_forward",
    )(*ins, *rest)

    parts = [pooled_parts[0]] + [swap(pooled_parts[b], "feat", b) for b in range(1, n)]
    node_new, pooled_grad, node_base, *messages = call(
        functools.partial(node_kernel, n),
        [node_lat, node_cot, gains, w_node_in, w_node_out, *parts, *w_node],
        [shape((own, d)), shape((own, d)), shape((own, d), F32)]
        + [shape((own, 2 * d + 2 * portion))] * n,
        [pltpu.VMEM((3, d, d), BF16)],
        name="node",
        flops=6 * own * square,
    )
    grad_near = [pooled_grad] + [swap(pooled_grad, "feat", b) for b in range(1, n)]
    messages = [messages[0]] + [swap(messages[b], "feat", b) for b in range(1, n)]

    ins = [edge_lat, edge_cot, hidden, slope, normed, inverse, receiver_at[:, None], sender_at[None], receiver_at[None]]
    rest = [gains, table, w_full, *grad_near]
    kept = [shape((n * 2 * portion + pairs * slots, d))] * 2 + [shape((nodes, d), F32)]
    edge_grad, keep, send, near_grad = pl.pallas_call(
        functools.partial(edge_backward_kernel, n, slots),
        out_shape=tuple([shape((share, d), F32)] + kept),
        grid=(steps,),
        in_specs=[by_rows(d)] * 5 + [by_rows(128), by_rows(1), by_columns, by_columns]
        + [whole_block(x.shape) for x in rest],
        out_specs=tuple([by_rows(d)] + [whole_block(x.shape) for x in kept]),
        scratch_shapes=[
            pltpu.VMEM((nodes, d), BF16),
            pltpu.VMEM((4, d, d), F32),
            pltpu.VMEM((table_size, d), F32),
            pltpu.VMEM((nodes, d), F32),
        ],
        compiler_params=edge_params,
        cost_estimate=pl.CostEstimate(
            flops=10 * share * square, bytes_accessed=16 * share * d, transcendentals=0
        ),
        name="edge_backward",
    )(*ins, *rest)
    got = swap(send, "region", 1)
    node_keep, node_send = call(
        functools.partial(node_weight_kernel, n),
        [*near, *messages],
        [shape((3 * half, d))] * 2,
        [pltpu.VMEM((n, own, portion), BF16), pltpu.VMEM((3 * portion, d), F32)],
        name="node_weights",
        flops=3 * nodes * square // n,
    )
    node_got = swap(node_send, "region", 1)
    outs = call(
        functools.partial(pair_sum_kernel, n, slots),
        [keep, got],
        [shape((4 * half, d))] * n + [shape((2 * slots, d))] * pairs,
        name="pair_sum",
    )
    parts = [outs[0]] + [swap(outs[b], "feat", b) for b in range(1, n)]
    returned = chip_exchange(outs[n:])
    grad_edge_in, grad_edge_out, grad_node_in, grad_node_out = reduce_grads(
        parts,
        [node_keep, node_got],
        portion,
        float((share * n * regions) ** -0.5),
        float((nodes * regions) ** -0.5),
    )

    parts = call(
        functools.partial(return_kernel, n, pairs),
        [near_grad, send_at[None], *returned],
        [shape((own, d))] * n,
        name="give_back",
        flops=2 * regions * slots * nodes * d,
    )
    node_grad = node_base + add_all([parts[0]] + [swap(parts[b], "feat", b) for b in range(1, n)])

    return (
        node_new,
        edge_new,
        node_grad,
        edge_grad,
        grad_edge_in.reshape(w_edge_in.shape),
        grad_edge_out,
        grad_node_in.reshape(w_node_in.shape),
        grad_node_out,
    )


def solution(mesh):
    rows = P(("region", "feat"), None)
    in_specs = (
        rows,
        rows,
        P("region"),
        P("region"),
        P("region", None, None),
        P(None, "feat", None),
        P("feat", None),
        P(None, "feat", None),
        P("feat", None),
        P("feat"),
        P("feat"),
        rows,
        rows,
    )
    out_specs = (
        rows,
        rows,
        rows,
        rows,
        P(None, "feat", None),
        P("feat", None),
        P(None, "feat", None),
        P("feat", None),
    )
    return jax.shard_map(shards, mesh=mesh, in_specs=in_specs, out_specs=out_specs, check_vma=False)
```

```python
import functools

import jax
import jax.numpy as jnp
from jax import lax
from jax.experimental import pallas as pl
from jax.experimental.pallas import tpu as pltpu
from jax.sharding import PartitionSpec as P


EPSILON = 1e-05
F32 = jnp.float32
BF16 = jnp.bfloat16
VMEM_LIMIT = 36 * 1024 * 1024


def dot(a, b):
    return jnp.dot(a, b, preferred_element_type=F32)


def dot_t(a, b):
    return lax.dot_general(a, b, (((1,), (1,)), ((), ())), preferred_element_type=F32)


def t_dot(a, b):
    return lax.dot_general(a, b, (((0,), (0,)), ((), ())), preferred_element_type=F32)


def swap(x, axis, bits):
    n = lax.axis_size(axis)
    return lax.ppermute(x, axis, [(i, i ^ bits) for i in range(n)])


def feat_swaps(parts):
    return [parts[0]] + [swap(parts[b], "feat", b) for b in range(1, len(parts))]


def add_all(parts):
    total = parts[0].astype(F32)
    for part in parts[1:]:
        total = total + part.astype(F32)
    return total


def layer_norm(values):
    breadth = values.shape[1]
    average = jnp.sum(values, axis=1, keepdims=True) / breadth
    variance = jnp.sum(values * values, axis=1, keepdims=True) / breadth - average * average
    inverse = lax.rsqrt(variance + EPSILON)
    return (values - average) * inverse, inverse


def layer_norm_back(scaled, normed, inverse):
    breadth = scaled.shape[1]
    first = jnp.sum(scaled, axis=1, keepdims=True) / breadth
    second = jnp.sum(scaled * normed, axis=1, keepdims=True) / breadth
    return (inverse * (scaled - first - normed * second)).astype(BF16)


def swish_and_slope(values):
    s = 1.0 / (1.0 + jnp.exp(-values))
    return (values * s).astype(BF16), s * (1.0 + values * (1.0 - s))


def hot(column, width):
    at = lax.broadcasted_iota(jnp.int32, (column.shape[0], width), 1)
    return jnp.where(column == at, 1.0, 0.0).astype(BF16)


def hot_t(row, height):
    at = lax.broadcasted_iota(jnp.int32, (height, row.shape[1]), 0)
    return jnp.where(row == at, 1.0, 0.0).astype(BF16)


def tile_of(rows):
    for size in (256, 192, 128, 96, 64, 48, 32, 16):
        if rows % size == 0:
            return size
    return rows


def shape(dims, dtype=BF16):
    return jax.ShapeDtypeStruct(tuple(dims), dtype)


def whole_block(dims):
    return pl.BlockSpec(tuple(dims), lambda *_: (0,) * len(dims))


def call(kernel, ins, outs, scratch=(), flops=0):
    return pl.pallas_call(
        kernel,
        out_shape=tuple(outs),
        grid=(1,),
        in_specs=[whole_block(x.shape) for x in ins],
        out_specs=tuple(whole_block(x.shape) for x in outs),
        scratch_shapes=list(scratch),
        compiler_params=pltpu.CompilerParams(vmem_limit_bytes=VMEM_LIMIT),
        cost_estimate=pl.CostEstimate(
            flops=flops,
            bytes_accessed=sum(x.size * x.dtype.itemsize for x in (*ins, *outs)),
            transcendentals=0,
        ),
    )(*ins)


def fill_weights(w_ref, own_in, own_out, pieces, parity, here):
    m = w_ref.shape[0]
    portion = own_out.shape[0]
    half = portion // 2
    at = pl.multiple_of(here * portion, half)
    for k in range(m):
        w_ref[k, pl.ds(at, portion), :] = own_in[k] if k < m - 1 else own_out[...]
    for b, (got, other) in enumerate(pieces, start=1):
        start = (here ^ b) * portion
        first = pl.multiple_of(start + parity * half, half)
        second = pl.multiple_of(start + (1 - parity) * half, half)
        for k in range(m):
            w_ref[k, pl.ds(first, half), :] = got[k * half : (k + 1) * half, :]
            w_ref[k, pl.ds(second, half), :] = other[k * half : (k + 1) * half, :]


def split_grads(grads, n, keep, send, parity, here):
    m = grads.shape[0]
    portion = grads.shape[1] // n
    half = portion // 2
    block = m * half
    for side in range(2):

        @pl.when(parity == side)
        def _():
            for f in range(n):
                for u in range(2 * m):
                    out = keep if u // m == side else send
                    at = f * portion + (u % 2) * half
                    start = pl.multiple_of((f ^ here) * block + (u % m) * half, half)
                    out[pl.ds(start, half), :] = grads[u // 2, at : at + half, :].astype(BF16)


def pack_kernel(inner, outer, *refs):
    gains, pack, sems = refs[:-2], refs[-2], refs[-1]
    half = outer.shape[0] // 2
    m = inner.shape[0] + 1
    at = pl.multiple_of(lax.axis_index("region") % 2 * half, half)
    copies = []
    for k in range(m):
        source = inner.at[k, pl.ds(at, half)] if k < m - 1 else outer.at[pl.ds(at, half)]
        copies.append(pltpu.make_async_copy(source, pack.at[pl.ds(k * half, half)], sems.at[k]))
        copies[-1].start()
    if gains:
        parts = []
        for gain in gains:
            left = gain[...]
            for _ in range(3):
                part = left.astype(BF16)
                left = left - part.astype(F32)
                parts.append(part.astype(F32))
        parts.append(jnp.zeros((16 - len(parts), left.shape[1]), F32))
        pack[m * half :, :] = jnp.zeros((16, pack.shape[1]), BF16)
        pack[m * half :, : left.shape[1]] = jnp.concatenate(parts, axis=0).astype(BF16)
    for copy in copies:
        copy.wait()


def pack_halves(inner, outer, gains):
    m, d = inner.shape[0] + 1, inner.shape[2]
    rows = m * (outer.shape[0] // 2) + (16 if gains else 0)
    return pl.pallas_call(
        pack_kernel,
        out_shape=shape((rows, d)),
        grid=(1,),
        in_specs=[pl.BlockSpec(memory_space=pltpu.HBM)] * 2 + [whole_block(x.shape) for x in gains],
        out_specs=whole_block((rows, d)),
        scratch_shapes=[pltpu.SemaphoreType.DMA((m,))],
        compiler_params=pltpu.CompilerParams(vmem_limit_bytes=VMEM_LIMIT),
        cost_estimate=pl.CostEstimate(flops=rows * d, bytes_accessed=4 * rows * d, transcendentals=0),
    )(inner, outer, *gains)


def fill_gains(gain_ref, blocks, own, pieces, here):
    portion = blocks.shape[2]
    blocks[here, 0:1, :] = own[0][...]
    blocks[here, 1:2, :] = own[1][...]
    for b, (got, _) in enumerate(pieces, start=1):
        parts = got[got.shape[0] - 16 :, :portion].astype(F32)
        blocks[here ^ b, 0:1, :] = parts[0:1] + parts[1:2] + parts[2:3]
        blocks[here ^ b, 1:2, :] = parts[3:4] + parts[4:5] + parts[5:6]
    for f in range(blocks.shape[0]):
        gain_ref[0:2, f * portion : (f + 1) * portion] = blocks[f, 0:2, :]


def outgoing_kernel(n, at_ref, *refs):
    near, (keep, send) = refs[:n], refs[n : n + 2]
    own = near[0].shape[0]
    rows = jnp.zeros((at_ref.shape[0], near[0].shape[1]), F32)
    for b in range(n):
        rows = rows + dot(hot(at_ref[...] - b * own, own), near[b][...])
    rows = rows.astype(BF16)
    pairs, slots, _ = keep.shape
    for b in range(pairs):
        keep[b] = rows[(2 * b) * slots : (2 * b + 1) * slots]
        send[b] = rows[(2 * b + 1) * slots : (2 * b + 2) * slots]


def edge_forward_kernel(n, pairs, *refs):
    edge, s_at, r_at, r_row, edge_gain, node_gain, own_in, own_out = refs[:8]
    refs = refs[8:]
    tables, refs = refs[: n + pairs], refs[n + pairs :]
    pieces = [(refs[2 * b], refs[2 * b + 1]) for b in range(n - 1)]
    refs = refs[2 * (n - 1) :]
    new, hidden_ref, slope_ref, normed_ref, inverse_ref, table, w, gains = refs[:8]
    pooled, total, blocks = refs[8 : 8 + n], refs[8 + n], refs[9 + n]
    here = lax.axis_index("feat")
    parity = lax.axis_index("region") % 2
    own = tables[0].shape[0]
    nodes = own * n

    @pl.when(pl.program_id(0) == 0)
    def _():
        at = 0
        for piece in tables:
            table[at : at + piece.shape[0], :] = piece[...]
            at += piece.shape[0]
        fill_weights(w, own_in, own_out, pieces, parity, here)
        fill_gains(gains, blocks, (edge_gain, node_gain), pieces, here)
        total[...] = jnp.zeros_like(total)

    lat = edge[...]
    senders = dot(hot(s_at[...], table.shape[0]), table[...]).astype(BF16)
    receivers = dot(hot(r_at[...], nodes), table[:nodes, :]).astype(BF16)
    pre = dot(lat, w[0]) + dot(senders, w[1]) + dot(receivers, w[2])
    hidden, slope = swish_and_slope(pre)
    hidden_ref[...] = hidden
    slope_ref[...] = slope.astype(BF16)
    normed, inverse = layer_norm(dot(hidden, w[3]))
    normed_ref[...] = normed.astype(BF16)
    inverse_ref[...] = jnp.broadcast_to(inverse, inverse_ref.shape)
    updated = (lat.astype(F32) + normed * gains[0:1, :]).astype(BF16)
    new[...] = updated
    total[...] += dot(hot_t(r_row[...], nodes), updated)

    @pl.when(pl.program_id(0) == pl.num_programs(0) - 1)
    def _():
        for b in range(n):
            pooled[b][...] = total[b * own : (b + 1) * own, :].astype(BF16)


def node_kernel(n, lat_ref, cot_ref, gains, own_in, own_out, *refs):
    parts, refs = refs[:n], refs[n:]
    pieces = [(refs[2 * b], refs[2 * b + 1]) for b in range(n - 1)]
    refs = refs[2 * (n - 1) :]
    new, pooled_grad, base = refs[:3]
    messages, w = refs[3 : 3 + n], refs[3 + n]
    here = lax.axis_index("feat")
    parity = lax.axis_index("region") % 2
    gain = gains[1:2, :]
    fill_weights(w, own_in, own_out, pieces, parity, here)
    pooled = add_all([part[...] for part in parts]).astype(BF16)
    lat = lat_ref[...]
    pre = dot(lat, w[0]) + dot(pooled, w[1])
    hidden, slope = swish_and_slope(pre)
    normed, inverse = layer_norm(dot(hidden, w[2]))
    new[...] = (lat.astype(F32) + normed * gain).astype(BF16)
    cot = cot_ref[...].astype(F32)
    mix_grad = layer_norm_back(cot * gain, normed, inverse)
    pre_grad = (dot_t(mix_grad, w[2]) * slope).astype(BF16)
    pooled_grad[...] = dot_t(pre_grad, w[1]).astype(BF16)
    base[...] = cot + dot_t(pre_grad, w[0])
    d = lat.shape[1]
    portion = d // n
    for b in range(n):
        messages[b][:, :d] = pre_grad
        messages[b][:, d : 2 * d] = mix_grad
    for f in range(n):

        @pl.when(here == f)
        def _():
            for b in range(n):
                block = slice((f ^ b) * portion, ((f ^ b) + 1) * portion)
                messages[b][:, 2 * d : 2 * d + portion] = pooled[:, block]
                messages[b][:, 2 * d + portion :] = hidden[:, block]


def node_weight_kernel(n, *refs):
    near, messages, (keep, send, lat, grads) = refs[:n], refs[n : 2 * n], refs[2 * n :]
    here = lax.axis_index("feat")
    parity = lax.axis_index("region") % 2
    _, d = near[0].shape
    portion = d // n
    for f in range(n):

        @pl.when(here == f)
        def _():
            for b in range(n):
                lat[b] = near[b][:, f * portion : (f + 1) * portion]

    totals = [jnp.zeros((portion, d), F32)] * 3
    for b in range(n):
        pre_grad = messages[b][:, :d]
        mix_grad = messages[b][:, d : 2 * d]
        totals[0] = totals[0] + t_dot(lat[b], pre_grad)
        totals[1] = totals[1] + t_dot(messages[b][:, 2 * d : 2 * d + portion], pre_grad)
        totals[2] = totals[2] + t_dot(messages[b][:, 2 * d + portion :], mix_grad)
    for k in range(3):
        grads[k * portion : (k + 1) * portion, :] = totals[k]
    half = keep.shape[0]
    keep[...] = grads[pl.ds(pl.multiple_of(parity * half, 16), half), :].astype(BF16)
    send[...] = grads[pl.ds(pl.multiple_of((1 - parity) * half, 16), half), :].astype(BF16)


def edge_backward_kernel(n, slots, *refs):
    edge, cot, hidden, slope, normed, inverse, r_at, s_row, r_row, gains, table, w = refs[:12]
    near, refs = refs[12 : 12 + n], refs[12 + n :]
    edge_grad, keep, send, near_grad = refs[:4]
    near_all, grads, sent, received = refs[4:]
    here = lax.axis_index("feat")
    parity = lax.axis_index("region") % 2
    own = near[0].shape[0]
    nodes = own * n

    @pl.when(pl.program_id(0) == 0)
    def _():
        for b in range(n):
            near_all[b * own : (b + 1) * own, :] = near[b][...]
        grads[...] = jnp.zeros_like(grads)
        sent[...] = jnp.zeros_like(sent)
        received[...] = jnp.zeros_like(received)

    total = cot[...].astype(F32) + dot(hot(r_at[...], nodes), near_all[...])
    mix_grad = layer_norm_back(total * gains[0:1, :], normed[...].astype(F32), inverse[:, :1])
    pre_grad = (dot_t(mix_grad, w[3]) * slope[...].astype(F32)).astype(BF16)
    edge_grad[...] = total + dot_t(pre_grad, w[0])
    grads[0] += t_dot(edge[...], pre_grad)
    grads[3] += t_dot(hidden[...], mix_grad)
    sent[...] += dot(hot_t(s_row[...], table.shape[0]), pre_grad)
    received[...] += dot(hot_t(r_row[...], nodes), pre_grad)

    @pl.when(pl.program_id(0) == pl.num_programs(0) - 1)
    def _():
        from_senders = sent[...].astype(BF16)
        from_receivers = received[...].astype(BF16)
        grads[1] = t_dot(table[...], from_senders)
        grads[2] = t_dot(table[:nodes, :], from_receivers)
        split_grads(grads, n, keep, send, parity, here)
        to_table = dot_t(from_senders, w[1])
        near_grad[...] = to_table[:nodes] + dot_t(from_receivers, w[2])
        back = to_table[nodes:].astype(BF16)
        at = n * grads.shape[0] * (grads.shape[1] // n // 2)
        count = (keep.shape[0] - at) // slots
        for b in range(count):
            rows = slice(at + b * slots, at + (b + 1) * slots)
            keep[rows, :] = back[(2 * b) * slots : (2 * b + 1) * slots]
            send[rows, :] = back[(2 * b + 1) * slots : (2 * b + 2) * slots]


def return_kernel(n, pairs, near_grad, at_row, *refs):
    blocks, outs = refs[:pairs], refs[pairs:]
    nodes, _ = near_grad.shape
    own = nodes // n
    rows = blocks[0].shape[0]
    total = near_grad[...]
    for b in range(pairs):
        total = total + dot(hot_t(at_row[:, b * rows : (b + 1) * rows], nodes), blocks[b][...])
    for b in range(n):
        outs[b][...] = total[b * own : (b + 1) * own, :].astype(BF16)


def pair_sum_kernel(n, slots, keep, got, *outs):
    block = outs[0].shape[0]
    for b in range(n):
        rows = slice(b * block, (b + 1) * block)
        outs[b][...] = (keep[rows, :].astype(F32) + got[rows, :].astype(F32)).astype(BF16)
    for b, out in enumerate(outs[n:]):
        rows = slice(n * block + b * slots, n * block + (b + 1) * slots)
        out[:slots, :] = keep[rows, :]
        out[slots:, :] = got[rows, :]


def scatter_sum_kernel(n, pairs, *refs):
    parts, node_parts = refs[:n], refs[n : n + 2]
    outs, total = refs[n + 2 : n + 2 + pairs], refs[n + 2 + pairs]
    z = lax.axis_index("region") // 2
    cut = parts[0].shape[0]
    total[:cut, :] = add_all([part[...] for part in parts])
    total[cut:, :] = add_all([part[...] for part in node_parts])
    rows = outs[0].shape[0]
    for b in range(pairs):
        outs[b][...] = total[pl.ds(pl.multiple_of((z ^ b) * rows, rows), rows), :].astype(BF16)


def sum_kernel(*refs):
    refs[-1][...] = add_all([part[...] for part in refs[:-1]]).astype(BF16)


def finish_kernel(pairs, edge_norm, node_norm, *refs):
    mine, theirs = refs[:pairs], refs[pairs : 2 * pairs]
    outs, total = refs[2 * pairs : -1], refs[-1]
    region = lax.axis_index("region")
    parity, z = region % 2, region // 2
    rows = mine[0].shape[0]
    for b in range(pairs):
        at = (z ^ b) * rows
        for side, ref in ((parity, mine[b]), (1 - parity, theirs[b])):
            start = pl.multiple_of(side * pairs * rows + at, rows)
            total[pl.ds(start, rows), :] = ref[...].astype(F32)
    spread(total, outs, edge_norm, node_norm)


def spread(total, outs, edge_norm, node_norm):
    portion = outs[1].shape[0]
    size = total.shape[0] // 2
    for norm, m, at, pair in ((edge_norm, 4, 0, outs[:2]), (node_norm, 3, 2 * portion, outs[2:])):
        half = m * portion // 2
        for u in range(2 * m):
            row = u * (portion // 2)
            source = (row // half) * size + at + row % half
            out, start = (pair[0], row) if u < 2 * m - 2 else (pair[1], row - (m - 1) * portion)
            out[start : start + portion // 2, :] = total[source : source + portion // 2, :] * norm


def gather_halves(mine):
    pieces = []
    for b in range(1, lax.axis_size("feat")):
        got = swap(mine, "feat", b)
        pieces += [got, swap(got, "region", 1)]
    return pieces


def chip_exchange(blocks):
    return [blocks[0]] + [swap(blocks[b], "region", 2 * b) for b in range(1, len(blocks))]


def reduce_grads(parts, node_parts, portion, edge_norm, node_norm):
    n = len(parts)
    half, d = parts[0].shape
    pairs = lax.axis_size("region") // 2
    z = lax.axis_index("region") // 2
    parity = lax.axis_index("region") % 2
    size = half + node_parts[0].shape[0]
    rows = size // pairs
    outs = [shape((k * portion, d), F32) for k in (3, 1, 2, 1)]
    if rows % 16 == 0:
        parts = call(
            functools.partial(scatter_sum_kernel, n, pairs),
            [*parts, *node_parts],
            [shape((rows, d))] * pairs,
            [pltpu.VMEM((size, d), F32)],
        )
    else:
        mine = jnp.concatenate([add_all(parts), add_all(node_parts)]).astype(BF16).reshape(pairs, rows, d)
        parts = [lax.dynamic_index_in_dim(mine, z ^ b, 0, keepdims=False) for b in range(pairs)]
    parts = chip_exchange(parts)
    if rows % 16 == 0:
        (chunk,) = call(sum_kernel, parts, [shape((rows, d))])
    else:
        chunk = add_all(parts).astype(BF16)
    mine = chip_exchange([chunk] * pairs)
    theirs = [swap(piece, "region", 1) for piece in mine]
    if rows % 16 == 0:
        return call(
            functools.partial(finish_kernel, pairs, edge_norm, node_norm),
            mine + theirs,
            outs,
            [pltpu.VMEM((2 * size, d), F32)],
        )
    order = jnp.arange(pairs) ^ z
    sides = [jnp.stack(side)[order].reshape(size, d) for side in (mine, theirs)]
    total = jnp.where(parity == 0, jnp.concatenate(sides), jnp.concatenate(sides[::-1])).astype(F32)

    def from_total(*refs):
        spread(refs[0], refs[1:], edge_norm, node_norm)

    return call(from_total, [total], outs)


def layer(
    node_lat,
    edge_lat,
    receiver_row,
    sender_slot,
    send_rows,
    w_edge_in,
    w_edge_out,
    w_node_in,
    w_node_out,
    edge_gain,
    node_gain,
    node_cot,
    edge_cot,
):
    n = lax.axis_size("feat")
    regions = lax.axis_size("region")
    pairs = regions // 2
    here = lax.axis_index("feat")
    region = lax.axis_index("region")
    own, d = node_lat.shape
    nodes = own * n
    share = edge_lat.shape[0]
    slots = send_rows.shape[2]
    table_size = nodes + regions * slots

    def relative(row):
        return ((row // own) ^ here) * own + row % own

    local_receivers = lax.dynamic_slice_in_dim(receiver_row, here * share, share)
    local_senders = lax.dynamic_slice_in_dim(sender_slot, here * share, share)
    remote = jnp.maximum(local_senders - nodes, 0)
    sender_at = jnp.where(
        local_senders < nodes,
        relative(local_senders),
        nodes + ((remote // slots) ^ region) * slots + remote % slots,
    )
    receiver_at = relative(local_receivers)
    send_at = relative(send_rows[0])[jnp.arange(regions) ^ region].reshape(-1)

    portion = d // n
    half = portion // 2
    gain_rows = [edge_gain[None], node_gain[None]]
    near = feat_swaps([node_lat] * n)
    edge_pack = pack_halves(w_edge_in, w_edge_out, gain_rows)
    node_pack = pack_halves(w_node_in, w_node_out, [])
    w_edge = gather_halves(edge_pack)

    square = 2 * d * d
    keep, send = call(
        functools.partial(outgoing_kernel, n),
        [send_at[:, None], *near],
        [shape((pairs, slots, d))] * 2,
        flops=2 * regions * slots * nodes * d,
    )
    other = swap(send, "region", 1)
    remote_rows = chip_exchange([jnp.concatenate([keep[b], other[b]], axis=0) for b in range(pairs)])
    w_node = gather_halves(node_pack)

    tile = tile_of(share)
    steps = share // tile
    by_rows = lambda width: pl.BlockSpec((tile, width), lambda i: (i, 0))
    by_columns = pl.BlockSpec((1, tile), lambda i: (0, i))
    edge_params = pltpu.CompilerParams(
        dimension_semantics=("arbitrary",), vmem_limit_bytes=VMEM_LIMIT
    )
    ins = [edge_lat, sender_at[:, None], receiver_at[:, None], receiver_at[None]]
    rest = [*gain_rows, w_edge_in, w_edge_out, *near, *remote_rows, *w_edge]
    outs = [shape((share, d))] * 4 + [shape((share, 128), F32)]
    kept = [shape((table_size, d)), shape((4, d, d)), shape((8, d), F32)] + [shape((own, d))] * n
    edge_new, hidden, slope, normed, inverse, table, w_full, gains, *pooled_parts = pl.pallas_call(
        functools.partial(edge_forward_kernel, n, pairs),
        out_shape=tuple(outs + kept),
        grid=(steps,),
        in_specs=[by_rows(d), by_rows(1), by_rows(1), by_columns]
        + [whole_block(x.shape) for x in rest],
        out_specs=tuple([by_rows(d)] * 4 + [by_rows(128)] + [whole_block(x.shape) for x in kept]),
        scratch_shapes=[pltpu.VMEM((nodes, d), F32), pltpu.VMEM((n, 8, portion), F32)],
        compiler_params=edge_params,
        cost_estimate=pl.CostEstimate(
            flops=7 * share * square, bytes_accessed=8 * share * d, transcendentals=share * d
        ),
        name="edge_forward",
    )(*ins, *rest)

    parts = feat_swaps(pooled_parts)
    node_new, pooled_grad, node_base, *messages = call(
        functools.partial(node_kernel, n),
        [node_lat, node_cot, gains, w_node_in, w_node_out, *parts, *w_node],
        [shape((own, d)), shape((own, d)), shape((own, d), F32)]
        + [shape((own, 2 * d + 2 * portion))] * n,
        [pltpu.VMEM((3, d, d), BF16)],
        flops=6 * own * square,
    )
    grad_near = feat_swaps([pooled_grad] * n)
    messages = feat_swaps(messages)

    ins = [edge_lat, edge_cot, hidden, slope, normed, inverse, receiver_at[:, None], sender_at[None], receiver_at[None]]
    rest = [gains, table, w_full, *grad_near]
    kept = [shape((n * 2 * portion + pairs * slots, d))] * 2 + [shape((nodes, d), F32)]
    edge_grad, keep, send, near_grad = pl.pallas_call(
        functools.partial(edge_backward_kernel, n, slots),
        out_shape=tuple([shape((share, d), F32)] + kept),
        grid=(steps,),
        in_specs=[by_rows(d)] * 5 + [by_rows(128), by_rows(1), by_columns, by_columns]
        + [whole_block(x.shape) for x in rest],
        out_specs=tuple([by_rows(d)] + [whole_block(x.shape) for x in kept]),
        scratch_shapes=[
            pltpu.VMEM((nodes, d), BF16),
            pltpu.VMEM((4, d, d), F32),
            pltpu.VMEM((table_size, d), F32),
            pltpu.VMEM((nodes, d), F32),
        ],
        compiler_params=edge_params,
        cost_estimate=pl.CostEstimate(
            flops=10 * share * square, bytes_accessed=16 * share * d, transcendentals=0
        ),
        name="edge_backward",
    )(*ins, *rest)
    got = swap(send, "region", 1)
    node_keep, node_send = call(
        functools.partial(node_weight_kernel, n),
        [*near, *messages],
        [shape((3 * half, d))] * 2,
        [pltpu.VMEM((n, own, portion), BF16), pltpu.VMEM((3 * portion, d), F32)],
        flops=3 * nodes * square // n,
    )
    node_got = swap(node_send, "region", 1)
    outs = call(
        functools.partial(pair_sum_kernel, n, slots),
        [keep, got],
        [shape((4 * half, d))] * n + [shape((2 * slots, d))] * pairs,
    )
    parts = feat_swaps(outs[:n])
    returned = chip_exchange(outs[n:])
    grad_edge_in, grad_edge_out, grad_node_in, grad_node_out = reduce_grads(
        parts,
        [node_keep, node_got],
        portion,
        float((share * n * regions) ** -0.5),
        float((nodes * regions) ** -0.5),
    )

    parts = call(
        functools.partial(return_kernel, n, pairs),
        [near_grad, send_at[None], *returned],
        [shape((own, d))] * n,
        flops=2 * regions * slots * nodes * d,
    )
    node_grad = node_base + add_all(feat_swaps(parts))

    return (
        node_new,
        edge_new,
        node_grad,
        edge_grad,
        grad_edge_in.reshape(w_edge_in.shape),
        grad_edge_out,
        grad_node_in.reshape(w_node_in.shape),
        grad_node_out,
    )


def solution(mesh):
    rows = P(("region", "feat"), None)
    in_specs = (
        rows,
        rows,
        P("region"),
        P("region"),
        P("region", None, None),
        P(None, "feat", None),
        P("feat", None),
        P(None, "feat", None),
        P("feat", None),
        P("feat"),
        P("feat"),
        rows,
        rows,
    )
    out_specs = (
        rows,
        rows,
        rows,
        rows,
        P(None, "feat", None),
        P("feat", None),
        P(None, "feat", None),
        P("feat", None),
    )
    return jax.shard_map(layer, mesh=mesh, in_specs=in_specs, out_specs=out_specs, check_vma=False)
```

```python
import functools

import jax
import jax.numpy as jnp
from jax import lax
from jax.experimental import pallas as pl
from jax.experimental.pallas import tpu as pltpu
from jax.sharding import PartitionSpec as P


EPSILON = 1e-05
F32 = jnp.float32
BF16 = jnp.bfloat16
VMEM_LIMIT = 36 * 1024 * 1024


def dot(a, b):
    return jnp.dot(a, b, preferred_element_type=F32)


def dot_t(a, b):
    return lax.dot_general(a, b, (((1,), (1,)), ((), ())), preferred_element_type=F32)


def t_dot(a, b):
    return lax.dot_general(a, b, (((0,), (0,)), ((), ())), preferred_element_type=F32)


def swap(x, axis, bits):
    n = lax.axis_size(axis)
    return lax.ppermute(x, axis, [(i, i ^ bits) for i in range(n)])


def feat_swaps(parts):
    return [parts[0]] + [swap(parts[b], "feat", b) for b in range(1, len(parts))]


def add_all(parts):
    total = parts[0].astype(F32)
    for part in parts[1:]:
        total = total + part.astype(F32)
    return total


def layer_norm(values):
    breadth = values.shape[1]
    average = jnp.sum(values, axis=1, keepdims=True) / breadth
    variance = jnp.sum(values * values, axis=1, keepdims=True) / breadth - average * average
    inverse = lax.rsqrt(variance + EPSILON)
    return (values - average) * inverse, inverse


def layer_norm_back(scaled, normed, inverse):
    breadth = scaled.shape[1]
    first = jnp.sum(scaled, axis=1, keepdims=True) / breadth
    second = jnp.sum(scaled * normed, axis=1, keepdims=True) / breadth
    return (inverse * (scaled - first - normed * second)).astype(BF16)


def swish_and_slope(values):
    s = 0.5 * jnp.tanh(0.5 * values) + 0.5
    return (values * s).astype(BF16), s * (1.0 + values * (1.0 - s))


def hot(column, width):
    at = lax.broadcasted_iota(jnp.int32, (column.shape[0], width), 1)
    return jnp.where(column == at, 1.0, 0.0).astype(BF16)


def hot_t(row, height):
    at = lax.broadcasted_iota(jnp.int32, (height, row.shape[1]), 0)
    return jnp.where(row == at, 1.0, 0.0).astype(BF16)


def tile_of(rows):
    for size in (256, 192, 128, 96, 64, 48, 32, 16):
        if rows % size == 0:
            return size
    return rows


def shape(dims, dtype=BF16):
    return jax.ShapeDtypeStruct(tuple(dims), dtype)


def whole_block(dims):
    return pl.BlockSpec(tuple(dims), lambda *_: (0,) * len(dims))


def call(kernel, ins, outs, scratch=(), flops=0):
    return pl.pallas_call(
        kernel,
        out_shape=tuple(outs),
        grid=(1,),
        in_specs=[whole_block(x.shape) for x in ins],
        out_specs=tuple(whole_block(x.shape) for x in outs),
        scratch_shapes=list(scratch),
        compiler_params=pltpu.CompilerParams(vmem_limit_bytes=VMEM_LIMIT),
        cost_estimate=pl.CostEstimate(
            flops=flops,
            bytes_accessed=sum(x.size * x.dtype.itemsize for x in (*ins, *outs)),
            transcendentals=0,
        ),
    )(*ins)


def fill_weights(w_ref, own_in, own_out, pieces, parity, here):
    m = w_ref.shape[0]
    portion = own_out.shape[0]
    half = portion // 2
    at = pl.multiple_of(here * portion, half)
    for k in range(m):
        w_ref[k, pl.ds(at, portion), :] = own_in[k] if k < m - 1 else own_out[...]
    for b, (got, other) in enumerate(pieces, start=1):
        start = (here ^ b) * portion
        first = pl.multiple_of(start + parity * half, half)
        second = pl.multiple_of(start + (1 - parity) * half, half)
        for k in range(m):
            w_ref[k, pl.ds(first, half), :] = got[k * half : (k + 1) * half, :]
            w_ref[k, pl.ds(second, half), :] = other[k * half : (k + 1) * half, :]


def split_grads(grads, n, keep, send, parity, here):
    m = grads.shape[0]
    portion = grads.shape[1] // n
    half = portion // 2
    block = m * half
    for side in range(2):

        @pl.when(parity == side)
        def _():
            for f in range(n):
                for u in range(2 * m):
                    out = keep if u // m == side else send
                    at = f * portion + (u % 2) * half
                    start = pl.multiple_of((f ^ here) * block + (u % m) * half, half)
                    out[pl.ds(start, half), :] = grads[u // 2, at : at + half, :].astype(BF16)


def pack_kernel(inner, outer, *refs):
    m = inner.shape[0] + 1
    half = outer.shape[0] // 2
    count = (len(refs) - 2) // 2
    gains, pack, sems, held = refs[:count], refs[count], refs[count + 1], refs[count + 2 :]
    at = pl.multiple_of(lax.axis_index("region") % 2 * half, half)
    copies = [pltpu.make_async_copy(gain, ref, sems.at[m + k]) for k, (gain, ref) in enumerate(zip(gains, held))]
    for k in range(m):
        source = inner.at[k, pl.ds(at, half)] if k < m - 1 else outer.at[pl.ds(at, half)]
        copies.append(pltpu.make_async_copy(source, pack.at[pl.ds(k * half, half)], sems.at[k]))
    for copy in copies:
        copy.start()
    for copy in copies:
        copy.wait()
    if gains:
        parts = []
        for ref in held:
            left = ref[...]
            for _ in range(3):
                part = left.astype(BF16)
                left = left - part.astype(F32)
                parts.append(part.astype(F32))
        parts.append(jnp.zeros((16 - len(parts), left.shape[1]), F32))
        pack[m * half :, :] = jnp.zeros((16, pack.shape[1]), BF16)
        pack[m * half :, : left.shape[1]] = jnp.concatenate(parts, axis=0).astype(BF16)


def pack_halves(inner, outer, gains):
    m, d = inner.shape[0] + 1, inner.shape[2]
    rows = m * (outer.shape[0] // 2) + (16 if gains else 0)
    ins = [pltpu.with_memory_space_constraint(x, pltpu.HBM) for x in (inner, outer, *gains)]
    return pl.pallas_call(
        pack_kernel,
        out_shape=shape((rows, d)),
        grid=(1,),
        in_specs=[pl.BlockSpec(memory_space=pltpu.HBM)] * len(ins),
        out_specs=whole_block((rows, d)),
        scratch_shapes=[pltpu.SemaphoreType.DMA((m + len(gains),))] + [pltpu.VMEM(x.shape, F32) for x in gains],
        compiler_params=pltpu.CompilerParams(vmem_limit_bytes=VMEM_LIMIT),
        cost_estimate=pl.CostEstimate(flops=rows * d, bytes_accessed=4 * rows * d, transcendentals=0),
    )(*ins)


def fill_gains(gain_ref, blocks, own, pieces, here):
    portion = blocks.shape[2]
    blocks[here, 0:1, :] = own[0][...]
    blocks[here, 1:2, :] = own[1][...]
    for b, (got, _) in enumerate(pieces, start=1):
        parts = got[got.shape[0] - 16 :, :portion].astype(F32)
        blocks[here ^ b, 0:1, :] = parts[0:1] + parts[1:2] + parts[2:3]
        blocks[here ^ b, 1:2, :] = parts[3:4] + parts[4:5] + parts[5:6]
    for f in range(blocks.shape[0]):
        gain_ref[0:2, f * portion : (f + 1) * portion] = blocks[f, 0:2, :]


def outgoing_kernel(n, rows_ref, *refs):
    near, (keep, send, at_ref) = refs[:n], refs[n:]
    own = near[0].shape[0]
    here = lax.axis_index("feat")
    region = lax.axis_index("region")
    regions, slots = rows_ref.shape
    for b in range(regions):
        row = rows_ref[pl.ds(region ^ b, 1), :]
        feat = jnp.zeros_like(row)
        for k in range(1, n):
            feat = feat + jnp.where(row >= k * own, 1, 0)
        at_ref[0:1, b * slots : (b + 1) * slots] = (feat ^ here) * own + row - feat * own
    at = at_ref[0:1, :]
    rows = jnp.zeros((at.shape[1], near[0].shape[1]), F32)
    for b in range(n):
        rows = rows + t_dot(hot_t(at - b * own, own), near[b][...])
    rows = rows.astype(BF16)
    pairs, slots, _ = keep.shape
    for b in range(pairs):
        keep[b] = rows[(2 * b) * slots : (2 * b + 1) * slots]
        send[b] = rows[(2 * b + 1) * slots : (2 * b + 2) * slots]


def join_kernel(keep, other, *outs):
    slots = keep.shape[1]
    for b, out in enumerate(outs):
        out[:slots, :] = keep[b]
        out[slots:, :] = other[b]


def edge_forward_kernel(n, pairs, *refs):
    edge, s_at, r_at, r_row, edge_gain, node_gain, own_in, own_out = refs[:8]
    refs = refs[8:]
    tables, refs = refs[: n + pairs], refs[n + pairs :]
    pieces = [(refs[2 * b], refs[2 * b + 1]) for b in range(n - 1)]
    refs = refs[2 * (n - 1) :]
    new, hidden_ref, slope_ref, normed_ref, inverse_ref, table, w, gains = refs[:8]
    pooled, total, blocks = refs[8 : 8 + n], refs[8 + n], refs[9 + n]
    here = lax.axis_index("feat")
    parity = lax.axis_index("region") % 2
    own = tables[0].shape[0]
    nodes = own * n

    @pl.when(pl.program_id(0) == 0)
    def _():
        at = 0
        for piece in tables:
            table[at : at + piece.shape[0], :] = piece[...]
            at += piece.shape[0]
        fill_weights(w, own_in, own_out, pieces, parity, here)
        fill_gains(gains, blocks, (edge_gain, node_gain), pieces, here)
        total[...] = jnp.zeros_like(total)

    lat = edge[...]
    senders = dot(hot(s_at[...], table.shape[0]), table[...]).astype(BF16)
    receivers = dot(hot(r_at[...], nodes), table[:nodes, :]).astype(BF16)
    pre = dot(lat, w[0]) + dot(senders, w[1]) + dot(receivers, w[2])
    hidden, slope = swish_and_slope(pre)
    hidden_ref[...] = hidden
    slope_ref[...] = slope.astype(BF16)
    normed, inverse = layer_norm(dot(hidden, w[3]))
    normed_ref[...] = normed.astype(BF16)
    inverse_ref[...] = jnp.broadcast_to(inverse, inverse_ref.shape)
    updated = (lat.astype(F32) + normed * gains[0:1, :]).astype(BF16)
    new[...] = updated
    total[...] += dot(hot_t(r_row[...], nodes), updated)

    @pl.when(pl.program_id(0) == pl.num_programs(0) - 1)
    def _():
        for b in range(n):
            pooled[b][...] = total[b * own : (b + 1) * own, :].astype(BF16)


def node_kernel(n, lat_ref, cot_ref, gains, own_in, own_out, *refs):
    parts, refs = refs[:n], refs[n:]
    pieces = [(refs[2 * b], refs[2 * b + 1]) for b in range(n - 1)]
    refs = refs[2 * (n - 1) :]
    new, pooled_grad, base = refs[:3]
    messages, w = refs[3 : 3 + n], refs[3 + n]
    here = lax.axis_index("feat")
    parity = lax.axis_index("region") % 2
    gain = gains[1:2, :]
    fill_weights(w, own_in, own_out, pieces, parity, here)
    pooled = add_all([part[...] for part in parts]).astype(BF16)
    lat = lat_ref[...]
    pre = dot(lat, w[0]) + dot(pooled, w[1])
    hidden, slope = swish_and_slope(pre)
    normed, inverse = layer_norm(dot(hidden, w[2]))
    new[...] = (lat.astype(F32) + normed * gain).astype(BF16)
    cot = cot_ref[...].astype(F32)
    mix_grad = layer_norm_back(cot * gain, normed, inverse)
    pre_grad = (dot_t(mix_grad, w[2]) * slope).astype(BF16)
    pooled_grad[...] = dot_t(pre_grad, w[1]).astype(BF16)
    base[...] = cot + dot_t(pre_grad, w[0])
    d = lat.shape[1]
    portion = d // n
    for b in range(n):
        messages[b][:, :d] = pre_grad
        messages[b][:, d : 2 * d] = mix_grad
    for f in range(n):

        @pl.when(here == f)
        def _():
            for b in range(n):
                block = slice((f ^ b) * portion, ((f ^ b) + 1) * portion)
                messages[b][:, 2 * d : 2 * d + portion] = pooled[:, block]
                messages[b][:, 2 * d + portion :] = hidden[:, block]


def node_weight_kernel(n, *refs):
    near, messages, (keep, send, lat, grads) = refs[:n], refs[n : 2 * n], refs[2 * n :]
    here = lax.axis_index("feat")
    parity = lax.axis_index("region") % 2
    _, d = near[0].shape
    portion = d // n
    for f in range(n):

        @pl.when(here == f)
        def _():
            for b in range(n):
                lat[b] = near[b][:, f * portion : (f + 1) * portion]

    totals = [jnp.zeros((portion, d), F32)] * 3
    for b in range(n):
        pre_grad = messages[b][:, :d]
        mix_grad = messages[b][:, d : 2 * d]
        totals[0] = totals[0] + t_dot(lat[b], pre_grad)
        totals[1] = totals[1] + t_dot(messages[b][:, 2 * d : 2 * d + portion], pre_grad)
        totals[2] = totals[2] + t_dot(messages[b][:, 2 * d + portion :], mix_grad)
    for k in range(3):
        grads[k * portion : (k + 1) * portion, :] = totals[k]
    half = keep.shape[0]
    keep[...] = grads[pl.ds(pl.multiple_of(parity * half, 16), half), :].astype(BF16)
    send[...] = grads[pl.ds(pl.multiple_of((1 - parity) * half, 16), half), :].astype(BF16)


def edge_backward_kernel(n, slots, *refs):
    edge, cot, hidden, slope, normed, inverse, r_at, s_row, r_row, gains, table, w = refs[:12]
    near, refs = refs[12 : 12 + n], refs[12 + n :]
    pre_grad_ref, keep, send, sent_ref, received_ref, near_all = refs[:6]
    grads, sent, received = refs[6:]
    here = lax.axis_index("feat")
    parity = lax.axis_index("region") % 2
    own = near[0].shape[0]
    nodes = own * n

    @pl.when(pl.program_id(0) == 0)
    def _():
        for b in range(n):
            near_all[b * own : (b + 1) * own, :] = near[b][...]
        grads[...] = jnp.zeros_like(grads)
        sent[...] = jnp.zeros_like(sent)
        received[...] = jnp.zeros_like(received)

    total = cot[...].astype(F32) + dot(hot(r_at[...], nodes), near_all[...])
    mix_grad = layer_norm_back(total * gains[0:1, :], normed[...].astype(F32), inverse[:, :1])
    pre_grad = (dot_t(mix_grad, w[3]) * slope[...].astype(F32)).astype(BF16)
    pre_grad_ref[...] = pre_grad
    grads[0] += t_dot(edge[...], pre_grad)
    grads[3] += t_dot(hidden[...], mix_grad)
    sent[...] += dot(hot_t(s_row[...], table.shape[0]), pre_grad)
    received[...] += dot(hot_t(r_row[...], nodes), pre_grad)

    @pl.when(pl.program_id(0) == pl.num_programs(0) - 1)
    def _():
        from_senders = sent[...].astype(BF16)
        from_receivers = received[...].astype(BF16)
        grads[1] = t_dot(table[...], from_senders)
        grads[2] = t_dot(table[:nodes, :], from_receivers)
        split_grads(grads, n, keep, send, parity, here)
        sent_ref[...] = from_senders
        received_ref[...] = from_receivers
        back = dot_t(from_senders[nodes:], w[1]).astype(BF16)
        at = n * grads.shape[0] * (grads.shape[1] // n // 2)
        count = (keep.shape[0] - at) // slots
        for b in range(count):
            rows = slice(at + b * slots, at + (b + 1) * slots)
            keep[rows, :] = back[(2 * b) * slots : (2 * b + 1) * slots]
            send[rows, :] = back[(2 * b + 1) * slots : (2 * b + 2) * slots]


def edge_grad_kernel(cot, r_at, near, pre_grad, w, out):
    total = cot[...].astype(F32) + dot(hot(r_at[...], near.shape[0]), near[...])
    out[...] = total + dot_t(pre_grad[...], w[0])


def return_kernel(n, pairs, sent, received, w, at_ref, *refs):
    blocks, outs = refs[:pairs], refs[pairs:]
    nodes = received.shape[0]
    own = nodes // n
    rows = blocks[0].shape[0]
    total = dot_t(sent[:nodes, :], w[1]) + dot_t(received[...], w[2])
    for b in range(pairs):
        total = total + dot(hot_t(at_ref[0:1, b * rows : (b + 1) * rows], nodes), blocks[b][...])
    for b in range(n):
        outs[b][...] = total[b * own : (b + 1) * own, :].astype(BF16)


def pair_sum_kernel(n, slots, keep, got, *outs):
    block = outs[0].shape[0]
    for b in range(n):
        rows = slice(b * block, (b + 1) * block)
        outs[b][...] = (keep[rows, :].astype(F32) + got[rows, :].astype(F32)).astype(BF16)
    for b, out in enumerate(outs[n:]):
        rows = slice(n * block + b * slots, n * block + (b + 1) * slots)
        out[:slots, :] = keep[rows, :]
        out[slots:, :] = got[rows, :]


def scatter_sum_kernel(n, pairs, *refs):
    parts, outs, total = refs[:n], refs[n : n + pairs], refs[n + pairs]
    z = lax.axis_index("region") // 2
    total[...] = add_all([part[...] for part in parts])
    rows = outs[0].shape[0]
    for b in range(pairs):
        outs[b][...] = total[pl.ds(pl.multiple_of((z ^ b) * rows, rows), rows), :].astype(BF16)


def sum_kernel(pairs, *refs):
    edge, node, out = refs[:pairs], refs[pairs : 2 * pairs], refs[2 * pairs]
    cut = edge[0].shape[0]
    out[:cut, :] = add_all([part[...] for part in edge]).astype(BF16)
    out[cut:, :] = add_all([part[...] for part in node]).astype(BF16)


def finish_kernel(pairs, cut, edge_norm, node_norm, *refs):
    mine, theirs = refs[:pairs], refs[pairs : 2 * pairs]
    outs, total = refs[2 * pairs : -1], refs[-1]
    region = lax.axis_index("region")
    parity, z = region % 2, region // 2
    rows = mine[0].shape[0]
    for b in range(pairs):
        for side, ref in ((parity, mine[b]), (1 - parity, theirs[b])):
            base = side * pairs * rows
            start = pl.multiple_of(base + (z ^ b) * cut, 16)
            total[pl.ds(start, cut), :] = ref[:cut, :].astype(F32)
            start = pl.multiple_of(base + pairs * cut + (z ^ b) * (rows - cut), 16)
            total[pl.ds(start, rows - cut), :] = ref[cut:, :].astype(F32)
    spread(total, outs, edge_norm, node_norm)


def spread(total, outs, edge_norm, node_norm):
    portion = outs[1].shape[0]
    size = total.shape[0] // 2
    for norm, m, at, pair in ((edge_norm, 4, 0, outs[:2]), (node_norm, 3, 2 * portion, outs[2:])):
        half = m * portion // 2
        for u in range(2 * m):
            row = u * (portion // 2)
            source = (row // half) * size + at + row % half
            out, start = (pair[0], row) if u < 2 * m - 2 else (pair[1], row - (m - 1) * portion)
            out[start : start + portion // 2, :] = total[source : source + portion // 2, :] * norm


def gather_halves(mine):
    pieces = []
    for b in range(1, lax.axis_size("feat")):
        got = swap(mine, "feat", b)
        pieces += [got, swap(got, "region", 1)]
    return pieces


def chip_exchange(blocks):
    return [blocks[0]] + [swap(blocks[b], "region", 2 * b) for b in range(1, len(blocks))]


def reduce_grads(parts, node_parts, portion, edge_norm, node_norm):
    half, d = parts[0].shape
    pairs = lax.axis_size("region") // 2
    z = lax.axis_index("region") // 2
    parity = lax.axis_index("region") % 2
    node_half = node_parts[0].shape[0]
    size = half + node_half
    rows, cut = size // pairs, half // pairs
    aligned = cut % 16 == 0 and rows % 16 == 0
    outs = [shape((k * portion, d), F32) for k in (3, 1, 2, 1)]

    def scattered(parts, total):
        rows = total // pairs
        if aligned:
            parts = call(
                functools.partial(scatter_sum_kernel, len(parts), pairs),
                parts,
                [shape((rows, d))] * pairs,
                [pltpu.VMEM((total, d), F32)],
            )
        else:
            mine = add_all(parts).astype(BF16).reshape(pairs, rows, d)
            parts = [lax.dynamic_index_in_dim(mine, z ^ b, 0, keepdims=False) for b in range(pairs)]
        return chip_exchange(parts)

    node_parts = scattered(node_parts, node_half)
    parts = scattered(parts, half)
    if aligned:
        (chunk,) = call(
            functools.partial(sum_kernel, pairs), [*parts, *node_parts], [shape((rows, d))]
        )
    else:
        chunk = jnp.concatenate([add_all(parts), add_all(node_parts)]).astype(BF16)
    mine = chip_exchange([chunk] * pairs)
    theirs = [swap(piece, "region", 1) for piece in mine]
    if aligned:
        return call(
            functools.partial(finish_kernel, pairs, cut, edge_norm, node_norm),
            mine + theirs,
            outs,
            [pltpu.VMEM((2 * size, d), F32)],
        )
    order = jnp.arange(pairs) ^ z
    sides = []
    for side in (mine, theirs):
        side = jnp.stack(side)[order]
        sides += [side[:, :cut].reshape(half, d), side[:, cut:].reshape(node_half, d)]
    swapped = sides[2:] + sides[:2]
    total = jnp.where(parity == 0, jnp.concatenate(sides), jnp.concatenate(swapped)).astype(F32)

    def from_total(*refs):
        spread(refs[0], refs[1:], edge_norm, node_norm)

    return call(from_total, [total], outs)


def layer(
    node_lat,
    edge_lat,
    receiver_row,
    sender_slot,
    send_rows,
    w_edge_in,
    w_edge_out,
    w_node_in,
    w_node_out,
    edge_gain,
    node_gain,
    node_cot,
    edge_cot,
):
    n = lax.axis_size("feat")
    regions = lax.axis_size("region")
    pairs = regions // 2
    here = lax.axis_index("feat")
    region = lax.axis_index("region")
    own, d = node_lat.shape
    nodes = own * n
    share = edge_lat.shape[0]
    slots = send_rows.shape[2]
    table_size = nodes + regions * slots

    def relative(row):
        return ((row // own) ^ here) * own + row % own

    local_receivers = lax.dynamic_slice_in_dim(receiver_row, here * share, share)
    local_senders = lax.dynamic_slice_in_dim(sender_slot, here * share, share)
    remote = jnp.maximum(local_senders - nodes, 0)
    sender_at = jnp.where(
        local_senders < nodes,
        relative(local_senders),
        nodes + ((remote // slots) ^ region) * slots + remote % slots,
    )
    receiver_at = relative(local_receivers)

    portion = d // n
    half = portion // 2
    gain_rows = [edge_gain[None], node_gain[None]]
    near = feat_swaps([node_lat] * n)
    edge_pack = pack_halves(w_edge_in, w_edge_out, gain_rows)
    node_pack = pack_halves(w_node_in, w_node_out, [])
    w_edge = gather_halves(edge_pack)

    square = 2 * d * d
    keep, send, send_at = call(
        functools.partial(outgoing_kernel, n),
        [send_rows[0], *near],
        [shape((pairs, slots, d))] * 2 + [shape((8, regions * slots), jnp.int32)],
        flops=2 * regions * slots * nodes * d,
    )
    other = swap(send, "region", 1)
    remote_rows = chip_exchange(call(join_kernel, [keep, other], [shape((2 * slots, d))] * pairs))
    w_node = gather_halves(node_pack)

    tile = tile_of(share)
    steps = share // tile
    by_rows = lambda width: pl.BlockSpec((tile, width), lambda i: (i, 0))
    by_columns = pl.BlockSpec((1, tile), lambda i: (0, i))
    edge_params = pltpu.CompilerParams(
        dimension_semantics=("arbitrary",), vmem_limit_bytes=VMEM_LIMIT
    )
    ins = [edge_lat, sender_at[:, None], receiver_at[:, None], receiver_at[None]]
    rest = [*gain_rows, w_edge_in, w_edge_out, *near, *remote_rows, *w_edge]
    outs = [shape((share, d))] * 4 + [shape((share, 128), F32)]
    kept = [shape((table_size, d)), shape((4, d, d)), shape((8, d), F32)] + [shape((own, d))] * n
    edge_new, hidden, slope, normed, inverse, table, w_full, gains, *pooled_parts = pl.pallas_call(
        functools.partial(edge_forward_kernel, n, pairs),
        out_shape=tuple(outs + kept),
        grid=(steps,),
        in_specs=[by_rows(d), by_rows(1), by_rows(1), by_columns]
        + [whole_block(x.shape) for x in rest],
        out_specs=tuple([by_rows(d)] * 4 + [by_rows(128)] + [whole_block(x.shape) for x in kept]),
        scratch_shapes=[pltpu.VMEM((nodes, d), F32), pltpu.VMEM((n, 8, portion), F32)],
        compiler_params=edge_params,
        cost_estimate=pl.CostEstimate(
            flops=7 * share * square, bytes_accessed=8 * share * d, transcendentals=share * d
        ),
        name="edge_forward",
    )(*ins, *rest)

    parts = feat_swaps(pooled_parts)
    node_new, pooled_grad, node_base, *messages = call(
        functools.partial(node_kernel, n),
        [node_lat, node_cot, gains, w_node_in, w_node_out, *parts, *w_node],
        [shape((own, d)), shape((own, d)), shape((own, d), F32)]
        + [shape((own, 2 * d + 2 * portion))] * n,
        [pltpu.VMEM((3, d, d), BF16)],
        flops=6 * own * square,
    )
    grad_near = feat_swaps([pooled_grad] * n)
    messages = feat_swaps(messages)

    ins = [edge_lat, edge_cot, hidden, slope, normed, inverse, receiver_at[:, None], sender_at[None], receiver_at[None]]
    rest = [gains, table, w_full, *grad_near]
    kept = [shape((n * 2 * portion + pairs * slots, d))] * 2
    kept += [shape((table_size, d)), shape((nodes, d)), shape((nodes, d))]
    edge_pre_grad, keep, send, sent, received, near_grad = pl.pallas_call(
        functools.partial(edge_backward_kernel, n, slots),
        out_shape=tuple([shape((share, d))] + kept),
        grid=(steps,),
        in_specs=[by_rows(d)] * 5 + [by_rows(128), by_rows(1), by_columns, by_columns]
        + [whole_block(x.shape) for x in rest],
        out_specs=tuple([by_rows(d)] + [whole_block(x.shape) for x in kept]),
        scratch_shapes=[
            pltpu.VMEM((4, d, d), F32),
            pltpu.VMEM((table_size, d), F32),
            pltpu.VMEM((nodes, d), F32),
        ],
        compiler_params=edge_params,
        cost_estimate=pl.CostEstimate(
            flops=10 * share * square, bytes_accessed=16 * share * d, transcendentals=0
        ),
        name="edge_backward",
    )(*ins, *rest)
    got = swap(send, "region", 1)
    node_keep, node_send = call(
        functools.partial(node_weight_kernel, n),
        [*near, *messages],
        [shape((3 * half, d))] * 2,
        [pltpu.VMEM((n, own, portion), BF16), pltpu.VMEM((3 * portion, d), F32)],
        flops=3 * nodes * square // n,
    )
    node_got = swap(node_send, "region", 1)
    outs = call(
        functools.partial(pair_sum_kernel, n, slots),
        [keep, got],
        [shape((4 * half, d))] * n + [shape((2 * slots, d))] * pairs,
    )
    parts = feat_swaps(outs[:n])
    returned = chip_exchange(outs[n:])
    grad_edge_in, grad_edge_out, grad_node_in, grad_node_out = reduce_grads(
        parts,
        [node_keep, node_got],
        portion,
        float((share * n * regions) ** -0.5),
        float((nodes * regions) ** -0.5),
    )

    edge_grad = pl.pallas_call(
        edge_grad_kernel,
        out_shape=shape((share, d), F32),
        grid=(steps,),
        in_specs=[by_rows(d), by_rows(1), whole_block((nodes, d)), by_rows(d), whole_block((1, d, d))],
        out_specs=by_rows(d),
        compiler_params=edge_params,
        cost_estimate=pl.CostEstimate(flops=2 * share * square, bytes_accessed=8 * share * d, transcendentals=0),
        name="edge_grad",
    )(edge_cot, receiver_at[:, None], near_grad, edge_pre_grad, w_full)
    parts = call(
        functools.partial(return_kernel, n, pairs),
        [sent, received, w_full, send_at, *returned],
        [shape((own, d))] * n,
        flops=4 * nodes * square,
    )
    node_grad = node_base + add_all(feat_swaps(parts))

    return (
        node_new,
        edge_new,
        node_grad,
        edge_grad,
        grad_edge_in.reshape(w_edge_in.shape),
        grad_edge_out,
        grad_node_in.reshape(w_node_in.shape),
        grad_node_out,
    )


def solution(mesh):
    rows = P(("region", "feat"), None)
    in_specs = (
        rows,
        rows,
        P("region"),
        P("region"),
        P("region", None, None),
        P(None, "feat", None),
        P("feat", None),
        P(None, "feat", None),
        P("feat", None),
        P("feat"),
        P("feat"),
        rows,
        rows,
    )
    out_specs = (
        rows,
        rows,
        rows,
        rows,
        P(None, "feat", None),
        P("feat", None),
        P(None, "feat", None),
        P("feat", None),
    )
    return jax.shard_map(layer, mesh=mesh, in_specs=in_specs, out_specs=out_specs, check_vma=False)
```

```python
import functools

import jax
import jax.numpy as jnp
from jax import lax
from jax.experimental import pallas as pl
from jax.experimental.pallas import tpu as pltpu
from jax.sharding import PartitionSpec as P


EPSILON = 1e-05
F32 = jnp.float32
BF16 = jnp.bfloat16
VMEM_LIMIT = 36 * 1024 * 1024


def dot(a, b):
    return jnp.dot(a, b, preferred_element_type=F32)


def dot_t(a, b):
    return lax.dot_general(a, b, (((1,), (1,)), ((), ())), preferred_element_type=F32)


def t_dot(a, b):
    return lax.dot_general(a, b, (((0,), (0,)), ((), ())), preferred_element_type=F32)


def swap(x, axis, bits):
    n = lax.axis_size(axis)
    return lax.ppermute(x, axis, [(i, i ^ bits) for i in range(n)])


def feat_swaps(parts):
    return [parts[0]] + [swap(parts[b], "feat", b) for b in range(1, len(parts))]


def add_all(parts):
    total = parts[0].astype(F32)
    for part in parts[1:]:
        total = total + part.astype(F32)
    return total


def layer_norm(values):
    breadth = values.shape[1]
    average = jnp.sum(values, axis=1, keepdims=True) / breadth
    variance = jnp.sum(values * values, axis=1, keepdims=True) / breadth - average * average
    inverse = lax.rsqrt(variance + EPSILON)
    return (values - average) * inverse, inverse


def layer_norm_back(scaled, normed, inverse):
    breadth = scaled.shape[1]
    first = jnp.sum(scaled, axis=1, keepdims=True) / breadth
    second = jnp.sum(scaled * normed, axis=1, keepdims=True) / breadth
    return (inverse * (scaled - first - normed * second)).astype(BF16)


def swish_and_slope(values):
    s = 0.5 * jnp.tanh(0.5 * values) + 0.5
    return (values * s).astype(BF16), s * (1.0 + values * (1.0 - s))


def hot(column, width):
    at = lax.broadcasted_iota(jnp.int32, (column.shape[0], width), 1)
    return jnp.where(column == at, 1.0, 0.0).astype(BF16)


def hot_t(row, height):
    at = lax.broadcasted_iota(jnp.int32, (height, row.shape[1]), 0)
    return jnp.where(row == at, 1.0, 0.0).astype(BF16)


def tile_of(rows):
    for size in (256, 192, 128, 96, 64, 48, 32, 16):
        if rows % size == 0:
            return size
    return rows


def shape(dims, dtype=BF16):
    return jax.ShapeDtypeStruct(tuple(dims), dtype)


def whole_block(dims):
    return pl.BlockSpec(tuple(dims), lambda *_: (0,) * len(dims))


def call(kernel, ins, outs, scratch=(), flops=0):
    return pl.pallas_call(
        kernel,
        out_shape=tuple(outs),
        grid=(1,),
        in_specs=[whole_block(x.shape) for x in ins],
        out_specs=tuple(whole_block(x.shape) for x in outs),
        scratch_shapes=list(scratch),
        compiler_params=pltpu.CompilerParams(vmem_limit_bytes=VMEM_LIMIT),
        cost_estimate=pl.CostEstimate(
            flops=flops,
            bytes_accessed=sum(x.size * x.dtype.itemsize for x in (*ins, *outs)),
            transcendentals=0,
        ),
    )(*ins)


def fill_weights(w_ref, own_in, own_out, pieces, parity, here):
    m = w_ref.shape[0]
    portion = own_out.shape[0]
    half = portion // 2
    at = pl.multiple_of(here * portion, half)
    for k in range(m):
        w_ref[k, pl.ds(at, portion), :] = own_in[k] if k < m - 1 else own_out[...]
    for b, (got, other) in enumerate(pieces, start=1):
        start = (here ^ b) * portion
        first = pl.multiple_of(start + parity * half, half)
        second = pl.multiple_of(start + (1 - parity) * half, half)
        for k in range(m):
            w_ref[k, pl.ds(first, half), :] = got[k * half : (k + 1) * half, :]
            w_ref[k, pl.ds(second, half), :] = other[k * half : (k + 1) * half, :]


def split_grads(grads, n, keep, send, parity, here):
    m = grads.shape[0]
    portion = grads.shape[1] // n
    half = portion // 2
    block = m * half
    for side in range(2):

        @pl.when(parity == side)
        def _():
            for f in range(n):
                for u in range(2 * m):
                    out = keep if u // m == side else send
                    at = f * portion + (u % 2) * half
                    start = pl.multiple_of((f ^ here) * block + (u % m) * half, half)
                    out[pl.ds(start, half), :] = grads[u // 2, at : at + half, :].astype(BF16)


def prepare_kernel(edge_in, edge_out, node_in, node_out, edge_gain, node_gain, lat, rows, *refs):
    edge_pack, node_pack, lat_out, rows_out, sems, edge_held, node_held = refs
    half = edge_out.shape[0] // 2
    at = pl.multiple_of(lax.axis_index("region") % 2 * half, half)
    moves = [(edge_gain, edge_held), (node_gain, node_held)]
    for inner, outer, pack in ((edge_in, edge_out, edge_pack), (node_in, node_out, node_pack)):
        m = inner.shape[0]
        for k in range(m):
            moves.append((inner.at[k, pl.ds(at, half)], pack.at[pl.ds(k * half, half)]))
        moves.append((outer.at[pl.ds(at, half)], pack.at[pl.ds(m * half, half)]))
    moves += [(lat, lat_out), (rows, rows_out)]
    copies = [pltpu.make_async_copy(a, b, sems.at[k]) for k, (a, b) in enumerate(moves)]
    for copy in copies:
        copy.start()
    below = edge_pack.shape[0] - 16
    edge_pack[below:, :] = jnp.zeros((16, edge_pack.shape[1]), BF16)
    for copy in copies:
        copy.wait()
    parts = []
    for ref in (edge_held, node_held):
        left = ref[...]
        for _ in range(3):
            part = left.astype(BF16)
            left = left - part.astype(F32)
            parts.append(part.astype(F32))
    parts.append(jnp.zeros((16 - len(parts), left.shape[1]), F32))
    edge_pack[below:, : left.shape[1]] = jnp.concatenate(parts, axis=0).astype(BF16)


def prepare(*ins):
    edge_in, edge_out, node_in, _, edge_gain, _, lat, rows = ins
    half, d = edge_out.shape[0] // 2, edge_out.shape[1]
    counts = [(edge_in.shape[0] + 1), (node_in.shape[0] + 1)]
    outs = [shape((counts[0] * half + 16, d)), shape((counts[1] * half, d)), shape(lat.shape), shape(rows.shape, rows.dtype)]
    return pl.pallas_call(
        prepare_kernel,
        out_shape=tuple(outs),
        grid=(1,),
        in_specs=[pl.BlockSpec(memory_space=pltpu.HBM)] * len(ins),
        out_specs=tuple(whole_block(x.shape) for x in outs),
        scratch_shapes=[pltpu.SemaphoreType.DMA((sum(counts) + 4,))] + [pltpu.VMEM(edge_gain.shape, F32)] * 2,
        compiler_params=pltpu.CompilerParams(vmem_limit_bytes=VMEM_LIMIT),
        cost_estimate=pl.CostEstimate(flops=8 * half * d, bytes_accessed=32 * half * d, transcendentals=0),
        name="prepare",
    )(*(pltpu.with_memory_space_constraint(x, pltpu.HBM) for x in ins))


def fill_gains(gain_ref, blocks, own, pieces, here):
    portion = blocks.shape[2]
    blocks[here, 0:1, :] = own[0][...]
    blocks[here, 1:2, :] = own[1][...]
    for b, (got, _) in enumerate(pieces, start=1):
        parts = got[got.shape[0] - 16 :, :portion].astype(F32)
        blocks[here ^ b, 0:1, :] = parts[0:1] + parts[1:2] + parts[2:3]
        blocks[here ^ b, 1:2, :] = parts[3:4] + parts[4:5] + parts[5:6]
    for f in range(blocks.shape[0]):
        gain_ref[0:2, f * portion : (f + 1) * portion] = blocks[f, 0:2, :]


def outgoing_kernel(n, rows_ref, *refs):
    near, (keep, send, at_ref) = refs[:n], refs[n:]
    own = near[0].shape[0]
    here = lax.axis_index("feat")
    region = lax.axis_index("region")
    regions, slots = rows_ref.shape
    for b in range(regions):
        row = rows_ref[pl.ds(region ^ b, 1), :]
        feat = jnp.zeros_like(row)
        for k in range(1, n):
            feat = feat + jnp.where(row >= k * own, 1, 0)
        at_ref[0:1, b * slots : (b + 1) * slots] = (feat ^ here) * own + row - feat * own
    at = at_ref[0:1, :]
    rows = jnp.zeros((at.shape[1], near[0].shape[1]), F32)
    for b in range(n):
        rows = rows + t_dot(hot_t(at - b * own, own), near[b][...])
    rows = rows.astype(BF16)
    pairs, slots, _ = keep.shape
    for b in range(pairs):
        keep[b] = rows[(2 * b) * slots : (2 * b + 1) * slots]
        send[b] = rows[(2 * b + 1) * slots : (2 * b + 2) * slots]


def join_kernel(keep, other, *outs):
    slots = keep.shape[1]
    for b, out in enumerate(outs):
        out[:slots, :] = keep[b]
        out[slots:, :] = other[b]


def edge_forward_kernel(n, pairs, *refs):
    edge, s_at, r_at, r_row, edge_gain, node_gain, own_in, own_out = refs[:8]
    refs = refs[8:]
    tables, refs = refs[: n + pairs], refs[n + pairs :]
    pieces = [(refs[2 * b], refs[2 * b + 1]) for b in range(n - 1)]
    refs = refs[2 * (n - 1) :]
    new, hidden_ref, slope_ref, normed_ref, inverse_ref, table, w, gains = refs[:8]
    pooled, total, blocks = refs[8 : 8 + n], refs[8 + n], refs[9 + n]
    here = lax.axis_index("feat")
    parity = lax.axis_index("region") % 2
    own = tables[0].shape[0]
    nodes = own * n

    @pl.when(pl.program_id(0) == 0)
    def _():
        at = 0
        for piece in tables:
            table[at : at + piece.shape[0], :] = piece[...]
            at += piece.shape[0]
        fill_weights(w, own_in, own_out, pieces, parity, here)
        fill_gains(gains, blocks, (edge_gain, node_gain), pieces, here)
        total[...] = jnp.zeros_like(total)

    lat = edge[...]
    senders = dot(hot(s_at[...], table.shape[0]), table[...]).astype(BF16)
    receivers = dot(hot(r_at[...], nodes), table[:nodes, :]).astype(BF16)
    pre = dot(lat, w[0]) + dot(senders, w[1]) + dot(receivers, w[2])
    hidden, slope = swish_and_slope(pre)
    hidden_ref[...] = hidden
    slope_ref[...] = slope.astype(BF16)
    normed, inverse = layer_norm(dot(hidden, w[3]))
    normed_ref[...] = normed.astype(BF16)
    inverse_ref[...] = jnp.broadcast_to(inverse, inverse_ref.shape)
    updated = (lat.astype(F32) + normed * gains[0:1, :]).astype(BF16)
    new[...] = updated
    total[...] += dot(hot_t(r_row[...], nodes), updated)

    @pl.when(pl.program_id(0) == pl.num_programs(0) - 1)
    def _():
        for b in range(n):
            pooled[b][...] = total[b * own : (b + 1) * own, :].astype(BF16)


def node_kernel(n, lat_ref, cot_ref, gains, own_in, own_out, *refs):
    parts, refs = refs[:n], refs[n:]
    pieces = [(refs[2 * b], refs[2 * b + 1]) for b in range(n - 1)]
    refs = refs[2 * (n - 1) :]
    new, pooled_grad, base = refs[:3]
    messages, w = refs[3 : 3 + n], refs[3 + n]
    here = lax.axis_index("feat")
    parity = lax.axis_index("region") % 2
    gain = gains[1:2, :]
    fill_weights(w, own_in, own_out, pieces, parity, here)
    pooled = add_all([part[...] for part in parts]).astype(BF16)
    lat = lat_ref[...]
    pre = dot(lat, w[0]) + dot(pooled, w[1])
    hidden, slope = swish_and_slope(pre)
    normed, inverse = layer_norm(dot(hidden, w[2]))
    new[...] = (lat.astype(F32) + normed * gain).astype(BF16)
    cot = cot_ref[...].astype(F32)
    mix_grad = layer_norm_back(cot * gain, normed, inverse)
    pre_grad = (dot_t(mix_grad, w[2]) * slope).astype(BF16)
    pooled_grad[...] = dot_t(pre_grad, w[1]).astype(BF16)
    base[...] = cot + dot_t(pre_grad, w[0])
    d = lat.shape[1]
    portion = d // n
    for b in range(n):
        messages[b][:, :d] = pre_grad
        messages[b][:, d : 2 * d] = mix_grad
    for f in range(n):

        @pl.when(here == f)
        def _():
            for b in range(n):
                block = slice((f ^ b) * portion, ((f ^ b) + 1) * portion)
                messages[b][:, 2 * d : 2 * d + portion] = pooled[:, block]
                messages[b][:, 2 * d + portion :] = hidden[:, block]


def node_weight_kernel(n, *refs):
    near, messages, (keep, send, lat, grads) = refs[:n], refs[n : 2 * n], refs[2 * n :]
    here = lax.axis_index("feat")
    parity = lax.axis_index("region") % 2
    _, d = near[0].shape
    portion = d // n
    for f in range(n):

        @pl.when(here == f)
        def _():
            for b in range(n):
                lat[b] = near[b][:, f * portion : (f + 1) * portion]

    totals = [jnp.zeros((portion, d), F32)] * 3
    for b in range(n):
        pre_grad = messages[b][:, :d]
        mix_grad = messages[b][:, d : 2 * d]
        totals[0] = totals[0] + t_dot(lat[b], pre_grad)
        totals[1] = totals[1] + t_dot(messages[b][:, 2 * d : 2 * d + portion], pre_grad)
        totals[2] = totals[2] + t_dot(messages[b][:, 2 * d + portion :], mix_grad)
    for k in range(3):
        grads[k * portion : (k + 1) * portion, :] = totals[k]
    half = keep.shape[0]
    keep[...] = grads[pl.ds(pl.multiple_of(parity * half, 16), half), :].astype(BF16)
    send[...] = grads[pl.ds(pl.multiple_of((1 - parity) * half, 16), half), :].astype(BF16)


def edge_backward_kernel(n, slots, *refs):
    edge, cot, hidden, slope, normed, inverse, r_at, s_row, r_row, gains, table, w = refs[:12]
    near, refs = refs[12 : 12 + n], refs[12 + n :]
    pre_grad_ref, keep, send, sent_ref, received_ref, near_all = refs[:6]
    grads, sent, received = refs[6:]
    here = lax.axis_index("feat")
    parity = lax.axis_index("region") % 2
    own = near[0].shape[0]
    nodes = own * n

    @pl.when(pl.program_id(0) == 0)
    def _():
        for b in range(n):
            near_all[b * own : (b + 1) * own, :] = near[b][...]
        grads[...] = jnp.zeros_like(grads)
        sent[...] = jnp.zeros_like(sent)
        received[...] = jnp.zeros_like(received)

    total = cot[...].astype(F32) + dot(hot(r_at[...], nodes), near_all[...])
    mix_grad = layer_norm_back(total * gains[0:1, :], normed[...].astype(F32), inverse[:, :1])
    pre_grad = (dot_t(mix_grad, w[3]) * slope[...].astype(F32)).astype(BF16)
    pre_grad_ref[...] = pre_grad
    grads[0] += t_dot(edge[...], pre_grad)
    grads[3] += t_dot(hidden[...], mix_grad)
    sent[...] += dot(hot_t(s_row[...], table.shape[0]), pre_grad)
    received[...] += dot(hot_t(r_row[...], nodes), pre_grad)

    @pl.when(pl.program_id(0) == pl.num_programs(0) - 1)
    def _():
        from_senders = sent[...].astype(BF16)
        from_receivers = received[...].astype(BF16)
        grads[1] = t_dot(table[...], from_senders)
        grads[2] = t_dot(table[:nodes, :], from_receivers)
        split_grads(grads, n, keep, send, parity, here)
        sent_ref[...] = from_senders
        received_ref[...] = from_receivers
        back = dot_t(from_senders[nodes:], w[1]).astype(BF16)
        at = n * grads.shape[0] * (grads.shape[1] // n // 2)
        count = (keep.shape[0] - at) // slots
        for b in range(count):
            rows = slice(at + b * slots, at + (b + 1) * slots)
            keep[rows, :] = back[(2 * b) * slots : (2 * b + 1) * slots]
            send[rows, :] = back[(2 * b + 1) * slots : (2 * b + 2) * slots]


def edge_grad_kernel(cot, r_at, near, pre_grad, w, out):
    total = cot[...].astype(F32) + dot(hot(r_at[...], near.shape[0]), near[...])
    out[...] = total + dot_t(pre_grad[...], w[0])


def return_kernel(n, pairs, sent, received, w, at_ref, *refs):
    blocks, outs = refs[:pairs], refs[pairs:]
    nodes = received.shape[0]
    own = nodes // n
    rows = at_ref.shape[1] // pairs
    total = dot_t(sent[:nodes, :], w[1]) + dot_t(received[...], w[2])
    for b in range(pairs):
        total = total + dot(hot_t(at_ref[0:1, b * rows : (b + 1) * rows], nodes), blocks[b][:rows, :])
    for b in range(n):
        outs[b][...] = total[b * own : (b + 1) * own, :].astype(BF16)


def pair_sum_kernel(n, keep, got, *outs):
    block = outs[0].shape[0]
    for b in range(n):
        rows = slice(b * block, (b + 1) * block)
        outs[b][...] = (keep[rows, :].astype(F32) + got[rows, :].astype(F32)).astype(BF16)


def chip_rows_kernel(slots, mine, theirs, *refs):
    pairs = mine.shape[0] // slots
    node_parts, outs, total = (refs[:2], refs[2:-1], refs[-1]) if len(refs) > pairs else ((), refs, None)
    z = lax.axis_index("region") // 2
    if node_parts:
        total[...] = add_all([part[...] for part in node_parts])
    for b, out in enumerate(outs):
        out[:slots, :] = mine[b * slots : (b + 1) * slots, :]
        out[slots : 2 * slots, :] = theirs[b * slots : (b + 1) * slots, :]
        if node_parts:
            rows = out.shape[0] - 2 * slots
            out[2 * slots :, :] = total[pl.ds(pl.multiple_of((z ^ b) * rows, 16), rows), :].astype(BF16)


def scatter_sum_kernel(n, pairs, *refs):
    parts, outs, total = refs[:n], refs[n : n + pairs], refs[n + pairs]
    z = lax.axis_index("region") // 2
    total[...] = add_all([part[...] for part in parts])
    rows = outs[0].shape[0]
    for b in range(pairs):
        outs[b][...] = total[pl.ds(pl.multiple_of((z ^ b) * rows, rows), rows), :].astype(BF16)


def sum_kernel(pairs, *refs):
    edge, node, out = refs[:pairs], refs[pairs : 2 * pairs], refs[2 * pairs]
    cut = edge[0].shape[0]
    first = node[0].shape[0] - (out.shape[0] - cut)
    out[:cut, :] = add_all([part[...] for part in edge]).astype(BF16)
    out[cut:, :] = add_all([part[first:, :] for part in node]).astype(BF16)


def finish_kernel(pairs, cut, edge_norm, node_norm, *refs):
    mine, theirs = refs[:pairs], refs[pairs : 2 * pairs]
    outs, total = refs[2 * pairs : -1], refs[-1]
    region = lax.axis_index("region")
    parity, z = region % 2, region // 2
    rows = mine[0].shape[0]
    for b in range(pairs):
        for side, ref in ((parity, mine[b]), (1 - parity, theirs[b])):
            base = side * pairs * rows
            start = pl.multiple_of(base + (z ^ b) * cut, 16)
            total[pl.ds(start, cut), :] = ref[:cut, :].astype(F32)
            start = pl.multiple_of(base + pairs * cut + (z ^ b) * (rows - cut), 16)
            total[pl.ds(start, rows - cut), :] = ref[cut:, :].astype(F32)
    spread(total, outs, edge_norm, node_norm)


def spread(total, outs, edge_norm, node_norm):
    portion = outs[1].shape[0]
    size = total.shape[0] // 2
    for norm, m, at, pair in ((edge_norm, 4, 0, outs[:2]), (node_norm, 3, 2 * portion, outs[2:])):
        half = m * portion // 2
        for u in range(2 * m):
            row = u * (portion // 2)
            source = (row // half) * size + at + row % half
            out, start = (pair[0], row) if u < 2 * m - 2 else (pair[1], row - (m - 1) * portion)
            out[start : start + portion // 2, :] = total[source : source + portion // 2, :] * norm


def gather_halves(mine):
    pieces = []
    for b in range(1, lax.axis_size("feat")):
        got = swap(mine, "feat", b)
        pieces += [got, swap(got, "region", 1)]
    return pieces


def chip_exchange(blocks):
    return [blocks[0]] + [swap(blocks[b], "region", 2 * b) for b in range(1, len(blocks))]


def reduce_grads(parts, node_parts, back, slots, portion, edge_norm, node_norm):
    n = len(parts)
    half, d = parts[0].shape
    pairs = lax.axis_size("region") // 2
    z = lax.axis_index("region") // 2
    parity = lax.axis_index("region") % 2
    node_half = node_parts[0].shape[0]
    size = half + node_half
    rows, cut = size // pairs, half // pairs
    aligned = cut % 16 == 0 and rows % 16 == 0
    outs = [shape((k * portion, d), F32) for k in (3, 1, 2, 1)]

    def chunks(parts):
        mine = add_all(parts).astype(BF16).reshape(pairs, -1, d)
        return [lax.dynamic_index_in_dim(mine, z ^ b, 0, keepdims=False) for b in range(pairs)]

    given = node_parts if aligned else []
    returned = call(
        functools.partial(chip_rows_kernel, slots),
        [*back, *given],
        [shape((2 * slots + (rows - cut if given else 0), d))] * pairs,
        [pltpu.VMEM((node_half, d), F32)] if given else [],
    )
    if not aligned:
        returned = [jnp.concatenate(pair) for pair in zip(returned, chunks(node_parts))]
    returned = chip_exchange(returned)
    if aligned:
        parts = call(
            functools.partial(scatter_sum_kernel, n, pairs),
            parts,
            [shape((cut, d))] * pairs,
            [pltpu.VMEM((half, d), F32)],
        )
    else:
        parts = chunks(parts)
    parts = chip_exchange(parts)
    if aligned:
        (chunk,) = call(functools.partial(sum_kernel, pairs), [*parts, *returned], [shape((rows, d))])
    else:
        node_parts = [part[2 * slots :] for part in returned]
        chunk = jnp.concatenate([add_all(parts), add_all(node_parts)]).astype(BF16)
    mine = chip_exchange([chunk] * pairs)
    theirs = [swap(piece, "region", 1) for piece in mine]
    if aligned:
        grads = call(
            functools.partial(finish_kernel, pairs, cut, edge_norm, node_norm),
            mine + theirs,
            outs,
            [pltpu.VMEM((2 * size, d), F32)],
        )
        return grads, returned
    order = jnp.arange(pairs) ^ z
    sides = []
    for side in (mine, theirs):
        side = jnp.stack(side)[order]
        sides += [side[:, :cut].reshape(half, d), side[:, cut:].reshape(node_half, d)]
    swapped = sides[2:] + sides[:2]
    total = jnp.where(parity == 0, jnp.concatenate(sides), jnp.concatenate(swapped)).astype(F32)

    def from_total(*refs):
        spread(refs[0], refs[1:], edge_norm, node_norm)

    return call(from_total, [total], outs), returned


def layer(
    node_lat,
    edge_lat,
    receiver_row,
    sender_slot,
    send_rows,
    w_edge_in,
    w_edge_out,
    w_node_in,
    w_node_out,
    edge_gain,
    node_gain,
    node_cot,
    edge_cot,
):
    n = lax.axis_size("feat")
    regions = lax.axis_size("region")
    pairs = regions // 2
    here = lax.axis_index("feat")
    region = lax.axis_index("region")
    own, d = node_lat.shape
    nodes = own * n
    share = edge_lat.shape[0]
    slots = send_rows.shape[2]
    table_size = nodes + regions * slots

    def relative(row):
        return ((row // own) ^ here) * own + row % own

    local_receivers = lax.dynamic_slice_in_dim(receiver_row, here * share, share)
    local_senders = lax.dynamic_slice_in_dim(sender_slot, here * share, share)
    remote = jnp.maximum(local_senders - nodes, 0)
    sender_at = jnp.where(
        local_senders < nodes,
        relative(local_senders),
        nodes + ((remote // slots) ^ region) * slots + remote % slots,
    )
    receiver_at = relative(local_receivers)
    sender_column, receiver_column, receiver_line = sender_at[:, None], receiver_at[:, None], receiver_at[None]

    portion = d // n
    half = portion // 2
    gain_rows = [edge_gain[None], node_gain[None]]
    edge_pack, node_pack, own_lat, listed = prepare(
        w_edge_in, w_edge_out, w_node_in, w_node_out, *gain_rows, node_lat, send_rows[0]
    )
    near = [own_lat] + feat_swaps([node_lat] * n)[1:]
    w_edge = gather_halves(edge_pack)

    square = 2 * d * d
    keep, send, send_at = call(
        functools.partial(outgoing_kernel, n),
        [listed, *near],
        [shape((pairs, slots, d))] * 2 + [shape((8, regions * slots), jnp.int32)],
        flops=2 * regions * slots * nodes * d,
    )
    other = swap(send, "region", 1)
    remote_rows = chip_exchange(call(join_kernel, [keep, other], [shape((2 * slots, d))] * pairs))
    w_node = gather_halves(node_pack)

    tile = tile_of(share)
    steps = share // tile
    by_rows = lambda width: pl.BlockSpec((tile, width), lambda i: (i, 0))
    by_columns = pl.BlockSpec((1, tile), lambda i: (0, i))
    edge_params = pltpu.CompilerParams(
        dimension_semantics=("arbitrary",), vmem_limit_bytes=VMEM_LIMIT
    )
    ins = [edge_lat, sender_column, receiver_column, receiver_line]
    rest = [*gain_rows, w_edge_in, w_edge_out, *near, *remote_rows, *w_edge]
    outs = [shape((share, d))] * 4 + [shape((share, 128), F32)]
    kept = [shape((table_size, d)), shape((4, d, d)), shape((8, d), F32)] + [shape((own, d))] * n
    edge_new, hidden, slope, normed, inverse, table, w_full, gains, *pooled_parts = pl.pallas_call(
        functools.partial(edge_forward_kernel, n, pairs),
        out_shape=tuple(outs + kept),
        grid=(steps,),
        in_specs=[by_rows(d), by_rows(1), by_rows(1), by_columns]
        + [whole_block(x.shape) for x in rest],
        out_specs=tuple([by_rows(d)] * 4 + [by_rows(128)] + [whole_block(x.shape) for x in kept]),
        scratch_shapes=[pltpu.VMEM((nodes, d), F32), pltpu.VMEM((n, 8, portion), F32)],
        compiler_params=edge_params,
        cost_estimate=pl.CostEstimate(
            flops=7 * share * square, bytes_accessed=8 * share * d, transcendentals=share * d
        ),
        name="edge_forward",
    )(*ins, *rest)

    parts = feat_swaps(pooled_parts)
    node_new, pooled_grad, node_base, *messages = call(
        functools.partial(node_kernel, n),
        [node_lat, node_cot, gains, w_node_in, w_node_out, *parts, *w_node],
        [shape((own, d)), shape((own, d)), shape((own, d), F32)]
        + [shape((own, 2 * d + 2 * portion))] * n,
        [pltpu.VMEM((3, d, d), BF16)],
        flops=6 * own * square,
    )
    grad_near = feat_swaps([pooled_grad] * n)
    messages = feat_swaps(messages)

    ins = [edge_lat, edge_cot, hidden, slope, normed, inverse, receiver_column, sender_at[None], receiver_line]
    rest = [gains, table, w_full, *grad_near]
    kept = [shape((n * 2 * portion + pairs * slots, d))] * 2
    kept += [shape((table_size, d)), shape((nodes, d)), shape((nodes, d))]
    edge_pre_grad, keep, send, sent, received, near_grad = pl.pallas_call(
        functools.partial(edge_backward_kernel, n, slots),
        out_shape=tuple([shape((share, d))] + kept),
        grid=(steps,),
        in_specs=[by_rows(d)] * 5 + [by_rows(128), by_rows(1), by_columns, by_columns]
        + [whole_block(x.shape) for x in rest],
        out_specs=tuple([by_rows(d)] + [whole_block(x.shape) for x in kept]),
        scratch_shapes=[
            pltpu.VMEM((4, d, d), F32),
            pltpu.VMEM((table_size, d), F32),
            pltpu.VMEM((nodes, d), F32),
        ],
        compiler_params=edge_params,
        cost_estimate=pl.CostEstimate(
            flops=10 * share * square, bytes_accessed=16 * share * d, transcendentals=0
        ),
        name="edge_backward",
    )(*ins, *rest)
    got = swap(send, "region", 1)
    node_keep, node_send = call(
        functools.partial(node_weight_kernel, n),
        [*near, *messages],
        [shape((3 * half, d))] * 2,
        [pltpu.VMEM((n, own, portion), BF16), pltpu.VMEM((3 * portion, d), F32)],
        flops=3 * nodes * square // n,
    )
    node_got = swap(node_send, "region", 1)
    outs = call(functools.partial(pair_sum_kernel, n), [keep, got], [shape((4 * half, d))] * n)
    below = n * 4 * half
    grads, returned = reduce_grads(
        feat_swaps(outs),
        [node_keep, node_got],
        [keep[below:], got[below:]],
        slots,
        portion,
        float((share * n * regions) ** -0.5),
        float((nodes * regions) ** -0.5),
    )
    grad_edge_in, grad_edge_out, grad_node_in, grad_node_out = grads

    edge_grad = pl.pallas_call(
        edge_grad_kernel,
        out_shape=shape((share, d), F32),
        grid=(steps,),
        in_specs=[by_rows(d), by_rows(1), whole_block((nodes, d)), by_rows(d), whole_block((1, d, d))],
        out_specs=by_rows(d),
        compiler_params=edge_params,
        cost_estimate=pl.CostEstimate(flops=2 * share * square, bytes_accessed=8 * share * d, transcendentals=0),
        name="edge_grad",
    )(edge_cot, receiver_column, near_grad, edge_pre_grad, w_full)
    parts = call(
        functools.partial(return_kernel, n, pairs),
        [sent, received, w_full, send_at, *returned],
        [shape((own, d))] * n,
        flops=4 * nodes * square,
    )
    node_grad = node_base + add_all(feat_swaps(parts))

    return (
        node_new,
        edge_new,
        node_grad,
        edge_grad,
        grad_edge_in.reshape(w_edge_in.shape),
        grad_edge_out,
        grad_node_in.reshape(w_node_in.shape),
        grad_node_out,
    )


def solution(mesh):
    rows = P(("region", "feat"), None)
    in_specs = (
        rows,
        rows,
        P("region"),
        P("region"),
        P("region", None, None),
        P(None, "feat", None),
        P("feat", None),
        P(None, "feat", None),
        P("feat", None),
        P("feat"),
        P("feat"),
        rows,
        rows,
    )
    out_specs = (
        rows,
        rows,
        rows,
        rows,
        P(None, "feat", None),
        P("feat", None),
        P(None, "feat", None),
        P("feat", None),
    )
    return jax.shard_map(layer, mesh=mesh, in_specs=in_specs, out_specs=out_specs, check_vma=False)
```

```python
import functools

import jax
import jax.numpy as jnp
from jax import lax
from jax.experimental import pallas as pl
from jax.experimental.pallas import tpu as pltpu
from jax.sharding import PartitionSpec as P


EPSILON = 1e-05
F32 = jnp.float32
BF16 = jnp.bfloat16
VMEM_LIMIT = 36 * 1024 * 1024


def dot(a, b):
    return jnp.dot(a, b, preferred_element_type=F32)


def dot_t(a, b):
    return lax.dot_general(a, b, (((1,), (1,)), ((), ())), preferred_element_type=F32)


def t_dot(a, b):
    return lax.dot_general(a, b, (((0,), (0,)), ((), ())), preferred_element_type=F32)


def swap(x, axis, bits):
    n = lax.axis_size(axis)
    return lax.ppermute(x, axis, [(i, i ^ bits) for i in range(n)])


def feat_swaps(parts):
    return [parts[0]] + [swap(parts[b], "feat", b) for b in range(1, len(parts))]


def add_all(parts):
    total = parts[0].astype(F32)
    for part in parts[1:]:
        total = total + part.astype(F32)
    return total


def layer_norm(values):
    breadth = values.shape[1]
    average = jnp.sum(values, axis=1, keepdims=True) / breadth
    variance = jnp.sum(values * values, axis=1, keepdims=True) / breadth - average * average
    inverse = lax.rsqrt(variance + EPSILON)
    return (values - average) * inverse, inverse


def layer_norm_back(scaled, normed, inverse):
    breadth = scaled.shape[1]
    first = jnp.sum(scaled, axis=1, keepdims=True) / breadth
    second = jnp.sum(scaled * normed, axis=1, keepdims=True) / breadth
    return (inverse * (scaled - first - normed * second)).astype(BF16)


def swish_and_slope(values):
    s = 0.5 * jnp.tanh(0.5 * values) + 0.5
    return (values * s).astype(BF16), s * (1.0 + values * (1.0 - s))


def hot(column, width):
    at = lax.broadcasted_iota(jnp.int32, (column.shape[0], width), 1)
    return jnp.where(column == at, 1.0, 0.0).astype(BF16)


def hot_t(row, height):
    at = lax.broadcasted_iota(jnp.int32, (height, row.shape[1]), 0)
    return jnp.where(row == at, 1.0, 0.0).astype(BF16)


def tile_of(rows):
    if rows <= 1024:
        return rows
    for size in (768, 512, 384, 256, 192, 128, 96, 64, 48, 32, 16):
        if rows % size == 0:
            return size
    return rows


def accumulate(ref, value):
    if pl.num_programs(0) == 1:
        ref[...] = value.astype(ref.dtype)
    else:

        @pl.when(pl.program_id(0) == 0)
        def _():
            ref[...] = value.astype(ref.dtype)

        @pl.when(pl.program_id(0) > 0)
        def _():
            ref[...] += value.astype(ref.dtype)


def shape(dims, dtype=BF16):
    return jax.ShapeDtypeStruct(tuple(dims), dtype)


def whole_block(dims):
    return pl.BlockSpec(tuple(dims), lambda *_: (0,) * len(dims))


def call(kernel, ins, outs, scratch=(), flops=0):
    return pl.pallas_call(
        kernel,
        out_shape=tuple(outs),
        grid=(1,),
        in_specs=[whole_block(x.shape) for x in ins],
        out_specs=tuple(whole_block(x.shape) for x in outs),
        scratch_shapes=list(scratch),
        compiler_params=pltpu.CompilerParams(vmem_limit_bytes=VMEM_LIMIT),
        cost_estimate=pl.CostEstimate(
            flops=flops,
            bytes_accessed=sum(x.size * x.dtype.itemsize for x in (*ins, *outs)),
            transcendentals=0,
        ),
    )(*ins)


def fill_weights(w_ref, own_in, own_out, pieces, parity, here):
    m = w_ref.shape[0]
    portion = own_out.shape[0]
    half = portion // 2
    at = pl.multiple_of(here * portion, half)
    for k in range(m):
        w_ref[k, pl.ds(at, portion), :] = own_in[k] if k < m - 1 else own_out[...]
    for b, (got, other) in enumerate(pieces, start=1):
        start = (here ^ b) * portion
        first = pl.multiple_of(start + parity * half, half)
        second = pl.multiple_of(start + (1 - parity) * half, half)
        for k in range(m):
            w_ref[k, pl.ds(first, half), :] = got[k * half : (k + 1) * half, :]
            w_ref[k, pl.ds(second, half), :] = other[k * half : (k + 1) * half, :]


def split_grads(grads, n, keep, send, parity, here):
    m = grads.shape[0]
    portion = grads.shape[1] // n
    half = portion // 2
    block = m * half
    for side in range(2):

        @pl.when(parity == side)
        def _():
            for f in range(n):
                for u in range(2 * m):
                    out = keep if u // m == side else send
                    at = f * portion + (u % 2) * half
                    start = pl.multiple_of((f ^ here) * block + (u % m) * half, half)
                    out[pl.ds(start, half), :] = grads[u // 2, at : at + half, :].astype(BF16)


def prepare_kernel(edge_in, edge_out, node_in, node_out, edge_gain, node_gain, lat, rows, *refs):
    edge_pack, node_pack, lat_out, rows_out, sems, edge_held, node_held = refs
    half = edge_out.shape[0] // 2
    at = pl.multiple_of(lax.axis_index("region") % 2 * half, half)
    moves = [(edge_gain, edge_held), (node_gain, node_held)]
    for inner, outer, pack in ((edge_in, edge_out, edge_pack), (node_in, node_out, node_pack)):
        m = inner.shape[0]
        for k in range(m):
            moves.append((inner.at[k, pl.ds(at, half)], pack.at[pl.ds(k * half, half)]))
        moves.append((outer.at[pl.ds(at, half)], pack.at[pl.ds(m * half, half)]))
    moves += [(lat, lat_out), (rows, rows_out)]
    copies = [pltpu.make_async_copy(a, b, sems.at[k]) for k, (a, b) in enumerate(moves)]
    for copy in copies:
        copy.start()
    below = edge_pack.shape[0] - 16
    edge_pack[below:, :] = jnp.zeros((16, edge_pack.shape[1]), BF16)
    for copy in copies:
        copy.wait()
    parts = []
    for ref in (edge_held, node_held):
        left = ref[...]
        for _ in range(3):
            part = left.astype(BF16)
            left = left - part.astype(F32)
            parts.append(part.astype(F32))
    parts.append(jnp.zeros((16 - len(parts), left.shape[1]), F32))
    edge_pack[below:, : left.shape[1]] = jnp.concatenate(parts, axis=0).astype(BF16)


def prepare(*ins):
    edge_in, edge_out, node_in, _, edge_gain, _, lat, rows = ins
    half, d = edge_out.shape[0] // 2, edge_out.shape[1]
    counts = [(edge_in.shape[0] + 1), (node_in.shape[0] + 1)]
    outs = [shape((counts[0] * half + 16, d)), shape((counts[1] * half, d)), shape(lat.shape), shape(rows.shape, rows.dtype)]
    return pl.pallas_call(
        prepare_kernel,
        out_shape=tuple(outs),
        grid=(1,),
        in_specs=[pl.BlockSpec(memory_space=pltpu.HBM)] * len(ins),
        out_specs=tuple(whole_block(x.shape) for x in outs),
        scratch_shapes=[pltpu.SemaphoreType.DMA((sum(counts) + 4,))] + [pltpu.VMEM(edge_gain.shape, F32)] * 2,
        compiler_params=pltpu.CompilerParams(vmem_limit_bytes=VMEM_LIMIT),
        cost_estimate=pl.CostEstimate(flops=8 * half * d, bytes_accessed=32 * half * d, transcendentals=0),
        name="prepare",
    )(*(pltpu.with_memory_space_constraint(x, pltpu.HBM) for x in ins))


def fill_gains(gain_ref, blocks, own, pieces, here):
    portion = blocks.shape[2]
    blocks[here, 0:1, :] = own[0][...]
    blocks[here, 1:2, :] = own[1][...]
    for b, (got, _) in enumerate(pieces, start=1):
        parts = got[got.shape[0] - 16 :, :portion].astype(F32)
        blocks[here ^ b, 0:1, :] = parts[0:1] + parts[1:2] + parts[2:3]
        blocks[here ^ b, 1:2, :] = parts[3:4] + parts[4:5] + parts[5:6]
    for f in range(blocks.shape[0]):
        gain_ref[0:2, f * portion : (f + 1) * portion] = blocks[f, 0:2, :]


def outgoing_kernel(n, rows_ref, *refs):
    near, (keep, send, at_ref) = refs[:n], refs[n:]
    own = near[0].shape[0]
    here = lax.axis_index("feat")
    region = lax.axis_index("region")
    regions, slots = rows_ref.shape
    for b in range(regions):
        row = rows_ref[pl.ds(region ^ b, 1), :]
        feat = jnp.zeros_like(row)
        for k in range(1, n):
            feat = feat + jnp.where(row >= k * own, 1, 0)
        at_ref[0:1, b * slots : (b + 1) * slots] = (feat ^ here) * own + row - feat * own
    at = at_ref[0:1, :]
    rows = jnp.zeros((at.shape[1], near[0].shape[1]), F32)
    for b in range(n):
        rows = rows + t_dot(hot_t(at - b * own, own), near[b][...])
    rows = rows.astype(BF16)
    pairs, slots, _ = keep.shape
    for b in range(pairs):
        keep[b] = rows[(2 * b) * slots : (2 * b + 1) * slots]
        send[b] = rows[(2 * b + 1) * slots : (2 * b + 2) * slots]


def join_kernel(keep, other, *outs):
    slots = keep.shape[1]
    for b, out in enumerate(outs):
        out[:slots, :] = keep[b]
        out[slots:, :] = other[b]


def edge_forward_kernel(n, pairs, *refs):
    edge, s_at, r_at, r_row, edge_gain, node_gain, own_in, own_out = refs[:8]
    refs = refs[8:]
    tables, refs = refs[: n + pairs], refs[n + pairs :]
    pieces = [(refs[2 * b], refs[2 * b + 1]) for b in range(n - 1)]
    refs = refs[2 * (n - 1) :]
    new, hidden_ref, slope_ref, normed_ref, inverse_ref, table, w, gains = refs[:8]
    pooled, total, blocks = refs[8 : 8 + n], refs[8 + n], refs[9 + n]
    here = lax.axis_index("feat")
    parity = lax.axis_index("region") % 2
    own = tables[0].shape[0]
    nodes = own * n

    @pl.when(pl.program_id(0) == 0)
    def _():
        at = 0
        for piece in tables:
            table[at : at + piece.shape[0], :] = piece[...]
            at += piece.shape[0]
        fill_weights(w, own_in, own_out, pieces, parity, here)
        fill_gains(gains, blocks, (edge_gain, node_gain), pieces, here)

    lat = edge[...]
    senders = dot(hot(s_at[...], table.shape[0]), table[...]).astype(BF16)
    receivers = dot(hot(r_at[...], nodes), table[:nodes, :]).astype(BF16)
    pre = dot(lat, w[0]) + dot(senders, w[1]) + dot(receivers, w[2])
    hidden, slope = swish_and_slope(pre)
    hidden_ref[...] = hidden
    slope_ref[...] = slope.astype(BF16)
    normed, inverse = layer_norm(dot(hidden, w[3]))
    normed_ref[...] = normed.astype(BF16)
    inverse_ref[...] = jnp.broadcast_to(inverse, inverse_ref.shape)
    updated = (lat.astype(F32) + normed * gains[0:1, :]).astype(BF16)
    new[...] = updated
    accumulate(total, dot(hot_t(r_row[...], nodes), updated))

    @pl.when(pl.program_id(0) == pl.num_programs(0) - 1)
    def _():
        for b in range(n):
            pooled[b][...] = total[b * own : (b + 1) * own, :].astype(BF16)


def node_kernel(n, lat_ref, cot_ref, gains, own_in, own_out, *refs):
    parts, refs = refs[:n], refs[n:]
    pieces = [(refs[2 * b], refs[2 * b + 1]) for b in range(n - 1)]
    refs = refs[2 * (n - 1) :]
    new, pooled_grad, base = refs[:3]
    messages, w = refs[3 : 3 + n], refs[3 + n]
    here = lax.axis_index("feat")
    parity = lax.axis_index("region") % 2
    gain = gains[1:2, :]
    fill_weights(w, own_in, own_out, pieces, parity, here)
    pooled = add_all([part[...] for part in parts]).astype(BF16)
    lat = lat_ref[...]
    pre = dot(lat, w[0]) + dot(pooled, w[1])
    hidden, slope = swish_and_slope(pre)
    normed, inverse = layer_norm(dot(hidden, w[2]))
    new[...] = (lat.astype(F32) + normed * gain).astype(BF16)
    cot = cot_ref[...].astype(F32)
    mix_grad = layer_norm_back(cot * gain, normed, inverse)
    pre_grad = (dot_t(mix_grad, w[2]) * slope).astype(BF16)
    pooled_grad[...] = dot_t(pre_grad, w[1]).astype(BF16)
    base[...] = cot + dot_t(pre_grad, w[0])
    d = lat.shape[1]
    portion = d // n
    for b in range(n):
        messages[b][:, :d] = pre_grad
        messages[b][:, d : 2 * d] = mix_grad
    for f in range(n):

        @pl.when(here == f)
        def _():
            for b in range(n):
                block = slice((f ^ b) * portion, ((f ^ b) + 1) * portion)
                messages[b][:, 2 * d : 2 * d + portion] = pooled[:, block]
                messages[b][:, 2 * d + portion :] = hidden[:, block]


def node_weight_kernel(n, *refs):
    near, messages, (keep, send, lat, grads) = refs[:n], refs[n : 2 * n], refs[2 * n :]
    here = lax.axis_index("feat")
    parity = lax.axis_index("region") % 2
    _, d = near[0].shape
    portion = d // n
    for f in range(n):

        @pl.when(here == f)
        def _():
            for b in range(n):
                lat[b] = near[b][:, f * portion : (f + 1) * portion]

    totals = [jnp.zeros((portion, d), F32)] * 3
    for b in range(n):
        pre_grad = messages[b][:, :d]
        mix_grad = messages[b][:, d : 2 * d]
        totals[0] = totals[0] + t_dot(lat[b], pre_grad)
        totals[1] = totals[1] + t_dot(messages[b][:, 2 * d : 2 * d + portion], pre_grad)
        totals[2] = totals[2] + t_dot(messages[b][:, 2 * d + portion :], mix_grad)
    for k in range(3):
        grads[k * portion : (k + 1) * portion, :] = totals[k]
    half = keep.shape[0]
    keep[...] = grads[pl.ds(pl.multiple_of(parity * half, 16), half), :].astype(BF16)
    send[...] = grads[pl.ds(pl.multiple_of((1 - parity) * half, 16), half), :].astype(BF16)


def edge_backward_kernel(n, slots, *refs):
    edge, cot, hidden, slope, normed, inverse, r_at, s_row, r_row, gains, table, w = refs[:12]
    near, refs = refs[12 : 12 + n], refs[12 + n :]
    pre_grad_ref, keep, send, sent_ref, received_ref, near_all = refs[:6]
    grads, sent, received = refs[6:]
    here = lax.axis_index("feat")
    parity = lax.axis_index("region") % 2
    own = near[0].shape[0]
    nodes = own * n

    @pl.when(pl.program_id(0) == 0)
    def _():
        for b in range(n):
            near_all[b * own : (b + 1) * own, :] = near[b][...]

    total = cot[...].astype(F32) + dot(hot(r_at[...], nodes), near_all[...])
    mix_grad = layer_norm_back(total * gains[0:1, :], normed[...].astype(F32), inverse[:, :1])
    pre_grad = (dot_t(mix_grad, w[3]) * slope[...].astype(F32)).astype(BF16)
    pre_grad_ref[...] = pre_grad
    accumulate(grads.at[0], t_dot(edge[...], pre_grad))
    accumulate(grads.at[3], t_dot(hidden[...], mix_grad))
    accumulate(sent, dot(hot_t(s_row[...], table.shape[0]), pre_grad))
    accumulate(received, dot(hot_t(r_row[...], nodes), pre_grad))

    @pl.when(pl.program_id(0) == pl.num_programs(0) - 1)
    def _():
        from_senders = sent[...].astype(BF16)
        from_receivers = received[...].astype(BF16)
        grads[1] = t_dot(table[...], from_senders).astype(grads.dtype)
        grads[2] = t_dot(table[:nodes, :], from_receivers).astype(grads.dtype)
        split_grads(grads, n, keep, send, parity, here)
        sent_ref[...] = from_senders
        received_ref[...] = from_receivers
        back = dot_t(from_senders[nodes:], w[1]).astype(BF16)
        at = n * grads.shape[0] * (grads.shape[1] // n // 2)
        count = (keep.shape[0] - at) // slots
        for b in range(count):
            rows = slice(at + b * slots, at + (b + 1) * slots)
            keep[rows, :] = back[(2 * b) * slots : (2 * b + 1) * slots]
            send[rows, :] = back[(2 * b + 1) * slots : (2 * b + 2) * slots]


def edge_grad_kernel(cot, r_at, near, pre_grad, w, out):
    total = cot[...].astype(F32) + dot(hot(r_at[...], near.shape[0]), near[...])
    out[...] = total + dot_t(pre_grad[...], w[0])


def return_kernel(n, pairs, sent, received, w, at_ref, *refs):
    blocks, outs = refs[:pairs], refs[pairs:]
    nodes = received.shape[0]
    own = nodes // n
    rows = at_ref.shape[1] // pairs
    total = dot_t(sent[:nodes, :], w[1]) + dot_t(received[...], w[2])
    for b in range(pairs):
        total = total + dot(hot_t(at_ref[0:1, b * rows : (b + 1) * rows], nodes), blocks[b][:rows, :])
    for b in range(n):
        outs[b][...] = total[b * own : (b + 1) * own, :].astype(BF16)


def total_kernel(*refs):
    refs[-1][...] = add_all([part[...] for part in refs[:-1]])


def pair_sum_kernel(n, keep, got, *outs):
    block = outs[0].shape[0]
    for b in range(n):
        rows = slice(b * block, (b + 1) * block)
        outs[b][...] = (keep[rows, :].astype(F32) + got[rows, :].astype(F32)).astype(BF16)


def chip_rows_kernel(slots, mine, theirs, *refs):
    pairs = mine.shape[0] // slots
    node_parts, outs, total = (refs[:2], refs[2:-1], refs[-1]) if len(refs) > pairs else ((), refs, None)
    z = lax.axis_index("region") // 2
    if node_parts:
        total[...] = add_all([part[...] for part in node_parts])
    for b, out in enumerate(outs):
        out[:slots, :] = mine[b * slots : (b + 1) * slots, :]
        out[slots : 2 * slots, :] = theirs[b * slots : (b + 1) * slots, :]
        if node_parts:
            rows = out.shape[0] - 2 * slots
            out[2 * slots :, :] = total[pl.ds(pl.multiple_of((z ^ b) * rows, 16), rows), :].astype(BF16)


def scatter_sum_kernel(n, pairs, *refs):
    parts, outs, total = refs[:n], refs[n : n + pairs], refs[n + pairs]
    z = lax.axis_index("region") // 2
    total[...] = add_all([part[...] for part in parts])
    rows = outs[0].shape[0]
    for b in range(pairs):
        outs[b][...] = total[pl.ds(pl.multiple_of((z ^ b) * rows, rows), rows), :].astype(BF16)


def sum_kernel(pairs, *refs):
    edge, node, out = refs[:pairs], refs[pairs : 2 * pairs], refs[2 * pairs]
    cut = edge[0].shape[0]
    first = node[0].shape[0] - (out.shape[0] - cut)
    out[:cut, :] = add_all([part[...] for part in edge]).astype(BF16)
    out[cut:, :] = add_all([part[first:, :] for part in node]).astype(BF16)


def finish_kernel(pairs, cut, edge_norm, node_norm, *refs):
    mine, theirs = refs[:pairs], refs[pairs : 2 * pairs]
    outs, total = refs[2 * pairs : -1], refs[-1]
    region = lax.axis_index("region")
    parity, z = region % 2, region // 2
    rows = mine[0].shape[0]
    for b in range(pairs):
        for side, ref in ((parity, mine[b]), (1 - parity, theirs[b])):
            base = side * pairs * rows
            start = pl.multiple_of(base + (z ^ b) * cut, 16)
            total[pl.ds(start, cut), :] = ref[:cut, :].astype(F32)
            start = pl.multiple_of(base + pairs * cut + (z ^ b) * (rows - cut), 16)
            total[pl.ds(start, rows - cut), :] = ref[cut:, :].astype(F32)
    spread(total, outs, edge_norm, node_norm)


def spread(total, outs, edge_norm, node_norm):
    portion = outs[1].shape[0]
    size = total.shape[0] // 2
    for norm, m, at, pair in ((edge_norm, 4, 0, outs[:2]), (node_norm, 3, 2 * portion, outs[2:])):
        half = m * portion // 2
        for u in range(2 * m):
            row = u * (portion // 2)
            source = (row // half) * size + at + row % half
            out, start = (pair[0], row) if u < 2 * m - 2 else (pair[1], row - (m - 1) * portion)
            out[start : start + portion // 2, :] = total[source : source + portion // 2, :] * norm


def gather_halves(mine):
    pieces = []
    for b in range(1, lax.axis_size("feat")):
        got = swap(mine, "feat", b)
        pieces += [got, swap(got, "region", 1)]
    return pieces


def chip_exchange(blocks):
    return [blocks[0]] + [swap(blocks[b], "region", 2 * b) for b in range(1, len(blocks))]


def reduce_grads(parts, node_parts, back, slots, portion, edge_norm, node_norm):
    n = len(parts)
    half, d = parts[0].shape
    pairs = lax.axis_size("region") // 2
    z = lax.axis_index("region") // 2
    parity = lax.axis_index("region") % 2
    node_half = node_parts[0].shape[0]
    size = half + node_half
    rows, cut = size // pairs, half // pairs
    aligned = cut % 16 == 0 and rows % 16 == 0
    outs = [shape((k * portion, d), F32) for k in (3, 1, 2, 1)]

    def chunks(parts):
        mine = add_all(parts).astype(BF16).reshape(pairs, -1, d)
        return [lax.dynamic_index_in_dim(mine, z ^ b, 0, keepdims=False) for b in range(pairs)]

    given = node_parts if aligned else []
    returned = call(
        functools.partial(chip_rows_kernel, slots),
        [*back, *given],
        [shape((2 * slots + (rows - cut if given else 0), d))] * pairs,
        [pltpu.VMEM((node_half, d), F32)] if given else [],
    )
    if not aligned:
        returned = [jnp.concatenate(pair) for pair in zip(returned, chunks(node_parts))]
    returned = chip_exchange(returned)
    if aligned:
        parts = call(
            functools.partial(scatter_sum_kernel, n, pairs),
            parts,
            [shape((cut, d))] * pairs,
            [pltpu.VMEM((half, d), F32)],
        )
    else:
        parts = chunks(parts)
    parts = chip_exchange(parts)
    if aligned:
        (chunk,) = call(functools.partial(sum_kernel, pairs), [*parts, *returned], [shape((rows, d))])
    else:
        node_parts = [part[2 * slots :] for part in returned]
        chunk = jnp.concatenate([add_all(parts), add_all(node_parts)]).astype(BF16)
    mine = chip_exchange([chunk] * pairs)
    theirs = [swap(piece, "region", 1) for piece in mine]
    if aligned:
        grads = call(
            functools.partial(finish_kernel, pairs, cut, edge_norm, node_norm),
            mine + theirs,
            outs,
            [pltpu.VMEM((2 * size, d), F32)],
        )
        return grads, returned
    order = jnp.arange(pairs) ^ z
    sides = []
    for side in (mine, theirs):
        side = jnp.stack(side)[order]
        sides += [side[:, :cut].reshape(half, d), side[:, cut:].reshape(node_half, d)]
    swapped = sides[2:] + sides[:2]
    total = jnp.where(parity == 0, jnp.concatenate(sides), jnp.concatenate(swapped)).astype(F32)

    def from_total(*refs):
        spread(refs[0], refs[1:], edge_norm, node_norm)

    return call(from_total, [total], outs), returned


def layer(
    node_lat,
    edge_lat,
    receiver_row,
    sender_slot,
    send_rows,
    w_edge_in,
    w_edge_out,
    w_node_in,
    w_node_out,
    edge_gain,
    node_gain,
    node_cot,
    edge_cot,
):
    n = lax.axis_size("feat")
    regions = lax.axis_size("region")
    pairs = regions // 2
    here = lax.axis_index("feat")
    region = lax.axis_index("region")
    own, d = node_lat.shape
    nodes = own * n
    share = edge_lat.shape[0]
    slots = send_rows.shape[2]
    table_size = nodes + regions * slots

    def relative(row):
        return ((row // own) ^ here) * own + row % own

    local_receivers = lax.dynamic_slice_in_dim(receiver_row, here * share, share)
    local_senders = lax.dynamic_slice_in_dim(sender_slot, here * share, share)
    remote = jnp.maximum(local_senders - nodes, 0)
    sender_at = jnp.where(
        local_senders < nodes,
        relative(local_senders),
        nodes + ((remote // slots) ^ region) * slots + remote % slots,
    )
    receiver_at = relative(local_receivers)
    sender_column, receiver_column, receiver_line = sender_at[:, None], receiver_at[:, None], receiver_at[None]

    portion = d // n
    half = portion // 2
    gain_rows = [edge_gain[None], node_gain[None]]
    edge_pack, node_pack, own_lat, listed = prepare(
        w_edge_in, w_edge_out, w_node_in, w_node_out, *gain_rows, node_lat, send_rows[0]
    )
    near = [own_lat] + feat_swaps([node_lat] * n)[1:]
    w_edge = gather_halves(edge_pack)

    square = 2 * d * d
    keep, send, send_at = call(
        functools.partial(outgoing_kernel, n),
        [listed, *near],
        [shape((pairs, slots, d))] * 2 + [shape((8, regions * slots), jnp.int32)],
        flops=2 * regions * slots * nodes * d,
    )
    other = swap(send, "region", 1)
    remote_rows = chip_exchange(call(join_kernel, [keep, other], [shape((2 * slots, d))] * pairs))
    w_node = gather_halves(node_pack)

    tile = tile_of(share)
    steps = share // tile
    sum_type = BF16 if steps == 1 else F32
    by_rows = lambda width: pl.BlockSpec((tile, width), lambda i: (i, 0))
    by_columns = pl.BlockSpec((1, tile), lambda i: (0, i))
    edge_params = pltpu.CompilerParams(
        dimension_semantics=("arbitrary",), vmem_limit_bytes=VMEM_LIMIT
    )
    ins = [edge_lat, sender_column, receiver_column, receiver_line]
    rest = [*gain_rows, w_edge_in, w_edge_out, *near, *remote_rows, *w_edge]
    outs = [shape((share, d))] * 4 + [shape((share, 128), F32)]
    kept = [shape((table_size, d)), shape((4, d, d)), shape((8, d), F32)] + [shape((own, d))] * n
    edge_new, hidden, slope, normed, inverse, table, w_full, gains, *pooled_parts = pl.pallas_call(
        functools.partial(edge_forward_kernel, n, pairs),
        out_shape=tuple(outs + kept),
        grid=(steps,),
        in_specs=[by_rows(d), by_rows(1), by_rows(1), by_columns]
        + [whole_block(x.shape) for x in rest],
        out_specs=tuple([by_rows(d)] * 4 + [by_rows(128)] + [whole_block(x.shape) for x in kept]),
        scratch_shapes=[pltpu.VMEM((nodes, d), F32), pltpu.VMEM((n, 8, portion), F32)],
        compiler_params=edge_params,
        cost_estimate=pl.CostEstimate(
            flops=7 * share * square, bytes_accessed=8 * share * d, transcendentals=share * d
        ),
        name="edge_forward",
    )(*ins, *rest)

    parts = feat_swaps(pooled_parts)
    node_new, pooled_grad, node_base, *messages = call(
        functools.partial(node_kernel, n),
        [node_lat, node_cot, gains, w_node_in, w_node_out, *parts, *w_node],
        [shape((own, d)), shape((own, d)), shape((own, d), F32)]
        + [shape((own, 2 * d + 2 * portion))] * n,
        [pltpu.VMEM((3, d, d), BF16)],
        flops=6 * own * square,
    )
    grad_near = feat_swaps([pooled_grad] * n)
    messages = feat_swaps(messages)

    ins = [edge_lat, edge_cot, hidden, slope, normed, inverse, receiver_column, sender_at[None], receiver_line]
    rest = [gains, table, w_full, *grad_near]
    kept = [shape((n * 2 * portion + pairs * slots, d))] * 2
    kept += [shape((table_size, d)), shape((nodes, d)), shape((nodes, d))]
    edge_pre_grad, keep, send, sent, received, near_grad = pl.pallas_call(
        functools.partial(edge_backward_kernel, n, slots),
        out_shape=tuple([shape((share, d))] + kept),
        grid=(steps,),
        in_specs=[by_rows(d)] * 5 + [by_rows(128), by_rows(1), by_columns, by_columns]
        + [whole_block(x.shape) for x in rest],
        out_specs=tuple([by_rows(d)] + [whole_block(x.shape) for x in kept]),
        scratch_shapes=[
            pltpu.VMEM((4, d, d), sum_type),
            pltpu.VMEM((table_size, d), sum_type),
            pltpu.VMEM((nodes, d), sum_type),
        ],
        compiler_params=edge_params,
        cost_estimate=pl.CostEstimate(
            flops=10 * share * square, bytes_accessed=16 * share * d, transcendentals=0
        ),
        name="edge_backward",
    )(*ins, *rest)
    got = swap(send, "region", 1)
    node_keep, node_send = call(
        functools.partial(node_weight_kernel, n),
        [*near, *messages],
        [shape((3 * half, d))] * 2,
        [pltpu.VMEM((n, own, portion), BF16), pltpu.VMEM((3 * portion, d), F32)],
        flops=3 * nodes * square // n,
    )
    node_got = swap(node_send, "region", 1)
    outs = call(functools.partial(pair_sum_kernel, n), [keep, got], [shape((4 * half, d))] * n)
    below = n * 4 * half
    grads, returned = reduce_grads(
        feat_swaps(outs),
        [node_keep, node_got],
        [keep[below:], got[below:]],
        slots,
        portion,
        float((share * n * regions) ** -0.5),
        float((nodes * regions) ** -0.5),
    )
    grad_edge_in, grad_edge_out, grad_node_in, grad_node_out = grads

    edge_grad = pl.pallas_call(
        edge_grad_kernel,
        out_shape=shape((share, d), F32),
        grid=(steps,),
        in_specs=[by_rows(d), by_rows(1), whole_block((nodes, d)), by_rows(d), whole_block((1, d, d))],
        out_specs=by_rows(d),
        compiler_params=edge_params,
        cost_estimate=pl.CostEstimate(flops=2 * share * square, bytes_accessed=8 * share * d, transcendentals=0),
        name="edge_grad",
    )(edge_cot, receiver_column, near_grad, edge_pre_grad, w_full)
    parts = call(
        functools.partial(return_kernel, n, pairs),
        [sent, received, w_full, send_at, *returned],
        [shape((own, d))] * n,
        flops=4 * nodes * square,
    )
    (node_grad,) = call(total_kernel, [node_base, *feat_swaps(parts)], [shape((own, d), F32)])

    return (
        node_new,
        edge_new,
        node_grad,
        edge_grad,
        grad_edge_in.reshape(w_edge_in.shape),
        grad_edge_out,
        grad_node_in.reshape(w_node_in.shape),
        grad_node_out,
    )


def solution(mesh):
    rows = P(("region", "feat"), None)
    in_specs = (
        rows,
        rows,
        P("region"),
        P("region"),
        P("region", None, None),
        P(None, "feat", None),
        P("feat", None),
        P(None, "feat", None),
        P("feat", None),
        P("feat"),
        P("feat"),
        rows,
        rows,
    )
    out_specs = (
        rows,
        rows,
        rows,
        rows,
        P(None, "feat", None),
        P("feat", None),
        P(None, "feat", None),
        P("feat", None),
    )
    return jax.shard_map(layer, mesh=mesh, in_specs=in_specs, out_specs=out_specs, check_vma=False)
```

```python
import functools

import jax
import jax.numpy as jnp
from jax import lax
from jax.experimental import pallas as pl
from jax.experimental.pallas import tpu as pltpu
from jax.sharding import PartitionSpec as P


EPSILON = 1e-05
F32 = jnp.float32
BF16 = jnp.bfloat16
VMEM_LIMIT = 36 * 1024 * 1024


def dot(a, b):
    return jnp.dot(a, b, preferred_element_type=F32)


def dot_t(a, b):
    return lax.dot_general(a, b, (((1,), (1,)), ((), ())), preferred_element_type=F32)


def t_dot(a, b):
    return lax.dot_general(a, b, (((0,), (0,)), ((), ())), preferred_element_type=F32)


def swap(x, axis, bits):
    n = lax.axis_size(axis)
    return lax.ppermute(x, axis, [(i, i ^ bits) for i in range(n)])


def feat_swaps(parts):
    return [parts[0]] + [swap(parts[b], "feat", b) for b in range(1, len(parts))]


def add_all(parts):
    total = parts[0].astype(F32)
    for part in parts[1:]:
        total = total + part.astype(F32)
    return total


def layer_norm(values):
    breadth = values.shape[1]
    average = jnp.sum(values, axis=1, keepdims=True) / breadth
    variance = jnp.sum(values * values, axis=1, keepdims=True) / breadth - average * average
    inverse = lax.rsqrt(variance + EPSILON)
    return (values - average) * inverse, inverse


def layer_norm_back(scaled, normed, inverse):
    breadth = scaled.shape[1]
    first = jnp.sum(scaled, axis=1, keepdims=True) / breadth
    second = jnp.sum(scaled * normed, axis=1, keepdims=True) / breadth
    return (inverse * (scaled - first - normed * second)).astype(BF16)


def swish_and_slope(values):
    s = 0.5 * jnp.tanh(0.5 * values) + 0.5
    return (values * s).astype(BF16), s * (1.0 + values * (1.0 - s))


def hot(column, width):
    at = lax.broadcasted_iota(jnp.int32, (column.shape[0], width), 1)
    return jnp.where(column == at, 1.0, 0.0).astype(BF16)


def hot_t(row, height):
    at = lax.broadcasted_iota(jnp.int32, (height, row.shape[1]), 0)
    return jnp.where(row == at, 1.0, 0.0).astype(BF16)


def tile_of(rows):
    if rows <= 1024:
        return rows
    for size in (768, 512, 384, 256, 192, 128, 96, 64, 48, 32, 16):
        if rows % size == 0:
            return size
    return rows


def accumulate(ref, value):
    if pl.num_programs(0) == 1:
        ref[...] = value.astype(ref.dtype)
    else:

        @pl.when(pl.program_id(0) == 0)
        def _():
            ref[...] = value.astype(ref.dtype)

        @pl.when(pl.program_id(0) > 0)
        def _():
            ref[...] += value.astype(ref.dtype)


def shape(dims, dtype=BF16):
    return jax.ShapeDtypeStruct(tuple(dims), dtype)


def whole_block(dims):
    return pl.BlockSpec(tuple(dims), lambda *_: (0,) * len(dims))


def call(kernel, ins, outs, scratch=(), flops=0):
    return pl.pallas_call(
        kernel,
        out_shape=tuple(outs),
        grid=(1,),
        in_specs=[whole_block(x.shape) for x in ins],
        out_specs=tuple(whole_block(x.shape) for x in outs),
        scratch_shapes=list(scratch),
        compiler_params=pltpu.CompilerParams(vmem_limit_bytes=VMEM_LIMIT),
        cost_estimate=pl.CostEstimate(
            flops=flops,
            bytes_accessed=sum(x.size * x.dtype.itemsize for x in (*ins, *outs)),
            transcendentals=0,
        ),
    )(*ins)


def fill_weights(w_ref, own_in, own_out, pieces, parity, here):
    m = w_ref.shape[0]
    portion = own_out.shape[0]
    half = portion // 2
    at = pl.multiple_of(here * portion, half)
    for k in range(m):
        w_ref[k, pl.ds(at, portion), :] = own_in[k] if k < m - 1 else own_out[...]
    for b, (got, other) in enumerate(pieces, start=1):
        start = (here ^ b) * portion
        first = pl.multiple_of(start + parity * half, half)
        second = pl.multiple_of(start + (1 - parity) * half, half)
        for k in range(m):
            w_ref[k, pl.ds(first, half), :] = got[k * half : (k + 1) * half, :]
            w_ref[k, pl.ds(second, half), :] = other[k * half : (k + 1) * half, :]


def split_grads(grads, n, keep, send, parity, here):
    m = grads.shape[0]
    portion = grads.shape[1] // n
    half = portion // 2
    block = m * half
    for side in range(2):

        @pl.when(parity == side)
        def _():
            for f in range(n):
                for u in range(2 * m):
                    out = keep if u // m == side else send
                    at = f * portion + (u % 2) * half
                    start = pl.multiple_of((f ^ here) * block + (u % m) * half, half)
                    out[pl.ds(start, half), :] = grads[u // 2, at : at + half, :].astype(BF16)


def prepare_kernel(edge_in, edge_out, node_in, node_out, edge_gain, node_gain, lat, rows, *refs):
    edge_pack, node_pack, lat_out, rows_out, sems, edge_held, node_held = refs
    half = edge_out.shape[0] // 2
    at = pl.multiple_of(lax.axis_index("region") % 2 * half, half)
    moves = [(edge_gain, edge_held), (node_gain, node_held)]
    for inner, outer, pack in ((edge_in, edge_out, edge_pack), (node_in, node_out, node_pack)):
        m = inner.shape[0]
        for k in range(m):
            moves.append((inner.at[k, pl.ds(at, half)], pack.at[pl.ds(k * half, half)]))
        moves.append((outer.at[pl.ds(at, half)], pack.at[pl.ds(m * half, half)]))
    moves += [(lat, lat_out), (rows, rows_out)]
    copies = [pltpu.make_async_copy(a, b, sems.at[k]) for k, (a, b) in enumerate(moves)]
    for copy in copies:
        copy.start()
    below = edge_pack.shape[0] - 16
    edge_pack[below:, :] = jnp.zeros((16, edge_pack.shape[1]), BF16)
    for copy in copies:
        copy.wait()
    parts = []
    for ref in (edge_held, node_held):
        left = ref[...]
        for _ in range(3):
            part = left.astype(BF16)
            left = left - part.astype(F32)
            parts.append(part.astype(F32))
    parts.append(jnp.zeros((16 - len(parts), left.shape[1]), F32))
    edge_pack[below:, : left.shape[1]] = jnp.concatenate(parts, axis=0).astype(BF16)


def prepare(*ins):
    edge_in, edge_out, node_in, _, edge_gain, _, lat, rows = ins
    half, d = edge_out.shape[0] // 2, edge_out.shape[1]
    counts = [(edge_in.shape[0] + 1), (node_in.shape[0] + 1)]
    outs = [shape((counts[0] * half + 16, d)), shape((counts[1] * half, d)), shape(lat.shape), shape(rows.shape, rows.dtype)]
    return pl.pallas_call(
        prepare_kernel,
        out_shape=tuple(outs),
        grid=(1,),
        in_specs=[pl.BlockSpec(memory_space=pltpu.HBM)] * len(ins),
        out_specs=tuple(whole_block(x.shape) for x in outs),
        scratch_shapes=[pltpu.SemaphoreType.DMA((sum(counts) + 4,))] + [pltpu.VMEM(edge_gain.shape, F32)] * 2,
        compiler_params=pltpu.CompilerParams(vmem_limit_bytes=VMEM_LIMIT),
        cost_estimate=pl.CostEstimate(flops=8 * half * d, bytes_accessed=32 * half * d, transcendentals=0),
        name="prepare",
    )(*(pltpu.with_memory_space_constraint(x, pltpu.HBM) for x in ins))


def fill_gains(gain_ref, blocks, own, pieces, here):
    portion = blocks.shape[2]
    blocks[here, 0:1, :] = own[0][...]
    blocks[here, 1:2, :] = own[1][...]
    for b, (got, _) in enumerate(pieces, start=1):
        parts = got[got.shape[0] - 16 :, :portion].astype(F32)
        blocks[here ^ b, 0:1, :] = parts[0:1] + parts[1:2] + parts[2:3]
        blocks[here ^ b, 1:2, :] = parts[3:4] + parts[4:5] + parts[5:6]
    for f in range(blocks.shape[0]):
        gain_ref[0:2, f * portion : (f + 1) * portion] = blocks[f, 0:2, :]


def outgoing_kernel(n, rows_ref, *refs):
    near, (keep, send, at_ref) = refs[:n], refs[n:]
    own = near[0].shape[0]
    here = lax.axis_index("feat")
    region = lax.axis_index("region")
    regions, slots = rows_ref.shape
    for b in range(regions):
        row = rows_ref[pl.ds(region ^ b, 1), :]
        feat = jnp.zeros_like(row)
        for k in range(1, n):
            feat = feat + jnp.where(row >= k * own, 1, 0)
        at_ref[0:1, b * slots : (b + 1) * slots] = (feat ^ here) * own + row - feat * own
    at = at_ref[0:1, :]
    rows = jnp.zeros((at.shape[1], near[0].shape[1]), F32)
    for b in range(n):
        rows = rows + t_dot(hot_t(at - b * own, own), near[b][...])
    rows = rows.astype(BF16)
    pairs, slots, _ = keep.shape
    for b in range(pairs):
        keep[b] = rows[(2 * b) * slots : (2 * b + 1) * slots]
        send[b] = rows[(2 * b + 1) * slots : (2 * b + 2) * slots]


def join_kernel(keep, other, *outs):
    slots = keep.shape[1]
    for b, out in enumerate(outs):
        out[:slots, :] = keep[b]
        out[slots:, :] = other[b]


def edge_forward_kernel(n, pairs, *refs):
    edge, s_at, r_at, r_row, edge_gain, node_gain, own_in, own_out = refs[:8]
    refs = refs[8:]
    tables, refs = refs[: n + pairs], refs[n + pairs :]
    pieces = [(refs[2 * b], refs[2 * b + 1]) for b in range(n - 1)]
    refs = refs[2 * (n - 1) :]
    new, hidden_ref, slope_ref, normed_ref, inverse_ref, table, w, gains = refs[:8]
    pooled, total, blocks = refs[8 : 8 + n], refs[8 + n], refs[9 + n]
    here = lax.axis_index("feat")
    parity = lax.axis_index("region") % 2
    own = tables[0].shape[0]
    nodes = own * n

    @pl.when(pl.program_id(0) == 0)
    def _():
        at = 0
        for piece in tables:
            table[at : at + piece.shape[0], :] = piece[...]
            at += piece.shape[0]
        fill_weights(w, own_in, own_out, pieces, parity, here)
        fill_gains(gains, blocks, (edge_gain, node_gain), pieces, here)

    lat = edge[...]
    senders = dot(hot(s_at[...], table.shape[0]), table[...]).astype(BF16)
    receivers = dot(hot(r_at[...], nodes), table[:nodes, :]).astype(BF16)
    pre = dot(lat, w[0]) + dot(senders, w[1]) + dot(receivers, w[2])
    hidden, slope = swish_and_slope(pre)
    hidden_ref[...] = hidden
    slope_ref[...] = slope.astype(BF16)
    normed, inverse = layer_norm(dot(hidden, w[3]))
    normed_ref[...] = normed.astype(BF16)
    inverse_ref[...] = jnp.broadcast_to(inverse, inverse_ref.shape)
    updated = (lat.astype(F32) + normed * gains[0:1, :]).astype(BF16)
    new[...] = updated
    accumulate(total, dot(hot_t(r_row[...], nodes), updated))

    @pl.when(pl.program_id(0) == pl.num_programs(0) - 1)
    def _():
        for b in range(n):
            pooled[b][...] = total[b * own : (b + 1) * own, :].astype(BF16)


def node_kernel(n, lat_ref, cot_ref, gains, own_in, own_out, *refs):
    parts, refs = refs[:n], refs[n:]
    pieces = [(refs[2 * b], refs[2 * b + 1]) for b in range(n - 1)]
    refs = refs[2 * (n - 1) :]
    new, pre_grad_ref, base, w_pooled = refs[:4]
    messages, w = refs[4 : 4 + n], refs[4 + n]
    here = lax.axis_index("feat")
    parity = lax.axis_index("region") % 2
    gain = gains[1:2, :]
    fill_weights(w, own_in, own_out, pieces, parity, here)
    pooled = add_all([part[...] for part in parts]).astype(BF16)
    lat = lat_ref[...]
    pre = dot(lat, w[0]) + dot(pooled, w[1])
    hidden, slope = swish_and_slope(pre)
    normed, inverse = layer_norm(dot(hidden, w[2]))
    new[...] = (lat.astype(F32) + normed * gain).astype(BF16)
    cot = cot_ref[...].astype(F32)
    mix_grad = layer_norm_back(cot * gain, normed, inverse)
    pre_grad = (dot_t(mix_grad, w[2]) * slope).astype(BF16)
    pre_grad_ref[...] = pre_grad
    w_pooled[...] = w[1]
    base[...] = cot + dot_t(pre_grad, w[0])
    d = lat.shape[1]
    portion = d // n
    for b in range(n):
        messages[b][:, :d] = mix_grad
    for f in range(n):

        @pl.when(here == f)
        def _():
            for b in range(n):
                block = slice((f ^ b) * portion, ((f ^ b) + 1) * portion)
                messages[b][:, d : d + portion] = pooled[:, block]
                messages[b][:, d + portion :] = hidden[:, block]


def node_weight_kernel(n, *refs):
    near, pre_grads, messages = refs[:n], refs[n : 2 * n], refs[2 * n : 3 * n]
    keep, send, lat, grads = refs[3 * n :]
    here = lax.axis_index("feat")
    parity = lax.axis_index("region") % 2
    _, d = near[0].shape
    portion = d // n
    for f in range(n):

        @pl.when(here == f)
        def _():
            for b in range(n):
                lat[b] = near[b][:, f * portion : (f + 1) * portion]

    totals = [jnp.zeros((portion, d), F32)] * 3
    for b in range(n):
        pre_grad = pre_grads[b][...]
        mix_grad = messages[b][:, :d]
        totals[0] = totals[0] + t_dot(lat[b], pre_grad)
        totals[1] = totals[1] + t_dot(messages[b][:, d : d + portion], pre_grad)
        totals[2] = totals[2] + t_dot(messages[b][:, d + portion :], mix_grad)
    for k in range(3):
        grads[k * portion : (k + 1) * portion, :] = totals[k]
    half = keep.shape[0]
    keep[...] = grads[pl.ds(pl.multiple_of(parity * half, 16), half), :].astype(BF16)
    send[...] = grads[pl.ds(pl.multiple_of((1 - parity) * half, 16), half), :].astype(BF16)


def edge_backward_kernel(n, slots, *refs):
    edge, cot, hidden, slope, normed, inverse, r_at, s_row, r_row, gains, table, w = refs[:12]
    w_pooled, near, refs = refs[12], refs[13 : 13 + n], refs[13 + n :]
    pre_grad_ref, keep, send, sent_ref, received_ref, near_all = refs[:6]
    grads, sent, received = refs[6:]
    here = lax.axis_index("feat")
    parity = lax.axis_index("region") % 2
    own = near[0].shape[0]
    nodes = own * n

    @pl.when(pl.program_id(0) == 0)
    def _():
        for b in range(n):
            near_all[b * own : (b + 1) * own, :] = near[b][...]
        near_all[...] = dot_t(near_all[...], w_pooled[...]).astype(BF16)

    total = cot[...].astype(F32) + dot(hot(r_at[...], nodes), near_all[...])
    mix_grad = layer_norm_back(total * gains[0:1, :], normed[...].astype(F32), inverse[:, :1])
    pre_grad = (dot_t(mix_grad, w[3]) * slope[...].astype(F32)).astype(BF16)
    pre_grad_ref[...] = pre_grad
    accumulate(grads.at[0], t_dot(edge[...], pre_grad))
    accumulate(grads.at[3], t_dot(hidden[...], mix_grad))
    accumulate(sent, dot(hot_t(s_row[...], table.shape[0]), pre_grad))
    accumulate(received, dot(hot_t(r_row[...], nodes), pre_grad))

    @pl.when(pl.program_id(0) == pl.num_programs(0) - 1)
    def _():
        from_senders = sent[...].astype(BF16)
        from_receivers = received[...].astype(BF16)
        grads[1] = t_dot(table[...], from_senders).astype(grads.dtype)
        grads[2] = t_dot(table[:nodes, :], from_receivers).astype(grads.dtype)
        split_grads(grads, n, keep, send, parity, here)
        sent_ref[...] = from_senders
        received_ref[...] = from_receivers
        back = dot_t(from_senders[nodes:], w[1]).astype(BF16)
        at = n * grads.shape[0] * (grads.shape[1] // n // 2)
        count = (keep.shape[0] - at) // slots
        for b in range(count):
            rows = slice(at + b * slots, at + (b + 1) * slots)
            keep[rows, :] = back[(2 * b) * slots : (2 * b + 1) * slots]
            send[rows, :] = back[(2 * b + 1) * slots : (2 * b + 2) * slots]


def edge_grad_kernel(cot, r_at, near, pre_grad, w, out):
    total = cot[...].astype(F32) + dot(hot(r_at[...], near.shape[0]), near[...])
    out[...] = total + dot_t(pre_grad[...], w[0])


def return_kernel(n, pairs, sent, received, w, at_ref, *refs):
    blocks, outs = refs[:pairs], refs[pairs:]
    nodes = received.shape[0]
    own = nodes // n
    rows = at_ref.shape[1] // pairs
    total = dot_t(sent[:nodes, :], w[1]) + dot_t(received[...], w[2])
    for b in range(pairs):
        total = total + dot(hot_t(at_ref[0:1, b * rows : (b + 1) * rows], nodes), blocks[b][:rows, :])
    for b in range(n):
        outs[b][...] = total[b * own : (b + 1) * own, :].astype(BF16)


def total_kernel(*refs):
    refs[-1][...] = add_all([part[...] for part in refs[:-1]])


def pair_sum_kernel(n, keep, got, *outs):
    block = outs[0].shape[0]
    for b in range(n):
        rows = slice(b * block, (b + 1) * block)
        outs[b][...] = (keep[rows, :].astype(F32) + got[rows, :].astype(F32)).astype(BF16)


def chip_rows_kernel(slots, mine, theirs, *refs):
    pairs = mine.shape[0] // slots
    node_parts, outs, total = (refs[:2], refs[2:-1], refs[-1]) if len(refs) > pairs else ((), refs, None)
    z = lax.axis_index("region") // 2
    if node_parts:
        total[...] = add_all([part[...] for part in node_parts])
    for b, out in enumerate(outs):
        out[:slots, :] = mine[b * slots : (b + 1) * slots, :]
        out[slots : 2 * slots, :] = theirs[b * slots : (b + 1) * slots, :]
        if node_parts:
            rows = out.shape[0] - 2 * slots
            out[2 * slots :, :] = total[pl.ds(pl.multiple_of((z ^ b) * rows, 16), rows), :].astype(BF16)


def scatter_sum_kernel(n, pairs, *refs):
    parts, outs, total = refs[:n], refs[n : n + pairs], refs[n + pairs]
    z = lax.axis_index("region") // 2
    total[...] = add_all([part[...] for part in parts])
    rows = outs[0].shape[0]
    for b in range(pairs):
        outs[b][...] = total[pl.ds(pl.multiple_of((z ^ b) * rows, rows), rows), :].astype(BF16)


def sum_kernel(pairs, *refs):
    edge, node, out = refs[:pairs], refs[pairs : 2 * pairs], refs[2 * pairs]
    cut = edge[0].shape[0]
    first = node[0].shape[0] - (out.shape[0] - cut)
    out[:cut, :] = add_all([part[...] for part in edge]).astype(BF16)
    out[cut:, :] = add_all([part[first:, :] for part in node]).astype(BF16)


def finish_kernel(pairs, cut, edge_norm, node_norm, *refs):
    mine, theirs = refs[:pairs], refs[pairs : 2 * pairs]
    outs, total = refs[2 * pairs : -1], refs[-1]
    region = lax.axis_index("region")
    parity, z = region % 2, region // 2
    rows = mine[0].shape[0]
    for b in range(pairs):
        for side, ref in ((parity, mine[b]), (1 - parity, theirs[b])):
            base = side * pairs * rows
            start = pl.multiple_of(base + (z ^ b) * cut, 16)
            total[pl.ds(start, cut), :] = ref[:cut, :]
            start = pl.multiple_of(base + pairs * cut + (z ^ b) * (rows - cut), 16)
            total[pl.ds(start, rows - cut), :] = ref[cut:, :]
    spread(total, outs, edge_norm, node_norm)


def spread(total, outs, edge_norm, node_norm):
    portion = outs[1].shape[0]
    size = total.shape[0] // 2
    for norm, m, at, pair in ((edge_norm, 4, 0, outs[:2]), (node_norm, 3, 2 * portion, outs[2:])):
        half = m * portion // 2
        for u in range(2 * m):
            row = u * (portion // 2)
            source = (row // half) * size + at + row % half
            out, start = (pair[0], row) if u < 2 * m - 2 else (pair[1], row - (m - 1) * portion)
            out[start : start + portion // 2, :] = total[source : source + portion // 2, :].astype(F32) * norm


def gather_halves(mine):
    pieces = []
    for b in range(1, lax.axis_size("feat")):
        got = swap(mine, "feat", b)
        pieces += [got, swap(got, "region", 1)]
    return pieces


def chip_exchange(blocks):
    return [blocks[0]] + [swap(blocks[b], "region", 2 * b) for b in range(1, len(blocks))]


def reduce_grads(parts, node_parts, back, slots, portion, edge_norm, node_norm):
    n = len(parts)
    half, d = parts[0].shape
    pairs = lax.axis_size("region") // 2
    z = lax.axis_index("region") // 2
    parity = lax.axis_index("region") % 2
    node_half = node_parts[0].shape[0]
    size = half + node_half
    rows, cut = size // pairs, half // pairs
    aligned = cut % 16 == 0 and rows % 16 == 0
    outs = [shape((k * portion, d), F32) for k in (3, 1, 2, 1)]

    def chunks(parts):
        mine = add_all(parts).astype(BF16).reshape(pairs, -1, d)
        return [lax.dynamic_index_in_dim(mine, z ^ b, 0, keepdims=False) for b in range(pairs)]

    given = node_parts if aligned else []
    returned = call(
        functools.partial(chip_rows_kernel, slots),
        [*back, *given],
        [shape((2 * slots + (rows - cut if given else 0), d))] * pairs,
        [pltpu.VMEM((node_half, d), F32)] if given else [],
    )
    if not aligned:
        returned = [jnp.concatenate(pair) for pair in zip(returned, chunks(node_parts))]
    returned = chip_exchange(returned)
    if aligned:
        parts = call(
            functools.partial(scatter_sum_kernel, n, pairs),
            parts,
            [shape((cut, d))] * pairs,
            [pltpu.VMEM((half, d), F32)],
        )
    else:
        parts = chunks(parts)
    parts = chip_exchange(parts)
    if aligned:
        (chunk,) = call(functools.partial(sum_kernel, pairs), [*parts, *returned], [shape((rows, d))])
    else:
        node_parts = [part[2 * slots :] for part in returned]
        chunk = jnp.concatenate([add_all(parts), add_all(node_parts)]).astype(BF16)
    mine = chip_exchange([chunk] * pairs)
    theirs = [swap(piece, "region", 1) for piece in mine]
    if aligned:
        grads = call(
            functools.partial(finish_kernel, pairs, cut, edge_norm, node_norm),
            mine + theirs,
            outs,
            [pltpu.VMEM((2 * size, d), BF16)],
        )
        return grads, returned
    order = jnp.arange(pairs) ^ z
    sides = []
    for side in (mine, theirs):
        side = jnp.stack(side)[order]
        sides += [side[:, :cut].reshape(half, d), side[:, cut:].reshape(node_half, d)]
    swapped = sides[2:] + sides[:2]
    total = jnp.where(parity == 0, jnp.concatenate(sides), jnp.concatenate(swapped)).astype(F32)

    def from_total(*refs):
        spread(refs[0], refs[1:], edge_norm, node_norm)

    return call(from_total, [total], outs), returned


def layer(
    node_lat,
    edge_lat,
    receiver_row,
    sender_slot,
    send_rows,
    w_edge_in,
    w_edge_out,
    w_node_in,
    w_node_out,
    edge_gain,
    node_gain,
    node_cot,
    edge_cot,
):
    n = lax.axis_size("feat")
    regions = lax.axis_size("region")
    pairs = regions // 2
    here = lax.axis_index("feat")
    region = lax.axis_index("region")
    own, d = node_lat.shape
    nodes = own * n
    share = edge_lat.shape[0]
    slots = send_rows.shape[2]
    table_size = nodes + regions * slots

    def relative(row):
        return ((row // own) ^ here) * own + row % own

    local_receivers = lax.dynamic_slice_in_dim(receiver_row, here * share, share)
    local_senders = lax.dynamic_slice_in_dim(sender_slot, here * share, share)
    remote = jnp.maximum(local_senders - nodes, 0)
    sender_at = jnp.where(
        local_senders < nodes,
        relative(local_senders),
        nodes + ((remote // slots) ^ region) * slots + remote % slots,
    )
    receiver_at = relative(local_receivers)
    sender_column, receiver_column, receiver_line = sender_at[:, None], receiver_at[:, None], receiver_at[None]

    portion = d // n
    half = portion // 2
    gain_rows = [edge_gain[None], node_gain[None]]
    edge_pack, node_pack, own_lat, listed = prepare(
        w_edge_in, w_edge_out, w_node_in, w_node_out, *gain_rows, node_lat, send_rows[0]
    )
    near = [own_lat] + feat_swaps([node_lat] * n)[1:]
    w_edge = gather_halves(edge_pack)

    square = 2 * d * d
    keep, send, send_at = call(
        functools.partial(outgoing_kernel, n),
        [listed, *near],
        [shape((pairs, slots, d))] * 2 + [shape((8, regions * slots), jnp.int32)],
        flops=2 * regions * slots * nodes * d,
    )
    other = swap(send, "region", 1)
    remote_rows = chip_exchange(call(join_kernel, [keep, other], [shape((2 * slots, d))] * pairs))
    w_node = gather_halves(node_pack)

    tile = tile_of(share)
    steps = share // tile
    sum_type = BF16 if steps == 1 else F32
    by_rows = lambda width: pl.BlockSpec((tile, width), lambda i: (i, 0))
    by_columns = pl.BlockSpec((1, tile), lambda i: (0, i))
    edge_params = pltpu.CompilerParams(
        dimension_semantics=("arbitrary",), vmem_limit_bytes=VMEM_LIMIT
    )
    ins = [edge_lat, sender_column, receiver_column, receiver_line]
    rest = [*gain_rows, w_edge_in, w_edge_out, *near, *remote_rows, *w_edge]
    outs = [shape((share, d))] * 4 + [shape((share, 128), F32)]
    kept = [shape((table_size, d)), shape((4, d, d)), shape((8, d), F32)] + [shape((own, d))] * n
    edge_new, hidden, slope, normed, inverse, table, w_full, gains, *pooled_parts = pl.pallas_call(
        functools.partial(edge_forward_kernel, n, pairs),
        out_shape=tuple(outs + kept),
        grid=(steps,),
        in_specs=[by_rows(d), by_rows(1), by_rows(1), by_columns]
        + [whole_block(x.shape) for x in rest],
        out_specs=tuple([by_rows(d)] * 4 + [by_rows(128)] + [whole_block(x.shape) for x in kept]),
        scratch_shapes=[pltpu.VMEM((nodes, d), F32), pltpu.VMEM((n, 8, portion), F32)],
        compiler_params=edge_params,
        cost_estimate=pl.CostEstimate(
            flops=7 * share * square, bytes_accessed=8 * share * d, transcendentals=share * d
        ),
        name="edge_forward",
    )(*ins, *rest)

    parts = feat_swaps(pooled_parts)
    node_new, node_pre_grad, node_base, w_pooled, *messages = call(
        functools.partial(node_kernel, n),
        [node_lat, node_cot, gains, w_node_in, w_node_out, *parts, *w_node],
        [shape((own, d)), shape((own, d)), shape((own, d), F32), shape((d, d))]
        + [shape((own, d + 2 * portion))] * n,
        [pltpu.VMEM((3, d, d), BF16)],
        flops=6 * own * square,
    )
    grad_near = feat_swaps([node_pre_grad] * n)
    messages = feat_swaps(messages)

    ins = [edge_lat, edge_cot, hidden, slope, normed, inverse, receiver_column, sender_at[None], receiver_line]
    rest = [gains, table, w_full, w_pooled, *grad_near]
    kept = [shape((n * 2 * portion + pairs * slots, d))] * 2
    kept += [shape((table_size, d)), shape((nodes, d)), shape((nodes, d))]
    edge_pre_grad, keep, send, sent, received, near_grad = pl.pallas_call(
        functools.partial(edge_backward_kernel, n, slots),
        out_shape=tuple([shape((share, d))] + kept),
        grid=(steps,),
        in_specs=[by_rows(d)] * 5 + [by_rows(128), by_rows(1), by_columns, by_columns]
        + [whole_block(x.shape) for x in rest],
        out_specs=tuple([by_rows(d)] + [whole_block(x.shape) for x in kept]),
        scratch_shapes=[
            pltpu.VMEM((4, d, d), sum_type),
            pltpu.VMEM((table_size, d), sum_type),
            pltpu.VMEM((nodes, d), sum_type),
        ],
        compiler_params=edge_params,
        cost_estimate=pl.CostEstimate(
            flops=10 * share * square, bytes_accessed=16 * share * d, transcendentals=0
        ),
        name="edge_backward",
    )(*ins, *rest)
    got = swap(send, "region", 1)
    node_keep, node_send = call(
        functools.partial(node_weight_kernel, n),
        [*near, *grad_near, *messages],
        [shape((3 * half, d))] * 2,
        [pltpu.VMEM((n, own, portion), BF16), pltpu.VMEM((3 * portion, d), F32)],
        flops=3 * nodes * square // n,
    )
    node_got = swap(node_send, "region", 1)
    outs = call(functools.partial(pair_sum_kernel, n), [keep, got], [shape((4 * half, d))] * n)
    below = n * 4 * half
    grads, returned = reduce_grads(
        feat_swaps(outs),
        [node_keep, node_got],
        [keep[below:], got[below:]],
        slots,
        portion,
        float((share * n * regions) ** -0.5),
        float((nodes * regions) ** -0.5),
    )
    grad_edge_in, grad_edge_out, grad_node_in, grad_node_out = grads

    edge_grad = pl.pallas_call(
        edge_grad_kernel,
        out_shape=shape((share, d), F32),
        grid=(steps,),
        in_specs=[by_rows(d), by_rows(1), whole_block((nodes, d)), by_rows(d), whole_block((1, d, d))],
        out_specs=by_rows(d),
        compiler_params=edge_params,
        cost_estimate=pl.CostEstimate(flops=2 * share * square, bytes_accessed=8 * share * d, transcendentals=0),
        name="edge_grad",
    )(edge_cot, receiver_column, near_grad, edge_pre_grad, w_full)
    parts = call(
        functools.partial(return_kernel, n, pairs),
        [sent, received, w_full, send_at, *returned],
        [shape((own, d))] * n,
        flops=4 * nodes * square,
    )
    (node_grad,) = call(total_kernel, [node_base, *feat_swaps(parts)], [shape((own, d), F32)])

    return (
        node_new,
        edge_new,
        node_grad,
        edge_grad,
        grad_edge_in.reshape(w_edge_in.shape),
        grad_edge_out,
        grad_node_in.reshape(w_node_in.shape),
        grad_node_out,
    )


def solution(mesh):
    rows = P(("region", "feat"), None)
    in_specs = (
        rows,
        rows,
        P("region"),
        P("region"),
        P("region", None, None),
        P(None, "feat", None),
        P("feat", None),
        P(None, "feat", None),
        P("feat", None),
        P("feat"),
        P("feat"),
        rows,
        rows,
    )
    out_specs = (
        rows,
        rows,
        rows,
        rows,
        P(None, "feat", None),
        P("feat", None),
        P(None, "feat", None),
        P("feat", None),
    )
    return jax.shard_map(layer, mesh=mesh, in_specs=in_specs, out_specs=out_specs, check_vma=False)
```
